8 devices in a mesh: dp: 2 (over z, y), vp: 4 (over x, core).
Axes of the slice: x: 2, y: 2, z: 1, core: 2. Of those that a mesh axis runs over, the one named last changes fastest.
Arguments:
- hidden: bfloat16 [512, 4096], P('dp'), parts along dimension 0
- w_head: bfloat16 [4096, 64000], P(None, 'vp')
- inv_temp: float32 [512], P('dp'), parts along dimension 0
- target_ids: int32 [512], P('dp'), parts along dimension 0
Outputs:
- output 1: float32 [512, 64000], P(('dp', 'vp')), parts along dimension 0
- output 2: float32 [512], P('dp'), parts along dimension 0
There are 2 independent parts. The reference program is written for one: setup_inputs(seed, part) draws one part's arguments, and reference() takes and returns one part's arrays. A program takes and returns all parts, laid end to end along the dimension named above; an argument that names none is the same for every part.
All inputs are finite; a program needn't handle non-finite values.
Results may differ from the reference program's by a relative error of at most 0.001.
Values are sent between devices in bfloat16 or wider.
A program may use at most 1 GiB of HBM per device.

```python
import math
import jax
import jax.numpy as jnp
from jax import lax

BATCH = 256
HIDDEN = 4096
VOCAB = 64000
W_ROW_BLOCK = 256


def draw_head(key, direction, profile):
    num_blocks = HIDDEN // W_ROW_BLOCK
    dir_blocks = direction.reshape(num_blocks, W_ROW_BLOCK)

    def one_block(block_args):
        block_idx, dir_rows = block_args
        noise_rows = jax.random.normal(jax.random.fold_in(key, block_idx), (W_ROW_BLOCK, VOCAB), jnp.float32)
        head_rows = (noise_rows + dir_rows[:, None] * profile[None, :]) * (HIDDEN ** -0.5)
        return head_rows.astype(jnp.bfloat16)

    blocks = lax.map(one_block, (jnp.arange(num_blocks), dir_blocks))
    return blocks.reshape(HIDDEN, VOCAB)


def setup_inputs(seed: int = 0, part: int = 0) -> dict:
    base_key = jax.random.key(seed)
    shared_key = jax.random.fold_in(base_key, 1)
    part_key = jax.random.fold_in(jax.random.fold_in(base_key, 2), part)
    key_dir, key_head = jax.random.split(shared_key)
    key_hid, key_gain, key_temp, key_ids = jax.random.split(part_key, 4)
    direction = jax.random.normal(key_dir, (HIDDEN,), jnp.float32)
    vocab_pos = jnp.arange(VOCAB, dtype=jnp.float32) / VOCAB
    profile = 1.5 * jnp.exp(-8.0 * vocab_pos)
    w_head = draw_head(key_head, direction, profile)
    row_gain = 2.0 + 0.5 * jax.random.normal(key_gain, (BATCH, 1), jnp.float32)
    hidden = jax.random.normal(key_hid, (BATCH, HIDDEN), jnp.float32) + row_gain * direction[None, :] * (HIDDEN ** -0.5)
    row_pos = jnp.arange(BATCH)
    log_temp = jax.random.uniform(key_temp, (BATCH,), jnp.float32, minval=math.log(0.5), maxval=math.log(32.0))
    inv_temp = jnp.where(row_pos == 0, 32.0, jnp.exp(log_temp))
    target_ids = jax.random.randint(key_ids, (BATCH,), 0, VOCAB, dtype=jnp.int32)
    target_ids = jnp.where(row_pos == 1, VOCAB - 1, target_ids)
    return {"hidden": hidden.astype(jnp.bfloat16), "w_head": w_head, "inv_temp": inv_temp, "target_ids": target_ids}


def reference(hidden, w_head, inv_temp, target_ids):
    logits = jnp.dot(hidden, w_head, preferred_element_type=jnp.float32)
    scaled = logits * inv_temp[:, None]
    row_max = jnp.max(scaled, axis=1, keepdims=True)
    exp_vals = jnp.exp(scaled - row_max)
    probabilities = exp_vals / jnp.sum(exp_vals, axis=1, keepdims=True)
    cdf_table = jnp.cumsum(probabilities, axis=1)
    cdf_at_target = jnp.take_along_axis(cdf_table, target_ids[:, None], axis=1)[:, 0]
    return cdf_table, cdf_at_target
```

```python
import functools

import jax
import jax.numpy as jnp
from jax import lax
from jax.experimental import pallas as pl
from jax.experimental.pallas import tpu as pltpu
from jax.sharding import PartitionSpec as P


LANES = 128
UNIT = 640
CHUNKS = (1, 3, 6, 7, 5, 2, 1)


def _to_rows(vec_1xn):
    n = vec_1xn.shape[1]
    return jnp.transpose(jnp.broadcast_to(vec_1xn, (LANES, n)))


def _logits_kernel(cfg, x_ref, w_ref, invt_ref, tgt_ref, *refs):
    n_dev, shard, base, first, last = cfg
    refs = list(refs)
    if first:
        m_in = s_in = t_in = None
    else:
        m_in, s_in, t_in = refs[:3]
        refs = refs[3:]
    outs, refs = refs[:n_dev], refs[n_dev:]
    m_ref, s_ref, t_ref = refs[:3]
    refs = refs[3:]
    if last:
        pack_ref = refs.pop(0)
    z_ref, invt_rows, tgt_rows = refs
    step = pl.program_id(0)
    me = lax.axis_index("vp")
    rows = x_ref.shape[0] // n_dev

    @pl.when(step == 0)
    def _():
        invt_rows[...] = _to_rows(invt_ref[...])
        tgt_rows[...] = _to_rows(tgt_ref[...].astype(jnp.float32))
        if first:
            m_ref[...] = jnp.full(m_ref.shape, -jnp.inf, jnp.float32)
            s_ref[...] = jnp.zeros_like(s_ref)
            t_ref[...] = jnp.zeros_like(t_ref)
        else:
            m_ref[...] = m_in[...]
            s_ref[...] = s_in[...]
            t_ref[...] = t_in[...]

    z_ref[...] = jnp.dot(x_ref[...], w_ref[...], preferred_element_type=jnp.float32)
    col0 = me * shard + base + step * UNIT
    lane = lax.broadcasted_iota(jnp.int32, (rows, LANES), 1)
    for p in range(n_dev):
        block = pl.ds(pl.multiple_of((me ^ p) * rows, rows), rows)
        scale = invt_rows[block, :]
        tiles = [z_ref[block, t * LANES:(t + 1) * LANES] * scale for t in range(UNIT // LANES)]
        for t, tile in enumerate(tiles):
            outs[p][:, t * LANES:(t + 1) * LANES] = tile
        m_old = m_ref[block, :]
        m_new = functools.reduce(jnp.maximum, tiles, m_old)
        keep = jnp.exp(m_old - m_new)
        total = s_ref[block, :] * keep
        upto = t_ref[block, :] * keep
        target = tgt_rows[block, :]
        for t, tile in enumerate(tiles):
            e = jnp.exp(tile - m_new)
            cols = (lane + (col0 + t * LANES)).astype(jnp.float32)
            total += e
            upto += jnp.where(cols <= target, e, 0.0)
        m_ref[block, :] = m_new
        s_ref[block, :] = total
        t_ref[block, :] = upto

    if last:
        @pl.when(step == pl.num_programs(0) - 1)
        def _():
            m = m_ref[...]
            m_row = jnp.max(m, axis=1, keepdims=True)
            keep = jnp.exp(m - m_row)
            s_row = jnp.sum(s_ref[...] * keep, axis=1, keepdims=True)
            t_row = jnp.sum(t_ref[...] * keep, axis=1, keepdims=True)
            which = lax.broadcasted_iota(jnp.int32, m.shape, 1)
            packed = jnp.where(which == 0, m_row, jnp.where(which == 1, s_row, t_row))
            pack_ref[...] = jnp.transpose(packed)[:8, :]


def _logits(x, w, invt, tgt, stats, n_dev, unit0, units, last):
    batch, depth = x.shape
    shard = w.shape[1]
    rows = batch // n_dev
    first = stats is None
    whole = lambda a: pl.BlockSpec(a, lambda i: (0, 0))
    stat = jax.ShapeDtypeStruct((batch, LANES), jnp.float32)
    out_shape = [jax.ShapeDtypeStruct((rows, units * UNIT), jnp.float32)] * n_dev + [stat] * 3
    out_specs = [pl.BlockSpec((rows, UNIT), lambda i: (0, i))] * n_dev + [whole((batch, LANES))] * 3
    if last:
        out_shape.append(jax.ShapeDtypeStruct((8, batch), jnp.float32))
        out_specs.append(whole((8, batch)))
    in_specs = [
        whole((batch, depth)),
        pl.BlockSpec((depth, UNIT), lambda i: (0, unit0 + i)),
        whole((1, batch)),
        whole((1, batch)),
    ] + ([] if first else [whole((batch, LANES))] * 3)
    cfg = (n_dev, shard, unit0 * UNIT, first, last)
    res = pl.pallas_call(
        functools.partial(_logits_kernel, cfg),
        grid=(units,),
        in_specs=in_specs,
        out_specs=out_specs,
        out_shape=out_shape,
        scratch_shapes=[
            pltpu.VMEM((batch, UNIT), jnp.float32),
            pltpu.VMEM((batch, LANES), jnp.float32),
            pltpu.VMEM((batch, LANES), jnp.float32),
        ],
        compiler_params=pltpu.CompilerParams(
            dimension_semantics=("arbitrary",), vmem_limit_bytes=40 * 2**20
        ),
        cost_estimate=pl.CostEstimate(
            flops=2 * batch * depth * units * UNIT,
            bytes_accessed=2 * depth * (units * UNIT + batch),
            transcendentals=batch * units * UNIT,
        ),
        name="logits",
    )(x, w, invt, tgt, *(() if first else stats))
    return res[:n_dev], res[n_dev:n_dev + 3], (res[n_dev + 3] if last else None)


def _merge_kernel(n_dev, *refs):
    stats, (params_ref, at_ref) = refs[:n_dev], refs[n_dev:]
    me = lax.axis_index("vp")
    batch = stats[0].shape[1]
    rows = batch // n_dev
    ms = [s[0:1, :] for s in stats]
    top = functools.reduce(jnp.maximum, ms)
    keep = [jnp.exp(m - top) for m in ms]
    mass = [s[1:2, :] * k for s, k in zip(stats, keep)]
    upto = sum(s[2:3, :] * k for s, k in zip(stats, keep))
    total = sum(mass)
    at_ref[...] = upto / total
    values = [top, 1.0 / total]
    for p in range(n_dev):
        start = jnp.zeros_like(total)
        for q in range(n_dev):
            start += jnp.where((me ^ q) < (me ^ p), mass[q], 0.0)
        values.append(start)
    which = lax.broadcasted_iota(jnp.int32, (LANES, batch), 0)
    table = jnp.zeros((LANES, batch), jnp.float32)
    for i, v in enumerate(values):
        table = jnp.where(which == i, v, table)
    per_row = jnp.transpose(table)
    out = jnp.zeros((rows, LANES), jnp.float32)
    for d in range(n_dev):
        out = jnp.where(me == d, per_row[d * rows:(d + 1) * rows, :], out)
    params_ref[...] = out


def _merge(stats):
    n_dev = len(stats)
    batch = stats[0].shape[1]
    vmem = pl.BlockSpec(memory_space=pltpu.VMEM)
    return pl.pallas_call(
        functools.partial(_merge_kernel, n_dev),
        in_specs=[vmem] * n_dev,
        out_specs=[vmem] * 2,
        out_shape=[
            jax.ShapeDtypeStruct((batch // n_dev, LANES), jnp.float32),
            jax.ShapeDtypeStruct((1, batch), jnp.float32),
        ],
        cost_estimate=pl.CostEstimate(flops=100_000, bytes_accessed=100_000, transcendentals=1000),
        name="merge",
    )(*stats)


def _cdf_kernel(cfg, *refs):
    peers, shard, base, units, first = cfg
    n = len(peers)
    params_ref = refs[n]
    out_ref, params_out, y_ref, sems = refs[n + (1 if first else 2):]
    me = lax.axis_index("vp")
    rows = params_ref.shape[0]
    tiles = UNIT // LANES
    params = params_ref[...]
    top = jnp.broadcast_to(params[:, 0:1], (rows, LANES))
    inv = jnp.broadcast_to(params[:, 1:2], (rows, LANES))
    k_id = lax.broadcasted_iota(jnp.int32, (3 * LANES, LANES), 0) % LANES
    n_id = lax.broadcasted_iota(jnp.int32, (3 * LANES, LANES), 1)
    tri = jnp.where(k_id <= n_id, 1.0, 0.0).astype(jnp.bfloat16)
    lane = lax.broadcasted_iota(jnp.int32, (rows, LANES), 1)
    updated = params
    copies = []
    for j, p in enumerate(peers):
        z_ref = refs[j]

        def unit(u, carry):
            def cols(t):
                return pl.ds(pl.multiple_of(u * UNIT, UNIT) + t * LANES, LANES)

            e = jnp.concatenate([jnp.exp(z_ref[:, cols(t)] - top) for t in range(tiles)], axis=0)
            hi = e.astype(jnp.bfloat16)
            r1 = e - hi.astype(jnp.float32)
            mid = r1.astype(jnp.bfloat16)
            lo = (r1 - mid.astype(jnp.float32)).astype(jnp.bfloat16)
            prefix = jnp.dot(
                jnp.concatenate([hi, mid, lo], axis=1), tri, preferred_element_type=jnp.float32
            )
            for t in range(tiles):
                part = prefix[t * rows:(t + 1) * rows, :] + carry
                y_ref[j, :, cols(t)] = part * inv
                carry = jnp.broadcast_to(part[:, LANES - 1:LANES], (rows, LANES))
            return carry

        start = jnp.broadcast_to(params[:, 2 + p:3 + p], (rows, LANES))
        end = lax.fori_loop(0, units, unit, start)
        updated = jnp.where(lane == 2 + p, end, updated)
        where = pl.multiple_of((me ^ p) * shard + base, LANES)
        copy = pltpu.make_async_copy(
            y_ref.at[j], out_ref.at[:, pl.ds(where, units * UNIT)], sems.at[j]
        )
        copy.start()
        copies.append(copy)
    params_out[...] = updated
    for copy in copies:
        copy.wait()


def _cdf(blocks, peers, params, out, n_dev, shard, unit0):
    rows, width = blocks[0].shape
    n = len(peers)
    first = out is None
    vmem = pl.BlockSpec(memory_space=pltpu.VMEM)
    hbm = pl.BlockSpec(memory_space=pl.ANY)
    cfg = (peers, shard, unit0 * UNIT, width // UNIT, first)
    return pl.pallas_call(
        functools.partial(_cdf_kernel, cfg),
        in_specs=[vmem] * (n + 1) + ([] if first else [hbm]),
        out_specs=[hbm, vmem],
        out_shape=[
            jax.ShapeDtypeStruct((rows, n_dev * shard), jnp.float32),
            jax.ShapeDtypeStruct(params.shape, jnp.float32),
        ],
        scratch_shapes=[
            pltpu.VMEM((n, rows, width), jnp.float32),
            pltpu.SemaphoreType.DMA((n,)),
        ],
        input_output_aliases={} if first else {n + 1: 0},
        compiler_params=pltpu.CompilerParams(vmem_limit_bytes=32 * 2**20),
        cost_estimate=pl.CostEstimate(
            flops=n * 2 * rows * width * 384,
            bytes_accessed=n * rows * width * 8,
            transcendentals=n * rows * width,
        ),
        name="cdf",
    )(*blocks, params, *(() if first else (out,)))


def solution(mesh):
    n_dev = mesh.shape["vp"]

    def swap(a, p):
        return lax.ppermute(a, "vp", [(i, i ^ p) for i in range(n_dev)])

    def local_step(hidden, w_local, inv_temp, target_ids):
        shard = w_local.shape[1]
        invt = inv_temp.reshape(1, -1)
        tgt = target_ids.reshape(1, -1)
        starts = [sum(CHUNKS[:k]) for k in range(len(CHUNKS))]
        stats, chunks = None, []
        for k, units in enumerate(CHUNKS):
            blocks, stats, packed = _logits(
                hidden, w_local, invt, tgt, stats, n_dev, starts[k], units, k == len(CHUNKS) - 1
            )
            got = [blocks[0]]
            for p in range(1, n_dev):
                got.append(swap(blocks[p], p))
            chunks.append(got)
        packs = [packed]
        for p in range(1, n_dev):
            packs.append(swap(packed, p))
        params, at_target = _merge(packs)
        out = None
        for k in range(len(CHUNKS)):
            out, params = _cdf(chunks[k][:2], (0, 1), params, out, n_dev, shard, starts[k])
        for k in range(len(CHUNKS)):
            out, params = _cdf(chunks[k][2:], (2, 3), params, out, n_dev, shard, starts[k])
        return out, at_target.reshape(-1)

    return jax.shard_map(
        local_step,
        mesh=mesh,
        in_specs=(P("dp", None), P(None, "vp"), P("dp"), P("dp")),
        out_specs=(P(("dp", "vp"), None), P("dp")),
        check_vma=False,
    )
```

```python
import functools

import jax
import jax.numpy as jnp
from jax import lax
from jax.experimental import pallas as pl
from jax.experimental.pallas import tpu as pltpu
from jax.sharding import PartitionSpec as P


LANES = 128
UNIT = 512
HALF = 256
SLOTS = 3
CHUNKS = (1024, 2048, 4096, 4608, 2560, 1024, 640)
EARLY = 3


def _to_rows(vec_1xn):
    n = vec_1xn.shape[1]
    return jnp.transpose(jnp.broadcast_to(vec_1xn, (LANES, n)))


def _logits_kernel(cfg, x_ref, w_ref, invt_ref, tgt_ref, *refs):
    n_dev, shard, base, widths, first, last = cfg
    refs = list(refs)
    if not first:
        m_in, s_in, t_in = refs[:3]
        refs = refs[3:]
    outs = [refs[c * n_dev:(c + 1) * n_dev] for c in range(len(widths))]
    refs = refs[len(widths) * n_dev:]
    m_ref, s_ref, t_ref = refs[:3]
    refs = refs[3:]
    if last:
        pack_ref = refs.pop(0)
    xs, wbuf, zbuf, invt_v, tgt_v, scale_rows, left_rows, tmp, x_sem, w_sem, z_sem, v_sem = refs
    me = lax.axis_index("vp")
    batch = xs.shape[0]
    rows = batch // n_dev
    total_cols = sum(widths)
    n_full, tail = total_cols // UNIT, total_cols % UNIT

    def rows_of(p):
        return pl.ds(pl.multiple_of((me ^ p) * rows, rows), rows)

    def fetch_x(p):
        return pltpu.make_async_copy(x_ref.at[rows_of(p), :], xs.at[pl.ds(p * rows, rows), :], x_sem.at[p])

    def fetch_w(step, width):
        slot = lax.rem(step, SLOTS)
        col = base + step * UNIT
        return [
            pltpu.make_async_copy(
                w_ref.at[:, pl.ds(pl.multiple_of(col + off, LANES), min(HALF, width - off))],
                wbuf.at[slot, :, pl.ds(off, min(HALF, width - off))],
                w_sem.at[slot, off // HALF],
            )
            for off in range(0, width, HALF)
        ]

    def put_z(step, c, off, width):
        slot = lax.rem(step, 2)
        return [
            pltpu.make_async_copy(
                zbuf.at[slot, pl.ds(p * rows, rows), pl.ds(0, width)],
                outs[c][p].at[:, pl.ds(off, width)],
                z_sem.at[slot, p],
            )
            for p in range(n_dev)
        ]

    small = [
        pltpu.make_async_copy(invt_ref, invt_v, v_sem.at[0]),
        pltpu.make_async_copy(tgt_ref, tgt_v, v_sem.at[1]),
    ]
    for copy in small:
        copy.start()
    for p in range(n_dev):
        fetch_x(p).start()
    for i in range(min(SLOTS - 1, n_full)):
        for copy in fetch_w(jnp.int32(i), UNIT):
            copy.start()
    if first:
        m_ref[...] = jnp.full(m_ref.shape, -jnp.inf, jnp.float32)
        s_ref[...] = jnp.zeros_like(s_ref)
        t_ref[...] = jnp.zeros_like(t_ref)
    else:
        m_ref[...] = m_in[...]
        s_ref[...] = s_in[...]
        t_ref[...] = t_in[...]
    for copy in small:
        copy.wait()
    tmp[...] = _to_rows(invt_v[...])
    for p in range(n_dev):
        scale_rows[pl.ds(p * rows, rows), :] = tmp[rows_of(p), :]
    tmp[...] = _to_rows(tgt_v[...].astype(jnp.float32))
    lane = lax.broadcasted_iota(jnp.int32, (rows, LANES), 1)
    for p in range(n_dev):
        left_rows[pl.ds(p * rows, rows), :] = tmp[rows_of(p), :].astype(jnp.int32) - me * shard - lane
    for p in range(n_dev):
        fetch_x(p).wait()

    def compute(step, width):
        slot, zslot = lax.rem(step, SLOTS), lax.rem(step, 2)
        for off, copy in zip(range(0, width, HALF), fetch_w(step, width)):
            wide = min(HALF, width - off)
            copy.wait()
            z = jnp.dot(xs[...], wbuf[slot, :, off:off + wide], preferred_element_type=jnp.float32)
            for t in range(0, wide, LANES):
                zbuf[zslot, :, off + t:off + t + LANES] = z[:, t:t + LANES] * scale_rows[...]
        col = base + step * UNIT
        group = 32
        for r in range(0, batch, group):
            block = slice(r, r + group)
            tiles = [zbuf[zslot, block, t:t + LANES] for t in range(0, width, LANES)]
            m_old = m_ref[block, :]
            m_new = functools.reduce(jnp.maximum, tiles, m_old)
            keep = jnp.exp(m_old - m_new)
            total = s_ref[block, :] * keep
            upto = t_ref[block, :] * keep
            left = left_rows[block, :]
            for t, tile in enumerate(tiles):
                e = jnp.exp(tile - m_new)
                total += e
                upto += jnp.where(left >= col + t * LANES, e, 0.0)
            m_ref[block, :] = m_new
            s_ref[block, :] = total
            t_ref[block, :] = upto

    def body(step, _):
        ahead = step + SLOTS - 1

        @pl.when(ahead < n_full)
        def _():
            for copy in fetch_w(ahead, UNIT):
                copy.start()

        if tail:
            @pl.when(ahead == n_full)
            def _():
                for copy in fetch_w(ahead, tail):
                    copy.start()

        @pl.when(step >= 2)
        def _():
            for copy in put_z(step, 0, 0, UNIT):
                copy.wait()

        compute(step, UNIT)
        begin = 0
        for c, width in enumerate(widths):
            lo = begin // UNIT
            hi = lo + width // UNIT

            @pl.when((step >= lo) & (step < hi))
            def _(c=c, lo=lo):
                for copy in put_z(step, c, pl.multiple_of((step - lo) * UNIT, UNIT), UNIT):
                    copy.start()

            begin += width
        return 0

    lax.fori_loop(0, n_full, body, 0)
    left_over = [(i, UNIT) for i in range(max(0, n_full - 2), n_full)]
    if tail:
        if n_full >= 2:
            for copy in put_z(jnp.int32(n_full), 0, 0, UNIT):
                copy.wait()
            left_over = left_over[1:]
        compute(jnp.int32(n_full), tail)
        for copy in put_z(jnp.int32(n_full), len(widths) - 1, widths[-1] - tail, tail):
            copy.start()
        left_over.append((n_full, tail))
    if last:
        m = m_ref[...]
        m_row = jnp.max(m, axis=1, keepdims=True)
        keep = jnp.exp(m - m_row)
        s_row = jnp.sum(s_ref[...] * keep, axis=1, keepdims=True)
        t_row = jnp.sum(t_ref[...] * keep, axis=1, keepdims=True)
        which = lax.broadcasted_iota(jnp.int32, m.shape, 1)
        packed = jnp.where(which == 0, m_row, jnp.where(which == 1, s_row, t_row))
        for p in range(n_dev):
            tmp[rows_of(p), :] = packed[p * rows:(p + 1) * rows, :]
        pack_ref[...] = jnp.transpose(tmp[...])[:8, :]
    for step, width in left_over:
        for copy in put_z(jnp.int32(step), 0, 0, width):
            copy.wait()


def _logits(x, w, invt, tgt, stats, n_dev, base, widths, last):
    batch, depth = x.shape
    shard = w.shape[1]
    rows = batch // n_dev
    first = stats is None
    cols = sum(widths)
    hbm = pl.BlockSpec(memory_space=pltpu.HBM)
    vmem = pl.BlockSpec(memory_space=pltpu.VMEM)
    stat = jax.ShapeDtypeStruct((batch, LANES), jnp.float32)
    out_shape = [pltpu.HBM((rows, width), jnp.float32) for width in widths for _ in range(n_dev)] + [stat] * 3
    out_specs = [hbm] * (n_dev * len(widths)) + [vmem] * 3
    if last:
        out_shape.append(jax.ShapeDtypeStruct((8, batch), jnp.float32))
        out_specs.append(vmem)
    cfg = (n_dev, shard, base, widths, first, last)
    res = pl.pallas_call(
        functools.partial(_logits_kernel, cfg),
        in_specs=[hbm] * 4 + ([] if first else [vmem] * 3),
        out_specs=out_specs,
        out_shape=out_shape,
        scratch_shapes=[
            pltpu.VMEM((batch, depth), jnp.bfloat16),
            pltpu.VMEM((SLOTS, depth, UNIT), jnp.bfloat16),
            pltpu.VMEM((2, batch, UNIT), jnp.float32),
            pltpu.VMEM((1, batch), jnp.float32),
            pltpu.VMEM((1, batch), jnp.int32),
            pltpu.VMEM((batch, LANES), jnp.float32),
            pltpu.VMEM((batch, LANES), jnp.int32),
            pltpu.VMEM((batch, LANES), jnp.float32),
            pltpu.SemaphoreType.DMA((n_dev,)),
            pltpu.SemaphoreType.DMA((SLOTS, UNIT // HALF)),
            pltpu.SemaphoreType.DMA((2, n_dev)),
            pltpu.SemaphoreType.DMA((2,)),
        ],
        compiler_params=pltpu.CompilerParams(vmem_limit_bytes=32 * 2**20),
        cost_estimate=pl.CostEstimate(
            flops=2 * batch * depth * cols,
            bytes_accessed=2 * depth * (cols + batch),
            transcendentals=batch * cols,
        ),
        name="logits",
    )(*(pltpu.with_memory_space_constraint(a, pltpu.HBM) for a in (x, w, invt, tgt)), *(() if first else stats))
    k = n_dev * len(widths)
    blocks = [res[c * n_dev:(c + 1) * n_dev] for c in range(len(widths))]
    return blocks, res[k:k + 3], (res[k + 3] if last else None)


def _merge_kernel(n_dev, *refs):
    stats, (params_ref, at_ref) = refs[:n_dev], refs[n_dev:]
    me = lax.axis_index("vp")
    batch = stats[0].shape[1]
    rows = batch // n_dev
    ms = [s[0:1, :] for s in stats]
    top = functools.reduce(jnp.maximum, ms)
    keep = [jnp.exp(m - top) for m in ms]
    mass = [s[1:2, :] * k for s, k in zip(stats, keep)]
    upto = sum(s[2:3, :] * k for s, k in zip(stats, keep))
    total = sum(mass)
    at_ref[...] = upto / total
    values = [top, 1.0 / total]
    for p in range(n_dev):
        start = jnp.zeros_like(total)
        for q in range(n_dev):
            start += jnp.where((me ^ q) < (me ^ p), mass[q], 0.0)
        values.append(start)
    which = lax.broadcasted_iota(jnp.int32, (LANES, batch), 0)
    table = jnp.zeros((LANES, batch), jnp.float32)
    for i, v in enumerate(values):
        table = jnp.where(which == i, v, table)
    per_row = jnp.transpose(table)
    out = jnp.zeros((rows, LANES), jnp.float32)
    for d in range(n_dev):
        out = jnp.where(me == d, per_row[d * rows:(d + 1) * rows, :], out)
    params_ref[...] = out


def _merge(stats):
    n_dev = len(stats)
    batch = stats[0].shape[1]
    vmem = pl.BlockSpec(memory_space=pltpu.VMEM)
    return pl.pallas_call(
        functools.partial(_merge_kernel, n_dev),
        in_specs=[vmem] * n_dev,
        out_specs=[vmem] * 2,
        out_shape=[
            jax.ShapeDtypeStruct((batch // n_dev, LANES), jnp.float32),
            jax.ShapeDtypeStruct((1, batch), jnp.float32),
        ],
        cost_estimate=pl.CostEstimate(flops=100_000, bytes_accessed=100_000, transcendentals=1000),
        name="merge",
    )(*stats)


def _cdf_kernel(cfg, *refs):
    peers, shard, base, width, first = cfg
    n = len(peers)
    params_ref = refs[n]
    out_ref, params_out, y_ref, sems = refs[n + (1 if first else 2):]
    me = lax.axis_index("vp")
    rows = params_ref.shape[0]
    params = params_ref[...]
    top = jnp.broadcast_to(params[:, 0:1], (rows, LANES))
    inv = jnp.broadcast_to(params[:, 1:2], (rows, LANES))
    k_id = lax.broadcasted_iota(jnp.int32, (3 * LANES, 2 * LANES), 0) % LANES
    n_id = lax.broadcasted_iota(jnp.int32, (3 * LANES, 2 * LANES), 1)
    tri = jnp.where(k_id <= n_id, 1.0, 0.0).astype(jnp.bfloat16)
    lane = lax.broadcasted_iota(jnp.int32, (rows, LANES), 1)

    def unit(col, wide, carries):
        ends = []
        for j in range(n):
            cols = [pl.ds(col + t, LANES) for t in range(0, wide, LANES)]
            e = jnp.concatenate([jnp.exp(refs[j][:, c] - top) for c in cols], axis=0)
            hi = e.astype(jnp.bfloat16)
            r1 = e - hi.astype(jnp.float32)
            mid = r1.astype(jnp.bfloat16)
            lo = (r1 - mid.astype(jnp.float32)).astype(jnp.bfloat16)
            sums = jnp.dot(jnp.concatenate([hi, mid, lo], axis=1), tri, preferred_element_type=jnp.float32)
            carry = carries[j]
            for t, c in enumerate(cols):
                block = slice(t * rows, (t + 1) * rows)
                y_ref[j, :, c] = (sums[block, :LANES] + carry) * inv
                carry = carry + sums[block, LANES:]
            ends.append(carry)
        return tuple(ends)

    carries = tuple(jnp.broadcast_to(params[:, 2 + p:3 + p], (rows, LANES)) for p in peers)
    n_full = width // UNIT
    if n_full:
        carries = lax.fori_loop(
            0, n_full, lambda u, c: unit(pl.multiple_of(u * UNIT, UNIT), UNIT, c), carries
        )
    if width % UNIT:
        carries = unit(n_full * UNIT, width % UNIT, carries)
    copies = []
    updated = params
    for j, p in enumerate(peers):
        where = pl.multiple_of((me ^ p) * shard + base, LANES)
        copy = pltpu.make_async_copy(y_ref.at[j], out_ref.at[:, pl.ds(where, width)], sems.at[j])
        copy.start()
        copies.append(copy)
        updated = jnp.where(lane == 2 + p, carries[j], updated)
    params_out[...] = updated
    for copy in copies:
        copy.wait()


def _cdf(blocks, peers, params, out, n_dev, shard, base):
    rows, width = blocks[0].shape
    n = len(peers)
    first = out is None
    vmem = pl.BlockSpec(memory_space=pltpu.VMEM)
    hbm = pl.BlockSpec(memory_space=pl.ANY)
    return pl.pallas_call(
        functools.partial(_cdf_kernel, (peers, shard, base, width, first)),
        in_specs=[vmem] * (n + 1) + ([] if first else [hbm]),
        out_specs=[hbm, vmem],
        out_shape=[
            jax.ShapeDtypeStruct((rows, n_dev * shard), jnp.float32),
            jax.ShapeDtypeStruct(params.shape, jnp.float32),
        ],
        scratch_shapes=[
            pltpu.VMEM((n, rows, width), jnp.float32),
            pltpu.SemaphoreType.DMA((n,)),
        ],
        input_output_aliases={} if first else {n + 1: 0},
        compiler_params=pltpu.CompilerParams(vmem_limit_bytes=24 * 2**20),
        cost_estimate=pl.CostEstimate(
            flops=n * 2 * rows * width * 384,
            bytes_accessed=n * rows * width * 8,
            transcendentals=n * rows * width,
        ),
        name="cdf",
    )(*blocks, params, *(() if first else (out,)))


def solution(mesh):
    n_dev = mesh.shape["vp"]

    def swap(a, p):
        return lax.ppermute(a, "vp", [(i, i ^ p) for i in range(n_dev)])

    def local_step(hidden, w_local, inv_temp, target_ids):
        shard = w_local.shape[1]
        invt = inv_temp.reshape(1, -1)
        tgt = target_ids.reshape(1, -1)
        starts = [sum(CHUNKS[:k]) for k in range(len(CHUNKS))]
        stats, chunks = None, []
        groups = [[k] for k in range(EARLY)] + [list(range(EARLY, len(CHUNKS)))]
        for g, group in enumerate(groups):
            blocks, stats, packed = _logits(
                hidden, w_local, invt, tgt, stats, n_dev, starts[group[0]],
                tuple(CHUNKS[k] for k in group), g == len(groups) - 1,
            )
            for k, sent in zip(group, blocks):
                got = [sent[0]]
                for p in range(1, n_dev):
                    got.append(swap(sent[p], p))
                chunks.append(got)
        packs = [packed]
        for p in range(1, n_dev):
            packs.append(swap(packed, p))
        params, at_target = _merge(packs)
        out = None
        for peers in ((0, 1), (2, 3)):
            for k, got in enumerate(chunks):
                out, params = _cdf([got[p] for p in peers], peers, params, out, n_dev, shard, starts[k])
        return out, at_target.reshape(-1)

    return jax.shard_map(
        local_step,
        mesh=mesh,
        in_specs=(P("dp", None), P(None, "vp"), P("dp"), P("dp")),
        out_specs=(P(("dp", "vp"), None), P("dp")),
        check_vma=False,
    )
```

```python
import functools

import jax
import jax.numpy as jnp
from jax import lax
from jax.experimental import pallas as pl
from jax.experimental.pallas import tpu as pltpu
from jax.sharding import PartitionSpec as P


LANES = 128
UNIT = 512
HALF = 256
DEPTH = 512
SLOTS = 6
EARLY = ((512, 2), (1024, 1), (2048, 2))
LATE = (4096, 2048, 2048, 1024, 640)
LATE_UNITS = ((2048, 2), (2048, 1), (2048, 1), (1024, 1), (640, 1))


def _to_rows(vec_1xn):
    n = vec_1xn.shape[1]
    return jnp.transpose(jnp.broadcast_to(vec_1xn, (LANES, n)))


def _peer(me, p):
    return [me, me + 1 - 2 * lax.rem(me, 2), lax.rem(me + 2, 4), 3 - me][p]


def _logits_kernel(cfg, x_ref, w_ref, invt_ref, tgt_ref, *refs):
    n_dev, shard, segments, n_late = cfg
    refs = list(refs)

    def take(n):
        out = refs[:n]
        del refs[:n]
        return out

    early = take(n_dev)
    late = [take(n_dev) for _ in range(n_late)]
    packs = take(n_dev)
    xs, wbuf, acc, zsend, zbuf, invt_v, tgt_v, pack_v = take(8)
    scale_rows, left_rows, tmp, m_ref, s_ref, t_ref = take(6)
    w_sem, z_sem, x_sem, v_sem, own_sem, send_sem, recv_sem, pack_send, pack_recv = take(9)
    me = lax.axis_index("vp")
    batch, depth = xs.shape
    rows = batch // n_dev
    k_steps = depth // DEPTH

    def rows_of(p):
        return pl.ds(pl.multiple_of(_peer(me, p) * rows, rows), rows)

    def fetch_w(seg, step):
        width, col0, g0 = segments[seg][0], segments[seg][3], segments[seg][4]
        slot = lax.rem(g0 + step, SLOTS)
        col = col0 + lax.div(step, k_steps) * width
        row = pl.multiple_of(lax.rem(step, k_steps) * DEPTH, DEPTH)
        return pltpu.make_async_copy(
            w_ref.at[pl.ds(row, DEPTH), pl.ds(pl.multiple_of(col, LANES), width)],
            wbuf.at[slot, :, pl.ds(0, width)],
            w_sem.at[slot],
        )

    def put_late(slot, c, off, width):
        return [
            pltpu.make_async_copy(
                zbuf.at[slot, pl.ds(p * rows, rows), pl.ds(0, width)],
                late[c][p].at[:, pl.ds(off, width)],
                z_sem.at[slot, p],
            )
            for p in range(n_dev)
        ]

    def put_own(u, off, width):
        return pltpu.make_async_copy(
            zsend.at[pl.ds(0, rows), pl.ds(off, width)], early[0].at[:, pl.ds(off, width)], own_sem.at[u]
        )

    def send(u, p, off, width):
        return pltpu.make_async_remote_copy(
            src_ref=zsend.at[pl.ds(p * rows, rows), pl.ds(off, width)],
            dst_ref=early[p].at[:, pl.ds(off, width)],
            send_sem=send_sem.at[u, p],
            recv_sem=recv_sem.at[u, p],
            device_id={"vp": _peer(me, p)},
            device_id_type=pl.DeviceIdType.MESH,
        )

    x_copies = [
        pltpu.make_async_copy(x_ref.at[rows_of(p), :], xs.at[pl.ds(p * rows, rows), :], x_sem.at[p])
        for p in range(n_dev)
    ]
    small = [
        pltpu.make_async_copy(invt_ref, invt_v, v_sem.at[0]),
        pltpu.make_async_copy(tgt_ref, tgt_v, v_sem.at[1]),
    ]
    for copy in small + x_copies:
        copy.start()
    for i in range(SLOTS - 1):
        fetch_w(0, jnp.int32(i)).start()
    barrier = pltpu.get_barrier_semaphore()
    for p in range(1, n_dev):
        pl.semaphore_signal(
            barrier, inc=1, device_id={"vp": _peer(me, p)}, device_id_type=pl.DeviceIdType.MESH
        )
    m_ref[...] = jnp.full(m_ref.shape, -jnp.inf, jnp.float32)
    s_ref[...] = jnp.zeros_like(s_ref)
    t_ref[...] = jnp.zeros_like(t_ref)
    for copy in small:
        copy.wait()
    tmp[...] = _to_rows(invt_v[...])
    for p in range(n_dev):
        scale_rows[pl.ds(p * rows, rows), :] = tmp[rows_of(p), :]
    tmp[...] = _to_rows(tgt_v[...].astype(jnp.float32))
    lane = lax.broadcasted_iota(jnp.int32, (rows, LANES), 1)
    for p in range(n_dev):
        left_rows[pl.ds(p * rows, rows), :] = tmp[rows_of(p), :].astype(jnp.int32) - me * shard - lane
    for copy in x_copies:
        copy.wait()

    def multiply(seg, step):
        width = segments[seg][0]
        slot, k = lax.rem(segments[seg][4] + step, SLOTS), lax.rem(step, k_steps)
        fetch_w(seg, step).wait()
        x = xs[:, pl.ds(pl.multiple_of(k * DEPTH, DEPTH), DEPTH)]
        for off in range(0, width, HALF):
            wide = min(HALF, width - off)
            part = jnp.dot(x, wbuf[slot, :, off:off + wide], preferred_element_type=jnp.float32)
            acc[:, off:off + wide] = part + jnp.where(k == 0, 0.0, acc[:, off:off + wide])

    def finish(col, width, out_ref, out_off):
        group = 32
        span = UNIT if width % UNIT == 0 else LANES

        def some(j, _):
            at = pl.multiple_of(j * span, span)
            for r in range(0, batch, group):
                block = slice(r, r + group)
                scale = scale_rows[block, :]
                tiles = []
                for t in range(0, span, LANES):
                    tile = acc[block, pl.ds(at + t, LANES)] * scale
                    out_ref[block, pl.ds(pl.multiple_of(out_off + at + t, LANES), LANES)] = tile
                    tiles.append(tile)
                m_old = m_ref[block, :]
                m_new = functools.reduce(jnp.maximum, tiles, m_old)
                keep = jnp.exp(m_old - m_new)
                total = s_ref[block, :] * keep
                upto = t_ref[block, :] * keep
                left = left_rows[block, :]
                for t, tile in enumerate(tiles):
                    e = jnp.exp(tile - m_new)
                    total += e
                    upto += jnp.where(left >= col + at + t * LANES, e, 0.0)
                m_ref[block, :] = m_new
                s_ref[block, :] = total
                t_ref[block, :] = upto
            return 0

        lax.fori_loop(0, width // span, some, 0)

    sent, own, stored = [], [], []
    for seg, (width, n, chunk, col0, g0) in enumerate(segments):
        for i in range(n):

            def body(k, _, seg=seg, i=i, n=n):
                step = i * k_steps + k
                ahead = step + SLOTS - 1

                @pl.when(ahead < n * k_steps)
                def _():
                    fetch_w(seg, ahead).start()

                if seg + 1 < len(segments):
                    @pl.when(ahead >= n * k_steps)
                    def _():
                        fetch_w(seg + 1, ahead - n * k_steps).start()

                multiply(seg, step)
                return 0

            lax.fori_loop(0, k_steps, body, 0)
            col = col0 + i * width
            if chunk is None:
                finish(col, width, zsend, col)
                if not sent:
                    pl.semaphore_wait(barrier, n_dev - 1)
                u = len(own)
                for p in (2, 3, 1):
                    copy = send(u, p, col, width)
                    copy.start()
                    sent.append(copy)
                copy = put_own(u, col, width)
                copy.start()
                own.append(copy)
            else:
                slot = len(stored) % 2
                if len(stored) >= 2:
                    for copy in stored[-2]:
                        copy.wait()
                finish(col, width, zbuf.at[slot], 0)
                c, off = chunk
                copies = put_late(slot, c, off + i * width, width)
                for copy in copies:
                    copy.start()
                stored.append(copies)
    m = m_ref[...]
    m_row = jnp.max(m, axis=1, keepdims=True)
    keep = jnp.exp(m - m_row)
    s_row = jnp.sum(s_ref[...] * keep, axis=1, keepdims=True)
    t_row = jnp.sum(t_ref[...] * keep, axis=1, keepdims=True)
    which = lax.broadcasted_iota(jnp.int32, m.shape, 1)
    packed = jnp.where(which == 0, m_row, jnp.where(which == 1, s_row, t_row))
    for p in range(n_dev):
        tmp[rows_of(p), :] = packed[p * rows:(p + 1) * rows, :]
    pack_v[...] = jnp.transpose(tmp[...])[:8, :]
    for p in (2, 3, 1):
        copy = pltpu.make_async_remote_copy(
            src_ref=pack_v,
            dst_ref=packs[p],
            send_sem=pack_send.at[p],
            recv_sem=pack_recv.at[p],
            device_id={"vp": _peer(me, p)},
            device_id_type=pl.DeviceIdType.MESH,
        )
        copy.start()
        sent.append(copy)
    copy = pltpu.make_async_copy(pack_v, packs[0], pack_send.at[0])
    copy.start()
    own.append(copy)
    for copies in stored[-2:]:
        for copy in copies:
            copy.wait()
    for copy in own + sent:
        copy.wait()


def _logits(x, w, invt, tgt, n_dev):
    batch, depth = x.shape
    shard = w.shape[1]
    rows = batch // n_dev
    segments, col, g0 = [], 0, 0
    chunk_of = {}
    begin = sum(width * n for width, n in EARLY)
    for c, width in enumerate(LATE):
        chunk_of.update({begin + i: (c, i) for i in range(0, width, LANES)})
        begin += width
    for i, (width, n) in enumerate(EARLY + LATE_UNITS):
        segments.append((width, n, None if i < len(EARLY) else chunk_of[col], col, g0))
        col += width * n
        g0 += n * (depth // DEPTH)
    assert col == shard == begin
    n_early = sum(n for _, n in EARLY)
    sent = sum(width * n for width, n in EARLY)
    hbm = pl.BlockSpec(memory_space=pltpu.HBM)
    out_shape = [pltpu.HBM((rows, sent), jnp.float32)] * n_dev
    out_shape += [pltpu.HBM((rows, width), jnp.float32) for width in LATE for _ in range(n_dev)]
    out_shape += [pltpu.HBM((8, batch), jnp.float32)] * n_dev
    table = pltpu.VMEM((batch, LANES), jnp.float32)
    widest = max(width for width, _ in EARLY + LATE_UNITS)
    dma = pltpu.SemaphoreType.DMA
    res = pl.pallas_call(
        functools.partial(_logits_kernel, (n_dev, shard, segments, len(LATE))),
        in_specs=[hbm] * 4,
        out_specs=[hbm] * len(out_shape),
        out_shape=out_shape,
        scratch_shapes=[
            pltpu.VMEM((batch, depth), jnp.bfloat16),
            pltpu.VMEM((SLOTS, DEPTH, widest), jnp.bfloat16),
            pltpu.VMEM((batch, widest), jnp.float32),
            pltpu.VMEM((batch, sent), jnp.float32),
            pltpu.VMEM((2, batch, widest), jnp.float32),
            pltpu.VMEM((1, batch), jnp.float32),
            pltpu.VMEM((1, batch), jnp.int32),
            pltpu.VMEM((8, batch), jnp.float32),
            table,
            pltpu.VMEM((batch, LANES), jnp.int32),
            table,
            table,
            table,
            table,
            dma((SLOTS,)),
            dma((2, n_dev)),
            dma((n_dev,)),
            dma((2,)),
            dma((n_early,)),
            dma((n_early, n_dev)),
            dma((n_early, n_dev)),
            dma((n_dev,)),
            dma((n_dev,)),
        ],
        compiler_params=pltpu.CompilerParams(
            collective_id=0, has_side_effects=True, vmem_limit_bytes=40 * 2**20
        ),
        cost_estimate=pl.CostEstimate(
            flops=2 * batch * depth * shard,
            bytes_accessed=2 * depth * shard,
            transcendentals=batch * shard,
        ),
        name="logits",
    )(*(pltpu.with_memory_space_constraint(a, pltpu.HBM) for a in (x, w, invt, tgt)))
    blocks = [res[c * n_dev:(c + 1) * n_dev] for c in range(len(LATE) + 2)]
    return blocks[0], blocks[1:-1], blocks[-1]


def _merge_kernel(n_dev, *refs):
    stats, (params_ref, at_ref) = refs[:n_dev], refs[n_dev:]
    me = lax.axis_index("vp")
    batch = stats[0].shape[1]
    rows = batch // n_dev
    ms = [s[0:1, :] for s in stats]
    top = functools.reduce(jnp.maximum, ms)
    keep = [jnp.exp(m - top) for m in ms]
    mass = [s[1:2, :] * k for s, k in zip(stats, keep)]
    upto = sum(s[2:3, :] * k for s, k in zip(stats, keep))
    total = sum(mass)
    at_ref[...] = upto / total
    values = [top, 1.0 / total]
    for p in range(n_dev):
        start = jnp.zeros_like(total)
        for q in range(n_dev):
            start += jnp.where((me ^ q) < (me ^ p), mass[q], 0.0)
        values.append(start)
    which = lax.broadcasted_iota(jnp.int32, (LANES, batch), 0)
    table = jnp.zeros((LANES, batch), jnp.float32)
    for i, v in enumerate(values):
        table = jnp.where(which == i, v, table)
    per_row = jnp.transpose(table)
    out = jnp.zeros((rows, LANES), jnp.float32)
    for d in range(n_dev):
        out = jnp.where(me == d, per_row[d * rows:(d + 1) * rows, :], out)
    params_ref[...] = out


def _merge(stats):
    n_dev = len(stats)
    batch = stats[0].shape[1]
    vmem = pl.BlockSpec(memory_space=pltpu.VMEM)
    return pl.pallas_call(
        functools.partial(_merge_kernel, n_dev),
        in_specs=[vmem] * n_dev,
        out_specs=[vmem] * 2,
        out_shape=[
            jax.ShapeDtypeStruct((batch // n_dev, LANES), jnp.float32),
            jax.ShapeDtypeStruct((1, batch), jnp.float32),
        ],
        cost_estimate=pl.CostEstimate(flops=100_000, bytes_accessed=100_000, transcendentals=1000),
        name="merge",
    )(*stats)


def _cdf_kernel(cfg, *refs):
    peers, shard, base, width, first = cfg
    n = len(peers)
    params_ref = refs[n]
    out_ref, params_out, y_ref, sems = refs[n + (1 if first else 2):]
    me = lax.axis_index("vp")
    rows = params_ref.shape[0]
    params = params_ref[...]
    top = jnp.broadcast_to(params[:, 0:1], (rows, LANES))
    inv = jnp.broadcast_to(params[:, 1:2], (rows, LANES))
    k_id = lax.broadcasted_iota(jnp.int32, (3 * LANES, 2 * LANES), 0) % LANES
    n_id = lax.broadcasted_iota(jnp.int32, (3 * LANES, 2 * LANES), 1)
    tri = jnp.where(k_id <= n_id, 1.0, 0.0).astype(jnp.bfloat16)
    lane = lax.broadcasted_iota(jnp.int32, (rows, LANES), 1)

    def unit(col, wide, carries):
        ends = []
        for j in range(n):
            cols = [pl.ds(col + t, LANES) for t in range(0, wide, LANES)]
            e = jnp.concatenate([jnp.exp(refs[j][:, c] - top) for c in cols], axis=0)
            hi = e.astype(jnp.bfloat16)
            r1 = e - hi.astype(jnp.float32)
            mid = r1.astype(jnp.bfloat16)
            lo = (r1 - mid.astype(jnp.float32)).astype(jnp.bfloat16)
            sums = jnp.dot(jnp.concatenate([hi, mid, lo], axis=1), tri, preferred_element_type=jnp.float32)
            carry = carries[j]
            for t, c in enumerate(cols):
                block = slice(t * rows, (t + 1) * rows)
                y_ref[j, :, c] = (sums[block, :LANES] + carry) * inv
                carry = carry + sums[block, LANES:]
            ends.append(carry)
        return tuple(ends)

    carries = tuple(jnp.broadcast_to(params[:, 2 + p:3 + p], (rows, LANES)) for p in peers)
    n_full = width // UNIT
    if n_full:
        carries = lax.fori_loop(
            0, n_full, lambda u, c: unit(pl.multiple_of(u * UNIT, UNIT), UNIT, c), carries
        )
    if width % UNIT:
        carries = unit(n_full * UNIT, width % UNIT, carries)
    copies = []
    updated = params
    for j, p in enumerate(peers):
        where = pl.multiple_of((me ^ p) * shard + base, LANES)
        copy = pltpu.make_async_copy(y_ref.at[j], out_ref.at[:, pl.ds(where, width)], sems.at[j])
        copy.start()
        copies.append(copy)
        updated = jnp.where(lane == 2 + p, carries[j], updated)
    params_out[...] = updated
    for copy in copies:
        copy.wait()


def _cdf(blocks, peers, params, out, n_dev, shard, base):
    rows, width = blocks[0].shape
    n = len(peers)
    first = out is None
    vmem = pl.BlockSpec(memory_space=pltpu.VMEM)
    hbm = pl.BlockSpec(memory_space=pl.ANY)
    return pl.pallas_call(
        functools.partial(_cdf_kernel, (peers, shard, base, width, first)),
        in_specs=[vmem] * (n + 1) + ([] if first else [hbm]),
        out_specs=[hbm, vmem],
        out_shape=[
            jax.ShapeDtypeStruct((rows, n_dev * shard), jnp.float32),
            jax.ShapeDtypeStruct(params.shape, jnp.float32),
        ],
        scratch_shapes=[
            pltpu.VMEM((n, rows, width), jnp.float32),
            pltpu.SemaphoreType.DMA((n,)),
        ],
        input_output_aliases={} if first else {n + 1: 0},
        compiler_params=pltpu.CompilerParams(vmem_limit_bytes=24 * 2**20),
        cost_estimate=pl.CostEstimate(
            flops=n * 2 * rows * width * 384,
            bytes_accessed=n * rows * width * 8,
            transcendentals=n * rows * width,
        ),
        name="cdf",
    )(*blocks, params, *(() if first else (out,)))


def solution(mesh):
    n_dev = mesh.shape["vp"]
    assert n_dev == 4

    def swap(a, p):
        return lax.ppermute(a, "vp", [(i, i ^ p) for i in range(n_dev)])

    def local_step(hidden, w_local, inv_temp, target_ids):
        shard = w_local.shape[1]
        early, late, packs = _logits(
            hidden, w_local, inv_temp.reshape(1, -1), target_ids.reshape(1, -1), n_dev
        )
        chunks = [(0, early)]
        begin = early[0].shape[1]
        for made in late:
            got = [made[0]]
            for p in range(1, n_dev):
                got.append(swap(made[p], p))
            chunks.append((begin, got))
            begin += made[0].shape[1]
        params, at_target = _merge(packs)
        out = None
        for peers in ((0, 1), (2, 3)):
            for begin, got in chunks:
                out, params = _cdf([got[p] for p in peers], peers, params, out, n_dev, shard, begin)
        return out, at_target.reshape(-1)

    return jax.shard_map(
        local_step,
        mesh=mesh,
        in_specs=(P("dp", None), P(None, "vp"), P("dp"), P("dp")),
        out_specs=(P(("dp", "vp"), None), P("dp")),
        check_vma=False,
    )
```

```python
import functools

import jax
import jax.numpy as jnp
from jax import lax
from jax.experimental import pallas as pl
from jax.experimental.pallas import tpu as pltpu
from jax.sharding import PartitionSpec as P


LANES = 128
UNIT = 512
HALF = 256
DEPTH = 512
SLOTS = 9
EARLY = ((256, 2), (512, 1), (1024, 1), (2048, 3))
LATE = (4096, 2048, 1024, 640)
LATE_UNITS = ((2048, 2), (2048, 1), (1024, 1), (640, 1))


def _to_rows(vec_1xn):
    n = vec_1xn.shape[1]
    return jnp.transpose(jnp.broadcast_to(vec_1xn, (LANES, n)))


def _peer(me, p):
    return [me, me + 1 - 2 * lax.rem(me, 2), lax.rem(me + 2, 4), 3 - me][p]


def _logits_kernel(cfg, x_ref, w_ref, invt_ref, tgt_ref, *refs):
    n_dev, shard, segments, n_late = cfg
    refs = list(refs)

    def take(n):
        out = refs[:n]
        del refs[:n]
        return out

    early = take(n_dev)
    late = [take(n_dev) for _ in range(n_late)]
    packs = take(n_dev)
    xs, wbuf, acc, zsend, zbuf, invt_v, tgt_v, pack_v = take(8)
    scale_rows, left_rows, tmp, m_ref, s_ref, t_ref = take(6)
    w_sem, z_sem, x_sem, v_sem, own_sem, send_sem, recv_sem, pack_send, pack_recv = take(9)
    me = lax.axis_index("vp")
    batch, depth = xs.shape
    rows = batch // n_dev
    k_steps = depth // DEPTH

    def rows_of(p):
        return pl.ds(pl.multiple_of(_peer(me, p) * rows, rows), rows)

    def fetch_w(seg, step):
        width, col0, g0 = segments[seg][0], segments[seg][3], segments[seg][4]
        slot = lax.rem(g0 + step, SLOTS)
        col = col0 + lax.div(step, k_steps) * width
        row = pl.multiple_of(lax.rem(step, k_steps) * DEPTH, DEPTH)
        return pltpu.make_async_copy(
            w_ref.at[pl.ds(row, DEPTH), pl.ds(pl.multiple_of(col, LANES), width)],
            wbuf.at[slot, :, pl.ds(0, width)],
            w_sem.at[slot],
        )

    def put_late(slot, c, off, width):
        return [
            pltpu.make_async_copy(
                zbuf.at[slot, pl.ds(p * rows, rows), pl.ds(0, width)],
                late[c][p].at[:, pl.ds(off, width)],
                z_sem.at[slot, p],
            )
            for p in range(n_dev)
        ]

    def put_own(u, off, width):
        return pltpu.make_async_copy(
            zsend.at[pl.ds(0, rows), pl.ds(off, width)], early[0].at[:, pl.ds(off, width)], own_sem.at[u]
        )

    def send(u, p, off, width):
        return pltpu.make_async_remote_copy(
            src_ref=zsend.at[pl.ds(p * rows, rows), pl.ds(off, width)],
            dst_ref=early[p].at[:, pl.ds(off, width)],
            send_sem=send_sem.at[u, p],
            recv_sem=recv_sem.at[u, p],
            device_id={"vp": _peer(me, p)},
            device_id_type=pl.DeviceIdType.MESH,
        )

    x_copies = [
        pltpu.make_async_copy(x_ref.at[rows_of(p), :], xs.at[pl.ds(p * rows, rows), :], x_sem.at[p])
        for p in range(n_dev)
    ]
    small = [
        pltpu.make_async_copy(invt_ref, invt_v, v_sem.at[0]),
        pltpu.make_async_copy(tgt_ref, tgt_v, v_sem.at[1]),
    ]
    for copy in small + x_copies:
        copy.start()
    for i in range(SLOTS - 1):
        fetch_w(0, jnp.int32(i)).start()
    barrier = pltpu.get_barrier_semaphore()
    for p in range(1, n_dev):
        pl.semaphore_signal(
            barrier, inc=1, device_id={"vp": _peer(me, p)}, device_id_type=pl.DeviceIdType.MESH
        )
    m_ref[...] = jnp.full(m_ref.shape, -jnp.inf, jnp.float32)
    s_ref[...] = jnp.zeros_like(s_ref)
    t_ref[...] = jnp.zeros_like(t_ref)
    for copy in small:
        copy.wait()
    tmp[...] = _to_rows(invt_v[...])
    for p in range(n_dev):
        scale_rows[pl.ds(p * rows, rows), :] = tmp[rows_of(p), :]
    tmp[...] = _to_rows(tgt_v[...].astype(jnp.float32))
    lane = lax.broadcasted_iota(jnp.int32, (rows, LANES), 1)
    for p in range(n_dev):
        left_rows[pl.ds(p * rows, rows), :] = tmp[rows_of(p), :].astype(jnp.int32) - me * shard - lane
    for copy in x_copies:
        copy.wait()

    def multiply(seg, step):
        width = segments[seg][0]
        slot, k = lax.rem(segments[seg][4] + step, SLOTS), lax.rem(step, k_steps)
        fetch_w(seg, step).wait()
        x = xs[:, pl.ds(pl.multiple_of(k * DEPTH, DEPTH), DEPTH)]
        for off in range(0, width, HALF):
            wide = min(HALF, width - off)
            part = jnp.dot(x, wbuf[slot, :, off:off + wide], preferred_element_type=jnp.float32)
            acc[:, off:off + wide] = part + jnp.where(k == 0, 0.0, acc[:, off:off + wide])

    def finish(col, width, out_ref, out_off):
        group = 32
        span = next(n for n in (UNIT, HALF, LANES) if width % n == 0)

        def some(j, _):
            at = pl.multiple_of(j * span, span)
            for r in range(0, batch, group):
                block = slice(r, r + group)
                scale = scale_rows[block, :]
                tiles = []
                for t in range(0, span, LANES):
                    tile = acc[block, pl.ds(at + t, LANES)] * scale
                    out_ref[block, pl.ds(pl.multiple_of(out_off + at + t, LANES), LANES)] = tile
                    tiles.append(tile)
                m_old = m_ref[block, :]
                m_new = functools.reduce(jnp.maximum, tiles, m_old)
                keep = jnp.exp(m_old - m_new)
                total = s_ref[block, :] * keep
                upto = t_ref[block, :] * keep
                left = left_rows[block, :]
                for t, tile in enumerate(tiles):
                    e = jnp.exp(tile - m_new)
                    total += e
                    upto += jnp.where(left >= col + at + t * LANES, e, 0.0)
                m_ref[block, :] = m_new
                s_ref[block, :] = total
                t_ref[block, :] = upto
            return 0

        lax.fori_loop(0, width // span, some, 0)

    sent, own, stored = [], [], []
    for seg, (width, n, chunk, col0, g0) in enumerate(segments):
        for i in range(n):

            def body(k, _, seg=seg, i=i, n=n):
                step = i * k_steps + k
                ahead = step + SLOTS - 1

                @pl.when(ahead < n * k_steps)
                def _():
                    fetch_w(seg, ahead).start()

                if seg + 1 < len(segments):
                    @pl.when(ahead >= n * k_steps)
                    def _():
                        fetch_w(seg + 1, ahead - n * k_steps).start()

                multiply(seg, step)
                return 0

            lax.fori_loop(0, k_steps, body, 0)
            col = col0 + i * width
            if chunk is None:
                finish(col, width, zsend, col)
                if not sent:
                    pl.semaphore_wait(barrier, n_dev - 1)
                u = len(own)
                for p in (2, 3, 1):
                    copy = send(u, p, col, width)
                    copy.start()
                    sent.append(copy)
                copy = put_own(u, col, width)
                copy.start()
                own.append(copy)
            else:
                slot = len(stored) % 2
                if len(stored) >= 2:
                    for copy in stored[-2]:
                        copy.wait()
                finish(col, width, zbuf.at[slot], 0)
                c, off = chunk
                copies = put_late(slot, c, off + i * width, width)
                for copy in copies:
                    copy.start()
                stored.append(copies)
    m = m_ref[...]
    m_row = jnp.max(m, axis=1, keepdims=True)
    keep = jnp.exp(m - m_row)
    s_row = jnp.sum(s_ref[...] * keep, axis=1, keepdims=True)
    t_row = jnp.sum(t_ref[...] * keep, axis=1, keepdims=True)
    which = lax.broadcasted_iota(jnp.int32, m.shape, 1)
    packed = jnp.where(which == 0, m_row, jnp.where(which == 1, s_row, t_row))
    for p in range(n_dev):
        tmp[rows_of(p), :] = packed[p * rows:(p + 1) * rows, :]
    pack_v[...] = jnp.transpose(tmp[...])[:8, :]
    for p in (2, 3, 1):
        copy = pltpu.make_async_remote_copy(
            src_ref=pack_v,
            dst_ref=packs[p],
            send_sem=pack_send.at[p],
            recv_sem=pack_recv.at[p],
            device_id={"vp": _peer(me, p)},
            device_id_type=pl.DeviceIdType.MESH,
        )
        copy.start()
        sent.append(copy)
    copy = pltpu.make_async_copy(pack_v, packs[0], pack_send.at[0])
    copy.start()
    own.append(copy)
    for copies in stored[-2:]:
        for copy in copies:
            copy.wait()
    for copy in own + sent:
        copy.wait()


def _logits(x, w, invt, tgt, n_dev):
    batch, depth = x.shape
    shard = w.shape[1]
    rows = batch // n_dev
    segments, col, g0 = [], 0, 0
    chunk_of = {}
    begin = sum(width * n for width, n in EARLY)
    for c, width in enumerate(LATE):
        chunk_of.update({begin + i: (c, i) for i in range(0, width, LANES)})
        begin += width
    for i, (width, n) in enumerate(EARLY + LATE_UNITS):
        segments.append((width, n, None if i < len(EARLY) else chunk_of[col], col, g0))
        col += width * n
        g0 += n * (depth // DEPTH)
    assert col == shard == begin
    n_early = sum(n for _, n in EARLY)
    sent = sum(width * n for width, n in EARLY)
    hbm = pl.BlockSpec(memory_space=pltpu.HBM)
    out_shape = [pltpu.HBM((rows, sent), jnp.float32)] * n_dev
    out_shape += [pltpu.HBM((rows, width), jnp.float32) for width in LATE for _ in range(n_dev)]
    out_shape += [pltpu.HBM((8, batch), jnp.float32)] * n_dev
    table = pltpu.VMEM((batch, LANES), jnp.float32)
    widest = max(width for width, _ in EARLY + LATE_UNITS)
    dma = pltpu.SemaphoreType.DMA
    res = pl.pallas_call(
        functools.partial(_logits_kernel, (n_dev, shard, segments, len(LATE))),
        in_specs=[hbm] * 4,
        out_specs=[hbm] * len(out_shape),
        out_shape=out_shape,
        scratch_shapes=[
            pltpu.VMEM((batch, depth), jnp.bfloat16),
            pltpu.VMEM((SLOTS, DEPTH, widest), jnp.bfloat16),
            pltpu.VMEM((batch, widest), jnp.float32),
            pltpu.VMEM((batch, sent), jnp.float32),
            pltpu.VMEM((2, batch, widest), jnp.float32),
            pltpu.VMEM((1, batch), jnp.float32),
            pltpu.VMEM((1, batch), jnp.int32),
            pltpu.VMEM((8, batch), jnp.float32),
            table,
            pltpu.VMEM((batch, LANES), jnp.int32),
            table,
            table,
            table,
            table,
            dma((SLOTS,)),
            dma((2, n_dev)),
            dma((n_dev,)),
            dma((2,)),
            dma((n_early,)),
            dma((n_early, n_dev)),
            dma((n_early, n_dev)),
            dma((n_dev,)),
            dma((n_dev,)),
        ],
        compiler_params=pltpu.CompilerParams(
            collective_id=0, has_side_effects=True, vmem_limit_bytes=52 * 2**20
        ),
        cost_estimate=pl.CostEstimate(
            flops=2 * batch * depth * shard,
            bytes_accessed=2 * depth * shard,
            transcendentals=batch * shard,
        ),
        name="logits",
    )(*(pltpu.with_memory_space_constraint(a, pltpu.HBM) for a in (x, w, invt, tgt)))
    blocks = [res[c * n_dev:(c + 1) * n_dev] for c in range(len(LATE) + 2)]
    return blocks[0], blocks[1:-1], blocks[-1]


def _merge_kernel(n_dev, *refs):
    stats, (params_ref, at_ref) = refs[:n_dev], refs[n_dev:]
    me = lax.axis_index("vp")
    batch = stats[0].shape[1]
    rows = batch // n_dev
    ms = [s[0:1, :] for s in stats]
    top = functools.reduce(jnp.maximum, ms)
    keep = [jnp.exp(m - top) for m in ms]
    mass = [s[1:2, :] * k for s, k in zip(stats, keep)]
    upto = sum(s[2:3, :] * k for s, k in zip(stats, keep))
    total = sum(mass)
    at_ref[...] = upto / total
    values = [top, 1.0 / total]
    for p in range(n_dev):
        start = jnp.zeros_like(total)
        for q in range(n_dev):
            start += jnp.where((me ^ q) < (me ^ p), mass[q], 0.0)
        values.append(start)
    which = lax.broadcasted_iota(jnp.int32, (LANES, batch), 0)
    table = jnp.zeros((LANES, batch), jnp.float32)
    for i, v in enumerate(values):
        table = jnp.where(which == i, v, table)
    per_row = jnp.transpose(table)
    out = jnp.zeros((rows, LANES), jnp.float32)
    for d in range(n_dev):
        out = jnp.where(me == d, per_row[d * rows:(d + 1) * rows, :], out)
    params_ref[...] = out


def _merge(stats):
    n_dev = len(stats)
    batch = stats[0].shape[1]
    vmem = pl.BlockSpec(memory_space=pltpu.VMEM)
    return pl.pallas_call(
        functools.partial(_merge_kernel, n_dev),
        in_specs=[vmem] * n_dev,
        out_specs=[vmem] * 2,
        out_shape=[
            jax.ShapeDtypeStruct((batch // n_dev, LANES), jnp.float32),
            jax.ShapeDtypeStruct((1, batch), jnp.float32),
        ],
        cost_estimate=pl.CostEstimate(flops=100_000, bytes_accessed=100_000, transcendentals=1000),
        name="merge",
    )(*stats)


def _cdf_kernel(cfg, *refs):
    peers, shard, base, width, first = cfg
    n = len(peers)
    params_ref = refs[n]
    out_ref, params_out, y_ref, sems = refs[n + (1 if first else 2):]
    me = lax.axis_index("vp")
    rows = params_ref.shape[0]
    params = params_ref[...]
    top = jnp.broadcast_to(params[:, 0:1], (rows, LANES))
    inv = jnp.broadcast_to(params[:, 1:2], (rows, LANES))
    k_id = lax.broadcasted_iota(jnp.int32, (3 * LANES, 2 * LANES), 0) % LANES
    n_id = lax.broadcasted_iota(jnp.int32, (3 * LANES, 2 * LANES), 1)
    tri = jnp.where(k_id <= n_id, 1.0, 0.0).astype(jnp.bfloat16)
    lane = lax.broadcasted_iota(jnp.int32, (rows, LANES), 1)

    def unit(col, wide, carries):
        ends = []
        for j in range(n):
            cols = [pl.ds(col + t, LANES) for t in range(0, wide, LANES)]
            e = jnp.concatenate([jnp.exp(refs[j][:, c] - top) for c in cols], axis=0)
            hi = e.astype(jnp.bfloat16)
            r1 = e - hi.astype(jnp.float32)
            mid = r1.astype(jnp.bfloat16)
            lo = (r1 - mid.astype(jnp.float32)).astype(jnp.bfloat16)
            sums = jnp.dot(jnp.concatenate([hi, mid, lo], axis=1), tri, preferred_element_type=jnp.float32)
            carry = carries[j]
            for t, c in enumerate(cols):
                block = slice(t * rows, (t + 1) * rows)
                y_ref[j, :, c] = (sums[block, :LANES] + carry) * inv
                carry = carry + sums[block, LANES:]
            ends.append(carry)
        return tuple(ends)

    carries = tuple(jnp.broadcast_to(params[:, 2 + p:3 + p], (rows, LANES)) for p in peers)
    n_full = width // UNIT
    if n_full:
        carries = lax.fori_loop(
            0, n_full, lambda u, c: unit(pl.multiple_of(u * UNIT, UNIT), UNIT, c), carries
        )
    if width % UNIT:
        carries = unit(n_full * UNIT, width % UNIT, carries)
    copies = []
    updated = params
    for j, p in enumerate(peers):
        where = pl.multiple_of((me ^ p) * shard + base, LANES)
        copy = pltpu.make_async_copy(y_ref.at[j], out_ref.at[:, pl.ds(where, width)], sems.at[j])
        copy.start()
        copies.append(copy)
        updated = jnp.where(lane == 2 + p, carries[j], updated)
    params_out[...] = updated
    for copy in copies:
        copy.wait()


def _cdf(blocks, peers, params, out, n_dev, shard, base):
    rows, width = blocks[0].shape
    n = len(peers)
    first = out is None
    vmem = pl.BlockSpec(memory_space=pltpu.VMEM)
    hbm = pl.BlockSpec(memory_space=pl.ANY)
    return pl.pallas_call(
        functools.partial(_cdf_kernel, (peers, shard, base, width, first)),
        in_specs=[vmem] * (n + 1) + ([] if first else [hbm]),
        out_specs=[hbm, vmem],
        out_shape=[
            jax.ShapeDtypeStruct((rows, n_dev * shard), jnp.float32),
            jax.ShapeDtypeStruct(params.shape, jnp.float32),
        ],
        scratch_shapes=[
            pltpu.VMEM((n, rows, width), jnp.float32),
            pltpu.SemaphoreType.DMA((n,)),
        ],
        input_output_aliases={} if first else {n + 1: 0},
        compiler_params=pltpu.CompilerParams(vmem_limit_bytes=24 * 2**20),
        cost_estimate=pl.CostEstimate(
            flops=n * 2 * rows * width * 384,
            bytes_accessed=n * rows * width * 8,
            transcendentals=n * rows * width,
        ),
        name="cdf",
    )(*blocks, params, *(() if first else (out,)))


def solution(mesh):
    n_dev = mesh.shape["vp"]
    assert n_dev == 4

    def swap(a, p):
        return lax.ppermute(a, "vp", [(i, i ^ p) for i in range(n_dev)])

    def local_step(hidden, w_local, inv_temp, target_ids):
        shard = w_local.shape[1]
        early, late, packs = _logits(
            hidden, w_local, inv_temp.reshape(1, -1), target_ids.reshape(1, -1), n_dev
        )
        chunks = [(0, early)]
        begin = early[0].shape[1]
        for made in late:
            got = [made[0]]
            for p in range(1, n_dev):
                got.append(swap(made[p], p))
            chunks.append((begin, got))
            begin += made[0].shape[1]
        params, at_target = _merge(packs)
        out = None
        for peers in ((0, 1), (2, 3)):
            for k, (begin, got) in enumerate(chunks):
                blocks = [got[p] for p in peers]
                if k < len(chunks) - 1 or peers[0] == 0:
                    blocks = [pltpu.with_memory_space_constraint(a, pltpu.HBM) for a in blocks]
                out, params = _cdf(blocks, peers, params, out, n_dev, shard, begin)
        return out, at_target.reshape(-1)

    return jax.shard_map(
        local_step,
        mesh=mesh,
        in_specs=(P("dp", None), P(None, "vp"), P("dp"), P("dp")),
        out_specs=(P(("dp", "vp"), None), P("dp")),
        check_vma=False,
    )
```

```python
import functools

import jax
import jax.numpy as jnp
from jax import lax
from jax.experimental import pallas as pl
from jax.experimental.pallas import tpu as pltpu
from jax.sharding import PartitionSpec as P


LANES = 128
UNIT = 512
HALF = 256
DEPTH = 512
SLOTS = 9
EARLY = ((256, 2), (512, 1), (1024, 1), (2048, 3))
LATE = (4096, 2048, 1280, 384)
LATE_UNITS = ((2048, 2), (2048, 1), (1280, 1), (384, 1))


def _to_rows(vec_1xn):
    n = vec_1xn.shape[1]
    return jnp.transpose(jnp.broadcast_to(vec_1xn, (LANES, n)))


def _peer(me, p):
    return [me, me + 1 - 2 * lax.rem(me, 2), lax.rem(me + 2, 4), 3 - me][p]


def _logits_kernel(cfg, x_ref, w_ref, invt_ref, tgt_ref, *refs):
    n_dev, shard, segments, n_late = cfg
    refs = list(refs)

    def take(n):
        out = refs[:n]
        del refs[:n]
        return out

    early = take(n_dev)
    late = [take(n_dev) for _ in range(n_late)]
    packs = take(n_dev)
    xs, wbuf, acc, zsend, zbuf, invt_v, tgt_v, pack_v = take(8)
    scale_rows, left_rows, tmp, m_ref, s_ref, t_ref = take(6)
    w_sem, z_sem, x_sem, v_sem, own_sem, send_sem, recv_sem, pack_send, pack_recv = take(9)
    me = lax.axis_index("vp")
    batch, depth = xs.shape
    rows = batch // n_dev
    k_steps = depth // DEPTH

    def rows_of(p):
        return pl.ds(pl.multiple_of(_peer(me, p) * rows, rows), rows)

    def fetch_w(seg, step):
        width, col0, g0 = segments[seg][0], segments[seg][3], segments[seg][4]
        slot = lax.rem(g0 + step, SLOTS)
        col = col0 + lax.div(step, k_steps) * width
        row = pl.multiple_of(lax.rem(step, k_steps) * DEPTH, DEPTH)
        return pltpu.make_async_copy(
            w_ref.at[pl.ds(row, DEPTH), pl.ds(pl.multiple_of(col, LANES), width)],
            wbuf.at[slot, :, pl.ds(0, width)],
            w_sem.at[slot],
        )

    def put_late(slot, c, off, width):
        return [
            pltpu.make_async_copy(
                zbuf.at[slot, pl.ds(p * rows, rows), pl.ds(0, width)],
                late[c][p].at[:, pl.ds(off, width)],
                z_sem.at[slot, p],
            )
            for p in range(n_dev)
        ]

    def put_own(u, off, width):
        return pltpu.make_async_copy(
            zsend.at[pl.ds(0, rows), pl.ds(off, width)], early[0].at[:, pl.ds(off, width)], own_sem.at[u]
        )

    def send(u, p, off, width):
        return pltpu.make_async_remote_copy(
            src_ref=zsend.at[pl.ds(p * rows, rows), pl.ds(off, width)],
            dst_ref=early[p].at[:, pl.ds(off, width)],
            send_sem=send_sem.at[u, p],
            recv_sem=recv_sem.at[u, p],
            device_id={"vp": _peer(me, p)},
            device_id_type=pl.DeviceIdType.MESH,
        )

    x_copies = [
        pltpu.make_async_copy(x_ref.at[rows_of(p), :], xs.at[pl.ds(p * rows, rows), :], x_sem.at[p])
        for p in range(n_dev)
    ]
    small = [
        pltpu.make_async_copy(invt_ref, invt_v, v_sem.at[0]),
        pltpu.make_async_copy(tgt_ref, tgt_v, v_sem.at[1]),
    ]
    for copy in small + x_copies:
        copy.start()
    for i in range(SLOTS - 1):
        fetch_w(0, jnp.int32(i)).start()
    barrier = pltpu.get_barrier_semaphore()
    for p in range(1, n_dev):
        pl.semaphore_signal(
            barrier, inc=1, device_id={"vp": _peer(me, p)}, device_id_type=pl.DeviceIdType.MESH
        )
    m_ref[...] = jnp.full(m_ref.shape, -jnp.inf, jnp.float32)
    s_ref[...] = jnp.zeros_like(s_ref)
    t_ref[...] = jnp.zeros_like(t_ref)
    for copy in small:
        copy.wait()
    tmp[...] = _to_rows(invt_v[...])
    for p in range(n_dev):
        scale_rows[pl.ds(p * rows, rows), :] = tmp[rows_of(p), :]
    tmp[...] = _to_rows(tgt_v[...].astype(jnp.float32))
    lane = lax.broadcasted_iota(jnp.int32, (rows, LANES), 1)
    for p in range(n_dev):
        left_rows[pl.ds(p * rows, rows), :] = tmp[rows_of(p), :].astype(jnp.int32) - me * shard - lane
    for copy in x_copies:
        copy.wait()

    def multiply(seg, step):
        width = segments[seg][0]
        slot, k = lax.rem(segments[seg][4] + step, SLOTS), lax.rem(step, k_steps)
        fetch_w(seg, step).wait()
        x = xs[:, pl.ds(pl.multiple_of(k * DEPTH, DEPTH), DEPTH)]
        for off in range(0, width, HALF):
            wide = min(HALF, width - off)
            part = jnp.dot(x, wbuf[slot, :, off:off + wide], preferred_element_type=jnp.float32)
            acc[:, off:off + wide] = part + jnp.where(k == 0, 0.0, acc[:, off:off + wide])

    def finish(col, width, out_ref, out_off):
        group = 32
        span = next(n for n in (UNIT, HALF, LANES) if width % n == 0)

        def some(j, _):
            at = pl.multiple_of(j * span, span)
            for r in range(0, batch, group):
                block = slice(r, r + group)
                scale = scale_rows[block, :]
                tiles = []
                for t in range(0, span, LANES):
                    tile = acc[block, pl.ds(at + t, LANES)] * scale
                    out_ref[block, pl.ds(pl.multiple_of(out_off + at + t, LANES), LANES)] = tile
                    tiles.append(tile)
                m_old = m_ref[block, :]
                m_new = functools.reduce(jnp.maximum, tiles, m_old)
                keep = jnp.exp(m_old - m_new)
                total = s_ref[block, :] * keep
                upto = t_ref[block, :] * keep
                left = left_rows[block, :]
                for t, tile in enumerate(tiles):
                    e = jnp.exp(tile - m_new)
                    total += e
                    upto += jnp.where(left >= col + at + t * LANES, e, 0.0)
                m_ref[block, :] = m_new
                s_ref[block, :] = total
                t_ref[block, :] = upto
            return 0

        lax.fori_loop(0, width // span, some, 0)

    sent, own, stored = [], [], []
    for seg, (width, n, chunk, col0, g0) in enumerate(segments):
        for i in range(n):

            def body(k, _, seg=seg, i=i, n=n):
                step = i * k_steps + k
                ahead = step + SLOTS - 1

                @pl.when(ahead < n * k_steps)
                def _():
                    fetch_w(seg, ahead).start()

                if seg + 1 < len(segments):
                    @pl.when(ahead >= n * k_steps)
                    def _():
                        fetch_w(seg + 1, ahead - n * k_steps).start()

                multiply(seg, step)
                return 0

            lax.fori_loop(0, k_steps, body, 0)
            col = col0 + i * width
            if chunk is None:
                finish(col, width, zsend, col)
                if not sent:
                    pl.semaphore_wait(barrier, n_dev - 1)
                u = len(own)
                for p in (2, 3, 1):
                    copy = send(u, p, col, width)
                    copy.start()
                    sent.append(copy)
                copy = put_own(u, col, width)
                copy.start()
                own.append(copy)
            else:
                slot = len(stored) % 2
                if len(stored) >= 2:
                    for copy in stored[-2]:
                        copy.wait()
                finish(col, width, zbuf.at[slot], 0)
                c, off = chunk
                copies = put_late(slot, c, off + i * width, width)
                for copy in copies:
                    copy.start()
                stored.append(copies)
    m = m_ref[...]
    m_row = jnp.max(m, axis=1, keepdims=True)
    keep = jnp.exp(m - m_row)
    s_row = jnp.sum(s_ref[...] * keep, axis=1, keepdims=True)
    t_row = jnp.sum(t_ref[...] * keep, axis=1, keepdims=True)
    which = lax.broadcasted_iota(jnp.int32, m.shape, 1)
    packed = jnp.where(which == 0, m_row, jnp.where(which == 1, s_row, t_row))
    for p in range(n_dev):
        tmp[rows_of(p), :] = packed[p * rows:(p + 1) * rows, :]
    pack_v[...] = jnp.transpose(tmp[...])[:8, :]
    for p in (2, 3, 1):
        copy = pltpu.make_async_remote_copy(
            src_ref=pack_v,
            dst_ref=packs[p],
            send_sem=pack_send.at[p],
            recv_sem=pack_recv.at[p],
            device_id={"vp": _peer(me, p)},
            device_id_type=pl.DeviceIdType.MESH,
        )
        copy.start()
        sent.append(copy)
    copy = pltpu.make_async_copy(pack_v, packs[0], pack_send.at[0])
    copy.start()
    own.append(copy)
    for copies in stored[-2:]:
        for copy in copies:
            copy.wait()
    for copy in own + sent:
        copy.wait()


def _logits(x, w, invt, tgt, n_dev):
    batch, depth = x.shape
    shard = w.shape[1]
    rows = batch // n_dev
    segments, col, g0 = [], 0, 0
    chunk_of = {}
    begin = sum(width * n for width, n in EARLY)
    for c, width in enumerate(LATE):
        chunk_of.update({begin + i: (c, i) for i in range(0, width, LANES)})
        begin += width
    for i, (width, n) in enumerate(EARLY + LATE_UNITS):
        segments.append((width, n, None if i < len(EARLY) else chunk_of[col], col, g0))
        col += width * n
        g0 += n * (depth // DEPTH)
    assert col == shard == begin
    n_early = sum(n for _, n in EARLY)
    sent = sum(width * n for width, n in EARLY)
    hbm = pl.BlockSpec(memory_space=pltpu.HBM)
    out_shape = [pltpu.HBM((rows, sent), jnp.float32)] * n_dev
    out_shape += [pltpu.HBM((rows, width), jnp.float32) for width in LATE for _ in range(n_dev)]
    out_shape += [pltpu.HBM((8, batch), jnp.float32)] * n_dev
    table = pltpu.VMEM((batch, LANES), jnp.float32)
    widest = max(width for width, _ in EARLY + LATE_UNITS)
    dma = pltpu.SemaphoreType.DMA
    res = pl.pallas_call(
        functools.partial(_logits_kernel, (n_dev, shard, segments, len(LATE))),
        in_specs=[hbm] * 4,
        out_specs=[hbm] * len(out_shape),
        out_shape=out_shape,
        scratch_shapes=[
            pltpu.VMEM((batch, depth), jnp.bfloat16),
            pltpu.VMEM((SLOTS, DEPTH, widest), jnp.bfloat16),
            pltpu.VMEM((batch, widest), jnp.float32),
            pltpu.VMEM((batch, sent), jnp.float32),
            pltpu.VMEM((2, batch, widest), jnp.float32),
            pltpu.VMEM((1, batch), jnp.float32),
            pltpu.VMEM((1, batch), jnp.int32),
            pltpu.VMEM((8, batch), jnp.float32),
            table,
            pltpu.VMEM((batch, LANES), jnp.int32),
            table,
            table,
            table,
            table,
            dma((SLOTS,)),
            dma((2, n_dev)),
            dma((n_dev,)),
            dma((2,)),
            dma((n_early,)),
            dma((n_early, n_dev)),
            dma((n_early, n_dev)),
            dma((n_dev,)),
            dma((n_dev,)),
        ],
        compiler_params=pltpu.CompilerParams(
            collective_id=0, has_side_effects=True, vmem_limit_bytes=52 * 2**20
        ),
        cost_estimate=pl.CostEstimate(
            flops=2 * batch * depth * shard,
            bytes_accessed=2 * depth * shard,
            transcendentals=batch * shard,
        ),
        name="logits",
    )(*(pltpu.with_memory_space_constraint(a, pltpu.HBM) for a in (x, w, invt, tgt)))
    blocks = [res[c * n_dev:(c + 1) * n_dev] for c in range(len(LATE) + 2)]
    return blocks[0], blocks[1:-1], blocks[-1]


def _merge_kernel(n_dev, *refs):
    stats, (params_ref, at_ref) = refs[:n_dev], refs[n_dev:]
    me = lax.axis_index("vp")
    batch = stats[0].shape[1]
    rows = batch // n_dev
    ms = [s[0:1, :] for s in stats]
    top = functools.reduce(jnp.maximum, ms)
    keep = [jnp.exp(m - top) for m in ms]
    mass = [s[1:2, :] * k for s, k in zip(stats, keep)]
    upto = sum(s[2:3, :] * k for s, k in zip(stats, keep))
    total = sum(mass)
    at_ref[...] = upto / total
    values = [top, 1.0 / total]
    for p in range(n_dev):
        start = jnp.zeros_like(total)
        for q in range(n_dev):
            start += jnp.where((me ^ q) < (me ^ p), mass[q], 0.0)
        values.append(start)
    which = lax.broadcasted_iota(jnp.int32, (LANES, batch), 0)
    table = jnp.zeros((LANES, batch), jnp.float32)
    for i, v in enumerate(values):
        table = jnp.where(which == i, v, table)
    per_row = jnp.transpose(table)
    out = jnp.zeros((rows, LANES), jnp.float32)
    for d in range(n_dev):
        out = jnp.where(me == d, per_row[d * rows:(d + 1) * rows, :], out)
    params_ref[...] = out


def _merge(stats):
    n_dev = len(stats)
    batch = stats[0].shape[1]
    vmem = pl.BlockSpec(memory_space=pltpu.VMEM)
    return pl.pallas_call(
        functools.partial(_merge_kernel, n_dev),
        in_specs=[vmem] * n_dev,
        out_specs=[vmem] * 2,
        out_shape=[
            jax.ShapeDtypeStruct((batch // n_dev, LANES), jnp.float32),
            jax.ShapeDtypeStruct((1, batch), jnp.float32),
        ],
        cost_estimate=pl.CostEstimate(flops=100_000, bytes_accessed=100_000, transcendentals=1000),
        name="merge",
    )(*stats)


def _cdf_kernel(cfg, *refs):
    peers, shard, base, width, first, last = cfg
    n = len(peers)
    params_ref = refs[n]
    if last:
        out_ref, y_ref, sems = refs[n + 2:]
    else:
        out_ref, params_out, y_ref, sems = refs[n + (1 if first else 2):]
    me = lax.axis_index("vp")
    rows = params_ref.shape[0]
    params = params_ref[...]
    top = jnp.broadcast_to(params[:, 0:1], (rows, LANES))
    inv = jnp.broadcast_to(params[:, 1:2], (rows, LANES))
    k_id = lax.broadcasted_iota(jnp.int32, (3 * LANES, 2 * LANES), 0) % LANES
    n_id = lax.broadcasted_iota(jnp.int32, (3 * LANES, 2 * LANES), 1)
    tri = jnp.where(k_id <= n_id, 1.0, 0.0).astype(jnp.bfloat16)
    lane = lax.broadcasted_iota(jnp.int32, (rows, LANES), 1)

    def unit(col, wide, carries):
        ends = []
        for j in range(n):
            cols = [pl.ds(col + t, LANES) for t in range(0, wide, LANES)]
            e = jnp.concatenate([jnp.exp(refs[j][:, c] - top) for c in cols], axis=0)
            hi = e.astype(jnp.bfloat16)
            r1 = e - hi.astype(jnp.float32)
            mid = r1.astype(jnp.bfloat16)
            lo = (r1 - mid.astype(jnp.float32)).astype(jnp.bfloat16)
            sums = jnp.dot(jnp.concatenate([hi, mid, lo], axis=1), tri, preferred_element_type=jnp.float32)
            carry = carries[j]
            for t, c in enumerate(cols):
                block = slice(t * rows, (t + 1) * rows)
                y_ref[j, :, c] = (sums[block, :LANES] + carry) * inv
                carry = carry + sums[block, LANES:]
            ends.append(carry)
        return tuple(ends)

    carries = tuple(jnp.broadcast_to(params[:, 2 + p:3 + p], (rows, LANES)) for p in peers)
    n_full = width // UNIT
    if n_full:
        carries = lax.fori_loop(
            0, n_full, lambda u, c: unit(pl.multiple_of(u * UNIT, UNIT), UNIT, c), carries
        )
    if width % UNIT:
        carries = unit(n_full * UNIT, width % UNIT, carries)
    copies = []
    updated = params
    for j, p in enumerate(peers):
        where = pl.multiple_of((me ^ p) * shard + base, LANES)
        copy = pltpu.make_async_copy(y_ref.at[j], out_ref.at[:, pl.ds(where, width)], sems.at[j])
        copy.start()
        copies.append(copy)
        updated = jnp.where(lane == 2 + p, carries[j], updated)
    if not last:
        params_out[...] = updated
    for copy in copies:
        copy.wait()


def _cdf(blocks, peers, params, out, n_dev, shard, base, last=False):
    rows, width = blocks[0].shape
    n = len(peers)
    first = out is None
    vmem = pl.BlockSpec(memory_space=pltpu.VMEM)
    hbm = pl.BlockSpec(memory_space=pl.ANY)
    return pl.pallas_call(
        functools.partial(_cdf_kernel, (peers, shard, base, width, first, last)),
        in_specs=[vmem] * (n + 1) + ([] if first else [hbm]),
        out_specs=[hbm] + ([] if last else [vmem]),
        out_shape=[jax.ShapeDtypeStruct((rows, n_dev * shard), jnp.float32)]
        + ([] if last else [jax.ShapeDtypeStruct(params.shape, jnp.float32)]),
        scratch_shapes=[
            pltpu.VMEM((n, rows, width), jnp.float32),
            pltpu.SemaphoreType.DMA((n,)),
        ],
        input_output_aliases={} if first else {n + 1: 0},
        compiler_params=pltpu.CompilerParams(vmem_limit_bytes=24 * 2**20),
        cost_estimate=pl.CostEstimate(
            flops=n * 2 * rows * width * 384,
            bytes_accessed=n * rows * width * 8,
            transcendentals=n * rows * width,
        ),
        name="cdf",
    )(*blocks, params, *(() if first else (out,)))


def solution(mesh):
    n_dev = mesh.shape["vp"]
    assert n_dev == 4

    def swap(a, p):
        return lax.ppermute(a, "vp", [(i, i ^ p) for i in range(n_dev)])

    def local_step(hidden, w_local, inv_temp, target_ids):
        shard = w_local.shape[1]
        early, late, packs = _logits(
            hidden, w_local, inv_temp.reshape(1, -1), target_ids.reshape(1, -1), n_dev
        )
        chunks = [(0, early)]
        begin = early[0].shape[1]
        for made in late:
            got = [made[0]]
            for p in range(1, n_dev):
                got.append(swap(made[p], p))
            chunks.append((begin, got))
            begin += made[0].shape[1]
        params, at_target = _merge(packs)
        out = None
        final = len(chunks) - 1
        plan = [(k, (0, 1)) for k in range(final + 1)] + [(k, (2, 3)) for k in range(final)]
        plan += [(final, (2,)), (final, (3,))]
        for i, (k, peers) in enumerate(plan):
            begin, got = chunks[k]
            blocks = [got[p] for p in peers]
            if k < final or peers[0] == 0:
                blocks = [pltpu.with_memory_space_constraint(a, pltpu.HBM) for a in blocks]
            res = _cdf(blocks, peers, params, out, n_dev, shard, begin, i == len(plan) - 1)
            out = res[0]
            params = res[1] if len(res) > 1 else None
        return out, at_target.reshape(-1)

    return jax.shard_map(
        local_step,
        mesh=mesh,
        in_specs=(P("dp", None), P(None, "vp"), P("dp"), P("dp")),
        out_specs=(P(("dp", "vp"), None), P("dp")),
        check_vma=False,
    )
```

```python
import functools

import jax
import jax.numpy as jnp
from jax import lax
from jax.experimental import pallas as pl
from jax.experimental.pallas import tpu as pltpu
from jax.sharding import PartitionSpec as P


LANES = 128
UNIT = 512
HALF = 256
DEPTH = 512
SLOTS = 9
EARLY = ((128, 2), (256, 1), (512, 1), (1024, 1), (2048, 3))
LATE = (1536, 2048, 2560, 1280, 384)
LATE_UNITS = ((1536, 1), (2048, 1), (1280, 2), (1280, 1), (384, 1))
STATS = 4


def _to_rows(vec_1xn):
    n = vec_1xn.shape[1]
    return jnp.transpose(jnp.broadcast_to(vec_1xn, (LANES, n)))


def _peer(me, p):
    return [me, me + 1 - 2 * lax.rem(me, 2), lax.rem(me + 2, 4), 3 - me][p]


def _logits_kernel(cfg, x_ref, w_ref, invt_ref, tgt_ref, *refs):
    n_dev, shard, segments, n_late = cfg
    refs = list(refs)

    def take(n):
        out = refs[:n]
        del refs[:n]
        return out

    early = take(n_dev)
    late = [take(n_dev) for _ in range(n_late)]
    packs = take(n_dev)
    (extra,) = take(1)
    xs, wbuf, acc, zsend, zextra, zbuf, invt_v, tgt_v, pack_v = take(9)
    scale_rows, left_rows, tmp, m_ref, s_ref, t_ref = take(6)
    w_sem, z_sem, x_sem, v_sem, own_sem, send_sem, recv_sem, pack_send, pack_recv, extra_sem = take(10)
    me = lax.axis_index("vp")
    batch, depth = xs.shape
    rows = batch // n_dev
    k_steps = depth // DEPTH

    def rows_of(p):
        return pl.ds(pl.multiple_of(_peer(me, p) * rows, rows), rows)

    def fetch_w(seg, step):
        width, col0, g0 = segments[seg][0], segments[seg][3], segments[seg][4]
        slot = lax.rem(g0 + step, SLOTS)
        col = col0 + lax.div(step, k_steps) * width
        row = pl.multiple_of(lax.rem(step, k_steps) * DEPTH, DEPTH)
        return pltpu.make_async_copy(
            w_ref.at[pl.ds(row, DEPTH), pl.ds(pl.multiple_of(col, LANES), width)],
            wbuf.at[slot, :, pl.ds(0, width)],
            w_sem.at[slot],
        )

    def put_late(src, slot, c, off, width):
        return [
            pltpu.make_async_copy(
                src.at[pl.ds(p * rows, rows), pl.ds(0, width)],
                late[c][p].at[:, pl.ds(off, width)],
                z_sem.at[slot, p],
            )
            for p in range(n_dev)
        ]

    def send_extra():
        return pltpu.make_async_remote_copy(
            src_ref=zextra.at[pl.ds(2 * rows, rows), :],
            dst_ref=extra,
            send_sem=extra_sem.at[0],
            recv_sem=extra_sem.at[1],
            device_id={"vp": _peer(me, 2)},
            device_id_type=pl.DeviceIdType.MESH,
        )

    def put_own(u, off, width):
        return pltpu.make_async_copy(
            zsend.at[pl.ds(0, rows), pl.ds(off, width)], early[0].at[:, pl.ds(off, width)], own_sem.at[u]
        )

    def send(u, p, off, width):
        return pltpu.make_async_remote_copy(
            src_ref=zsend.at[pl.ds(p * rows, rows), pl.ds(off, width)],
            dst_ref=early[p].at[:, pl.ds(off, width)],
            send_sem=send_sem.at[u, p],
            recv_sem=recv_sem.at[u, p],
            device_id={"vp": _peer(me, p)},
            device_id_type=pl.DeviceIdType.MESH,
        )

    x_copies = [
        pltpu.make_async_copy(x_ref.at[rows_of(p), :], xs.at[pl.ds(p * rows, rows), :], x_sem.at[p])
        for p in range(n_dev)
    ]
    small = [
        pltpu.make_async_copy(invt_ref, invt_v, v_sem.at[0]),
        pltpu.make_async_copy(tgt_ref, tgt_v, v_sem.at[1]),
    ]
    for copy in small + x_copies:
        copy.start()
    for i in range(SLOTS - 1):
        fetch_w(0, jnp.int32(i)).start()
    barrier = pltpu.get_barrier_semaphore()
    for p in range(1, n_dev):
        pl.semaphore_signal(
            barrier, inc=1, device_id={"vp": _peer(me, p)}, device_id_type=pl.DeviceIdType.MESH
        )
    m_ref[...] = jnp.full(m_ref.shape, -jnp.inf, jnp.float32)
    s_ref[...] = jnp.zeros_like(s_ref)
    t_ref[...] = jnp.zeros_like(t_ref)
    for copy in small:
        copy.wait()
    tmp[...] = _to_rows(invt_v[...])
    for p in range(n_dev):
        scale_rows[pl.ds(p * rows, rows), :] = tmp[rows_of(p), :]
    tmp[...] = _to_rows(tgt_v[...].astype(jnp.float32))
    lane = lax.broadcasted_iota(jnp.int32, (rows, LANES), 1)
    for p in range(n_dev):
        left_rows[pl.ds(p * rows, rows), :] = tmp[rows_of(p), :].astype(jnp.int32) - me * shard - lane
    for copy in x_copies:
        copy.wait()

    def multiply(seg, step):
        width = segments[seg][0]
        slot, k = lax.rem(segments[seg][4] + step, SLOTS), lax.rem(step, k_steps)
        fetch_w(seg, step).wait()
        x = xs[:, pl.ds(pl.multiple_of(k * DEPTH, DEPTH), DEPTH)]
        for off in range(0, width, HALF):
            wide = min(HALF, width - off)
            part = jnp.dot(x, wbuf[slot, :, off:off + wide], preferred_element_type=jnp.float32)
            acc[:, off:off + wide] = part + jnp.where(k == 0, 0.0, acc[:, off:off + wide])

    def finish(col, width, out_ref, out_off):
        group = 32
        span = next(n for n in (UNIT, HALF, LANES) if width % n == 0)

        def some(j, _):
            at = pl.multiple_of(j * span, span)
            for r in range(0, batch, group):
                block = slice(r, r + group)
                scale = scale_rows[block, :]
                tiles = []
                for t in range(0, span, LANES):
                    tile = acc[block, pl.ds(at + t, LANES)] * scale
                    out_ref[block, pl.ds(pl.multiple_of(out_off + at + t, LANES), LANES)] = tile
                    tiles.append(tile)
                m_old = m_ref[block, :]
                m_new = functools.reduce(jnp.maximum, tiles, m_old)
                keep = jnp.exp(m_old - m_new)
                total = s_ref[block, :] * keep
                upto = t_ref[block, :] * keep
                left = left_rows[block, :]
                for t, tile in enumerate(tiles):
                    e = jnp.exp(tile - m_new)
                    total += e
                    upto += jnp.where(left >= col + at + t * LANES, e, 0.0)
                m_ref[block, :] = m_new
                s_ref[block, :] = total
                t_ref[block, :] = upto
            return 0

        lax.fori_loop(0, width // span, some, 0)

    sent, own, stored = [], [], []
    for seg, (width, n, chunk, col0, g0) in enumerate(segments):
        for i in range(n):

            def body(k, _, seg=seg, i=i, n=n):
                step = i * k_steps + k
                ahead = step + SLOTS - 1

                @pl.when(ahead < n * k_steps)
                def _():
                    fetch_w(seg, ahead).start()

                if seg + 1 < len(segments):
                    @pl.when(ahead >= n * k_steps)
                    def _():
                        fetch_w(seg + 1, ahead - n * k_steps).start()

                multiply(seg, step)
                return 0

            lax.fori_loop(0, k_steps, body, 0)
            col = col0 + i * width
            if chunk is None:
                finish(col, width, zsend, col)
                if not sent:
                    pl.semaphore_wait(barrier, n_dev - 1)
                u = len(own)
                for p in (2, 3, 1):
                    copy = send(u, p, col, width)
                    copy.start()
                    sent.append(copy)
                copy = put_own(u, col, width)
                copy.start()
                own.append(copy)
            else:
                c, off = chunk
                slot = 2 if c == 0 else len(stored) % 2
                if c and len(stored) > 2:
                    for copy in stored[-2]:
                        copy.wait()
                src = zbuf.at[slot] if c else zextra
                finish(col, width, src, 0)
                copies = put_late(src, slot, c, off + i * width, width)
                for copy in copies:
                    copy.start()
                stored.append(copies)
    m = m_ref[...]
    m_row = jnp.max(m, axis=1, keepdims=True)
    keep = jnp.exp(m - m_row)
    s_row = jnp.sum(s_ref[...] * keep, axis=1, keepdims=True)
    t_row = jnp.sum(t_ref[...] * keep, axis=1, keepdims=True)
    which = lax.broadcasted_iota(jnp.int32, m.shape, 1)
    packed = jnp.where(which == 0, m_row, jnp.where(which == 1, s_row, t_row))
    for p in range(n_dev):
        tmp[rows_of(p), :] = packed[p * rows:(p + 1) * rows, :]
    pack_v[...] = jnp.transpose(tmp[...])[:STATS, :]
    for p in (2, 3, 1):
        copy = pltpu.make_async_remote_copy(
            src_ref=pack_v,
            dst_ref=packs[p],
            send_sem=pack_send.at[p],
            recv_sem=pack_recv.at[p],
            device_id={"vp": _peer(me, p)},
            device_id_type=pl.DeviceIdType.MESH,
        )
        copy.start()
        sent.append(copy)
    copy = pltpu.make_async_copy(pack_v, packs[0], pack_send.at[0])
    copy.start()
    own.append(copy)

    @pl.when(lax.rem(me, 2) == 1)
    def _():
        send_extra().start()

    for copies in [stored[0]] + stored[-2:]:
        for copy in copies:
            copy.wait()
    for copy in own + sent:
        copy.wait()

    @pl.when(lax.rem(me, 2) == 1)
    def _():
        send_extra().wait()


def _logits(x, w, invt, tgt, n_dev):
    batch, depth = x.shape
    shard = w.shape[1]
    rows = batch // n_dev
    segments, col, g0 = [], 0, 0
    chunk_of = {}
    begin = sum(width * n for width, n in EARLY)
    for c, width in enumerate(LATE):
        chunk_of.update({begin + i: (c, i) for i in range(0, width, LANES)})
        begin += width
    for i, (width, n) in enumerate(EARLY + LATE_UNITS):
        segments.append((width, n, None if i < len(EARLY) else chunk_of[col], col, g0))
        col += width * n
        g0 += n * (depth // DEPTH)
    assert col == shard == begin
    n_early = sum(n for _, n in EARLY)
    sent = sum(width * n for width, n in EARLY)
    hbm = pl.BlockSpec(memory_space=pltpu.HBM)
    out_shape = [pltpu.HBM((rows, sent), jnp.float32)] * n_dev
    out_shape += [pltpu.HBM((rows, width), jnp.float32) for width in LATE for _ in range(n_dev)]
    out_shape += [pltpu.HBM((STATS, batch), jnp.float32)] * n_dev
    out_shape += [pltpu.HBM((rows, LATE[0]), jnp.float32)]
    assert LATE_UNITS[0] == (LATE[0], 1)
    table = pltpu.VMEM((batch, LANES), jnp.float32)
    widest = max(width for width, _ in EARLY + LATE_UNITS)
    dma = pltpu.SemaphoreType.DMA
    res = pl.pallas_call(
        functools.partial(_logits_kernel, (n_dev, shard, segments, len(LATE))),
        in_specs=[hbm] * 4,
        out_specs=[hbm] * len(out_shape),
        out_shape=out_shape,
        scratch_shapes=[
            pltpu.VMEM((batch, depth), jnp.bfloat16),
            pltpu.VMEM((SLOTS, DEPTH, widest), jnp.bfloat16),
            pltpu.VMEM((batch, widest), jnp.float32),
            pltpu.VMEM((batch, sent), jnp.float32),
            pltpu.VMEM((batch, LATE[0]), jnp.float32),
            pltpu.VMEM((2, batch, widest), jnp.float32),
            pltpu.VMEM((1, batch), jnp.float32),
            pltpu.VMEM((1, batch), jnp.int32),
            pltpu.VMEM((STATS, batch), jnp.float32),
            table,
            pltpu.VMEM((batch, LANES), jnp.int32),
            table,
            table,
            table,
            table,
            dma((SLOTS,)),
            dma((3, n_dev)),
            dma((n_dev,)),
            dma((2,)),
            dma((n_early,)),
            dma((n_early, n_dev)),
            dma((n_early, n_dev)),
            dma((n_dev,)),
            dma((n_dev,)),
            dma((2,)),
        ],
        compiler_params=pltpu.CompilerParams(
            collective_id=0, has_side_effects=True, vmem_limit_bytes=52 * 2**20
        ),
        cost_estimate=pl.CostEstimate(
            flops=2 * batch * depth * shard,
            bytes_accessed=2 * depth * shard,
            transcendentals=batch * shard,
        ),
        name="logits",
    )(*(pltpu.with_memory_space_constraint(a, pltpu.HBM) for a in (x, w, invt, tgt)))
    blocks = [res[c * n_dev:(c + 1) * n_dev] for c in range(len(LATE) + 2)]
    return blocks[0], blocks[1:-1], blocks[-1], res[-1]


def _merge_kernel(n_dev, *refs):
    stats, (params_ref, at_ref) = refs[:n_dev], refs[n_dev:]
    me = lax.axis_index("vp")
    batch = stats[0].shape[1]
    rows = batch // n_dev
    ms = [s[0:1, :] for s in stats]
    top = functools.reduce(jnp.maximum, ms)
    keep = [jnp.exp(m - top) for m in ms]
    mass = [s[1:2, :] * k for s, k in zip(stats, keep)]
    upto = sum(s[2:3, :] * k for s, k in zip(stats, keep))
    total = sum(mass)
    at_ref[...] = upto / total
    values = [top, 1.0 / total]
    for p in range(n_dev):
        start = jnp.zeros_like(total)
        for q in range(n_dev):
            start += jnp.where((me ^ q) < (me ^ p), mass[q], 0.0)
        values.append(start)
    which = lax.broadcasted_iota(jnp.int32, (LANES, batch), 0)
    table = jnp.zeros((LANES, batch), jnp.float32)
    for i, v in enumerate(values):
        table = jnp.where(which == i, v, table)
    per_row = jnp.transpose(table)
    out = jnp.zeros((rows, LANES), jnp.float32)
    for d in range(n_dev):
        out = jnp.where(me == d, per_row[d * rows:(d + 1) * rows, :], out)
    params_ref[...] = out


def _merge(stats):
    n_dev = len(stats)
    batch = stats[0].shape[1]
    vmem = pl.BlockSpec(memory_space=pltpu.VMEM)
    return pl.pallas_call(
        functools.partial(_merge_kernel, n_dev),
        in_specs=[vmem] * n_dev,
        out_specs=[vmem] * 2,
        out_shape=[
            jax.ShapeDtypeStruct((batch // n_dev, LANES), jnp.float32),
            jax.ShapeDtypeStruct((1, batch), jnp.float32),
        ],
        cost_estimate=pl.CostEstimate(flops=100_000, bytes_accessed=100_000, transcendentals=1000),
        name="merge",
    )(*stats)


def _cdf_kernel(cfg, *refs):
    peers, shard, base, width, first, last, two_sources = cfg
    n = len(peers)
    if two_sources:
        other_ref, refs = refs[n], refs[:n] + refs[n + 1:]
    params_ref = refs[n]
    if last:
        out_ref, y_ref, sems = refs[n + 2:]
    else:
        out_ref, params_out, y_ref, sems = refs[n + (1 if first else 2):]
    me = lax.axis_index("vp")
    rows = params_ref.shape[0]
    params = params_ref[...]
    top = jnp.broadcast_to(params[:, 0:1], (rows, LANES))
    inv = jnp.broadcast_to(params[:, 1:2], (rows, LANES))
    k_id = lax.broadcasted_iota(jnp.int32, (3 * LANES, 2 * LANES), 0) % LANES
    n_id = lax.broadcasted_iota(jnp.int32, (3 * LANES, 2 * LANES), 1)
    tri = jnp.where(k_id <= n_id, 1.0, 0.0).astype(jnp.bfloat16)
    lane = lax.broadcasted_iota(jnp.int32, (rows, LANES), 1)

    odd = lax.rem(me, 2) == 1

    def unit(col, wide, carries):
        ends = []
        for j in range(n):
            cols = [pl.ds(col + t, LANES) for t in range(0, wide, LANES)]
            zs = [refs[j][:, c] for c in cols]
            if two_sources and j == 0:
                zs = [jnp.where(odd, other_ref[:, c], z) for c, z in zip(cols, zs)]
            e = jnp.concatenate([jnp.exp(z - top) for z in zs], axis=0)
            hi = e.astype(jnp.bfloat16)
            r1 = e - hi.astype(jnp.float32)
            mid = r1.astype(jnp.bfloat16)
            lo = (r1 - mid.astype(jnp.float32)).astype(jnp.bfloat16)
            sums = jnp.dot(jnp.concatenate([hi, mid, lo], axis=1), tri, preferred_element_type=jnp.float32)
            carry = carries[j]
            for t, c in enumerate(cols):
                block = slice(t * rows, (t + 1) * rows)
                y_ref[j, :, c] = (sums[block, :LANES] + carry) * inv
                carry = carry + sums[block, LANES:]
            ends.append(carry)
        return tuple(ends)

    carries = tuple(jnp.broadcast_to(params[:, 2 + p:3 + p], (rows, LANES)) for p in peers)
    n_full = width // UNIT
    if n_full:
        carries = lax.fori_loop(
            0, n_full, lambda u, c: unit(pl.multiple_of(u * UNIT, UNIT), UNIT, c), carries
        )
    if width % UNIT:
        carries = unit(n_full * UNIT, width % UNIT, carries)
    copies = []
    updated = params
    for j, p in enumerate(peers):
        where = pl.multiple_of((me ^ p) * shard + base, LANES)
        copy = pltpu.make_async_copy(y_ref.at[j], out_ref.at[:, pl.ds(where, width)], sems.at[j])
        copy.start()
        copies.append(copy)
        updated = jnp.where(lane == 2 + p, carries[j], updated)
    if not last:
        params_out[...] = updated
    for copy in copies:
        copy.wait()


def _cdf(blocks, peers, params, out, n_dev, shard, base, last=False, other=None):
    rows, width = blocks[0].shape
    n = len(peers)
    first = out is None
    extra = [] if other is None else [other]
    vmem = pl.BlockSpec(memory_space=pltpu.VMEM)
    hbm = pl.BlockSpec(memory_space=pl.ANY)
    return pl.pallas_call(
        functools.partial(_cdf_kernel, (peers, shard, base, width, first, last, bool(extra))),
        in_specs=[vmem] * (n + len(extra) + 1) + ([] if first else [hbm]),
        out_specs=[hbm] + ([] if last else [vmem]),
        out_shape=[jax.ShapeDtypeStruct((rows, n_dev * shard), jnp.float32)]
        + ([] if last else [jax.ShapeDtypeStruct(params.shape, jnp.float32)]),
        scratch_shapes=[
            pltpu.VMEM((n, rows, width), jnp.float32),
            pltpu.SemaphoreType.DMA((n,)),
        ],
        input_output_aliases={} if first else {n + len(extra) + 1: 0},
        compiler_params=pltpu.CompilerParams(vmem_limit_bytes=24 * 2**20),
        cost_estimate=pl.CostEstimate(
            flops=n * 2 * rows * width * 384,
            bytes_accessed=n * rows * width * 8,
            transcendentals=n * rows * width,
        ),
        name="cdf",
    )(*blocks, *extra, params, *(() if first else (out,)))


def solution(mesh):
    n_dev = mesh.shape["vp"]
    assert n_dev == 4

    def swap(a, p, step=1):
        return lax.ppermute(a, "vp", [(i, i ^ p) for i in range(0, n_dev, step)])

    def local_step(hidden, w_local, inv_temp, target_ids):
        shard = w_local.shape[1]
        early, late, packs, extra = _logits(hidden, w_local, inv_temp.reshape(1, -1), target_ids.reshape(1, -1), n_dev)
        chunks = [(0, early)]
        begin = early[0].shape[1]
        for k, made in enumerate(late):
            got = [made[0]]
            for p in range(1, n_dev):
                got.append(swap(made[p], p, 2 if k == 0 and p == 2 else 1))
            chunks.append((begin, got))
            begin += made[0].shape[1]
        params, at_target = _merge(packs)
        out = None
        final = len(chunks) - 1
        plan = [(k, (0, 1)) for k in range(final + 1)] + [(k, (2, 3)) for k in range(final)]
        plan += [(final, (2,)), (final, (3,))]
        for i, (k, peers) in enumerate(plan):
            begin, got = chunks[k]
            blocks = [got[p] for p in peers]
            if k < final or peers[0] == 0:
                blocks = [pltpu.with_memory_space_constraint(a, pltpu.HBM) for a in blocks]
            other = pltpu.with_memory_space_constraint(extra, pltpu.HBM) if k == 1 and peers[0] == 2 else None
            res = _cdf(blocks, peers, params, out, n_dev, shard, begin, i == len(plan) - 1, other)
            out = res[0]
            params = res[1] if len(res) > 1 else None
        return out, at_target.reshape(-1)

    return jax.shard_map(
        local_step,
        mesh=mesh,
        in_specs=(P("dp", None), P(None, "vp"), P("dp"), P("dp")),
        out_specs=(P(("dp", "vp"), None), P("dp")),
        check_vma=False,
    )
```

```python
import functools

import jax
import jax.numpy as jnp
from jax import lax
from jax.experimental import pallas as pl
from jax.experimental.pallas import tpu as pltpu
from jax.sharding import PartitionSpec as P


LANES = 128
UNIT = 512
HALF = 256
DEPTH = 512
SLOTS = 9
EARLY = ((256, 2), (512, 1), (1024, 1), (2048, 3))
LATE = (4096, 2048, 1280, 384)
LATE_UNITS = ((2048, 2), (2048, 1), (1280, 1), (384, 1))
STATS = 4


def _to_rows(vec_1xn):
    n = vec_1xn.shape[1]
    return jnp.transpose(jnp.broadcast_to(vec_1xn, (LANES, n)))


def _peer(me, p):
    return [me, me + 1 - 2 * lax.rem(me, 2), lax.rem(me + 2, 4), 3 - me][p]


def _logits_kernel(cfg, x_ref, w_ref, invt_ref, tgt_ref, *refs):
    n_dev, shard, segments, n_late = cfg
    refs = list(refs)

    def take(n):
        out = refs[:n]
        del refs[:n]
        return out

    early = take(n_dev)
    late = [take(n_dev) for _ in range(n_late)]
    packs = take(n_dev)
    xs, wbuf, acc, zsend, zbuf, invt_v, tgt_v, pack_v = take(8)
    scale_rows, left_rows, tmp, m_ref, s_ref, t_ref = take(6)
    w_sem, z_sem, x_sem, v_sem, own_sem, send_sem, recv_sem, pack_send, pack_recv = take(9)
    me = lax.axis_index("vp")
    batch, depth = xs.shape
    rows = batch // n_dev
    k_steps = depth // DEPTH
    assert SLOTS == k_steps + 1

    def rows_of(p):
        return pl.ds(pl.multiple_of(_peer(me, p) * rows, rows), rows)

    def fetch_w(seg, step):
        width, col0, g0 = segments[seg][0], segments[seg][3], segments[seg][4]
        slot = lax.rem(g0 + step, SLOTS)
        col = col0 + lax.div(step, k_steps) * width
        row = pl.multiple_of(lax.rem(step, k_steps) * DEPTH, DEPTH)
        return pltpu.make_async_copy(
            w_ref.at[pl.ds(row, DEPTH), pl.ds(pl.multiple_of(col, LANES), width)],
            wbuf.at[slot, :, pl.ds(0, width)],
            w_sem.at[slot],
        )

    def put_late(slot, c, off, width):
        return [
            pltpu.make_async_copy(
                zbuf.at[slot, pl.ds(p * rows, rows), pl.ds(0, width)],
                late[c][p].at[:, pl.ds(off, width)],
                z_sem.at[slot, p],
            )
            for p in range(n_dev)
        ]

    def put_own(u, off, width):
        return pltpu.make_async_copy(
            zsend.at[pl.ds(0, rows), pl.ds(off, width)], early[0].at[:, pl.ds(off, width)], own_sem.at[u]
        )

    def send(u, p, off, width):
        return pltpu.make_async_remote_copy(
            src_ref=zsend.at[pl.ds(p * rows, rows), pl.ds(off, width)],
            dst_ref=early[p].at[:, pl.ds(off, width)],
            send_sem=send_sem.at[u, p],
            recv_sem=recv_sem.at[u, p],
            device_id={"vp": _peer(me, p)},
            device_id_type=pl.DeviceIdType.MESH,
        )

    x_copies = [
        pltpu.make_async_copy(x_ref.at[rows_of(p), :], xs.at[pl.ds(p * rows, rows), :], x_sem.at[p])
        for p in range(n_dev)
    ]
    small = [
        pltpu.make_async_copy(invt_ref, invt_v, v_sem.at[0]),
        pltpu.make_async_copy(tgt_ref, tgt_v, v_sem.at[1]),
    ]
    for copy in small + x_copies[2:]:
        copy.start()
    for i in range(k_steps):
        fetch_w(0, jnp.int32(i)).start()
    for copy in x_copies[:2]:
        copy.start()
    barrier = pltpu.get_barrier_semaphore()
    for p in range(1, n_dev):
        pl.semaphore_signal(
            barrier, inc=1, device_id={"vp": _peer(me, p)}, device_id_type=pl.DeviceIdType.MESH
        )
    m_ref[...] = jnp.full(m_ref.shape, -jnp.inf, jnp.float32)
    s_ref[...] = jnp.zeros_like(s_ref)
    t_ref[...] = jnp.zeros_like(t_ref)
    for copy in small:
        copy.wait()
    tmp[...] = _to_rows(invt_v[...])
    for p in range(n_dev):
        scale_rows[pl.ds(p * rows, rows), :] = tmp[rows_of(p), :]
    tmp[...] = _to_rows(tgt_v[...].astype(jnp.float32))
    lane = lax.broadcasted_iota(jnp.int32, (rows, LANES), 1)
    for p in range(n_dev):
        left_rows[pl.ds(p * rows, rows), :] = tmp[rows_of(p), :].astype(jnp.int32) - me * shard - lane
    for copy in x_copies[2:]:
        copy.wait()

    def multiply(seg, step, lo=0, hi=batch):
        width = segments[seg][0]
        slot, k = lax.rem(segments[seg][4] + step, SLOTS), lax.rem(step, k_steps)
        x = xs[lo:hi, pl.ds(pl.multiple_of(k * DEPTH, DEPTH), DEPTH)]
        for off in range(0, width, HALF):
            wide = min(HALF, width - off)
            part = jnp.dot(x, wbuf[slot, :, off:off + wide], preferred_element_type=jnp.float32)
            acc[lo:hi, off:off + wide] = part + jnp.where(k == 0, 0.0, acc[lo:hi, off:off + wide])

    def finish(col, width, out_ref, out_off, lo=0, hi=batch):
        group = 32
        span = next(n for n in (UNIT, HALF, LANES) if width % n == 0)

        def some(j, _):
            at = pl.multiple_of(j * span, span)
            for r in range(lo, hi, group):
                block = slice(r, r + group)
                scale = scale_rows[block, :]
                tiles = []
                for t in range(0, span, LANES):
                    tile = acc[block, pl.ds(at + t, LANES)] * scale
                    out_ref[block, pl.ds(pl.multiple_of(out_off + at + t, LANES), LANES)] = tile
                    tiles.append(tile)
                m_old = m_ref[block, :]
                m_new = functools.reduce(jnp.maximum, tiles, m_old)
                keep = jnp.exp(m_old - m_new)
                total = s_ref[block, :] * keep
                upto = t_ref[block, :] * keep
                left = left_rows[block, :]
                for t, tile in enumerate(tiles):
                    e = jnp.exp(tile - m_new)
                    total += e
                    upto += jnp.where(left >= col + at + t * LANES, e, 0.0)
                m_ref[block, :] = m_new
                s_ref[block, :] = total
                t_ref[block, :] = upto
            return 0

        lax.fori_loop(0, width // span, some, 0)

    sent, own, stored = [], [], []

    def send_early(u, peers, col, width):
        for p in peers:
            copy = send(u, p, col, width)
            copy.start()
            sent.append(copy)

    far, first_width = 2 * rows, segments[0][0]

    def far_body(k, _):
        fetch_w(0, k).wait()
        multiply(0, k, far, batch)
        return 0

    lax.fori_loop(0, k_steps, far_body, 0)
    finish(0, first_width, zsend, 0, far, batch)
    pl.semaphore_wait(barrier, n_dev - 1)
    send_early(0, (2, 3), 0, first_width)
    for copy in x_copies[:2]:
        copy.wait()

    for seg, (width, n, chunk, col0, g0) in enumerate(segments):
        for i in range(n):

            again = seg == 0 and i == 0

            def body(k, _, seg=seg, i=i, n=n, again=again):
                step = i * k_steps + k
                ahead = step + SLOTS - 1

                @pl.when(ahead < n * k_steps)
                def _():
                    fetch_w(seg, ahead).start()

                if seg + 1 < len(segments):
                    @pl.when(ahead >= n * k_steps)
                    def _():
                        fetch_w(seg + 1, ahead - n * k_steps).start()

                if again:
                    multiply(seg, step, 0, far)
                else:
                    fetch_w(seg, step).wait()
                    multiply(seg, step)
                return 0

            lax.fori_loop(0, k_steps, body, 0)
            col = col0 + i * width
            if chunk is None:
                finish(col, width, zsend, col, 0, far if again else batch)
                u = len(own)
                send_early(u, (1,) if again else (2, 3, 1), col, width)
                copy = put_own(u, col, width)
                copy.start()
                own.append(copy)
            else:
                slot = len(stored) % 2
                if len(stored) >= 2:
                    for copy in stored[-2]:
                        copy.wait()
                finish(col, width, zbuf.at[slot], 0)
                c, off = chunk
                copies = put_late(slot, c, off + i * width, width)
                for copy in copies:
                    copy.start()
                stored.append(copies)
    m = m_ref[...]
    m_row = jnp.max(m, axis=1, keepdims=True)
    keep = jnp.exp(m - m_row)
    s_row = jnp.sum(s_ref[...] * keep, axis=1, keepdims=True)
    t_row = jnp.sum(t_ref[...] * keep, axis=1, keepdims=True)
    which = lax.broadcasted_iota(jnp.int32, m.shape, 1)
    packed = jnp.where(which == 0, m_row, jnp.where(which == 1, s_row, t_row))
    for p in range(n_dev):
        tmp[rows_of(p), :] = packed[p * rows:(p + 1) * rows, :]
    pack_v[...] = jnp.transpose(tmp[...])[:STATS, :]
    for p in (2, 3, 1):
        copy = pltpu.make_async_remote_copy(
            src_ref=pack_v,
            dst_ref=packs[p],
            send_sem=pack_send.at[p],
            recv_sem=pack_recv.at[p],
            device_id={"vp": _peer(me, p)},
            device_id_type=pl.DeviceIdType.MESH,
        )
        copy.start()
        sent.append(copy)
    copy = pltpu.make_async_copy(pack_v, packs[0], pack_send.at[0])
    copy.start()
    own.append(copy)
    for copies in stored[-2:]:
        for copy in copies:
            copy.wait()
    for copy in own + sent:
        copy.wait()


def _logits(x, w, invt, tgt, n_dev):
    batch, depth = x.shape
    shard = w.shape[1]
    rows = batch // n_dev
    segments, col, g0 = [], 0, 0
    chunk_of = {}
    begin = sum(width * n for width, n in EARLY)
    for c, width in enumerate(LATE):
        chunk_of.update({begin + i: (c, i) for i in range(0, width, LANES)})
        begin += width
    for i, (width, n) in enumerate(EARLY + LATE_UNITS):
        segments.append((width, n, None if i < len(EARLY) else chunk_of[col], col, g0))
        col += width * n
        g0 += n * (depth // DEPTH)
    assert col == shard == begin
    n_early = sum(n for _, n in EARLY)
    sent = sum(width * n for width, n in EARLY)
    hbm = pl.BlockSpec(memory_space=pltpu.HBM)
    out_shape = [pltpu.HBM((rows, sent), jnp.float32)] * n_dev
    out_shape += [pltpu.HBM((rows, width), jnp.float32) for width in LATE for _ in range(n_dev)]
    out_shape += [pltpu.HBM((STATS, batch), jnp.float32)] * n_dev
    table = pltpu.VMEM((batch, LANES), jnp.float32)
    widest = max(width for width, _ in EARLY + LATE_UNITS)
    dma = pltpu.SemaphoreType.DMA
    res = pl.pallas_call(
        functools.partial(_logits_kernel, (n_dev, shard, segments, len(LATE))),
        in_specs=[hbm] * 4,
        out_specs=[hbm] * len(out_shape),
        out_shape=out_shape,
        scratch_shapes=[
            pltpu.VMEM((batch, depth), jnp.bfloat16),
            pltpu.VMEM((SLOTS, DEPTH, widest), jnp.bfloat16),
            pltpu.VMEM((batch, widest), jnp.float32),
            pltpu.VMEM((batch, sent), jnp.float32),
            pltpu.VMEM((2, batch, widest), jnp.float32),
            pltpu.VMEM((1, batch), jnp.float32),
            pltpu.VMEM((1, batch), jnp.int32),
            pltpu.VMEM((STATS, batch), jnp.float32),
            table,
            pltpu.VMEM((batch, LANES), jnp.int32),
            table,
            table,
            table,
            table,
            dma((SLOTS,)),
            dma((2, n_dev)),
            dma((n_dev,)),
            dma((2,)),
            dma((n_early,)),
            dma((n_early, n_dev)),
            dma((n_early, n_dev)),
            dma((n_dev,)),
            dma((n_dev,)),
        ],
        compiler_params=pltpu.CompilerParams(
            collective_id=0, has_side_effects=True, vmem_limit_bytes=52 * 2**20
        ),
        cost_estimate=pl.CostEstimate(
            flops=2 * batch * depth * shard,
            bytes_accessed=2 * depth * shard,
            transcendentals=batch * shard,
        ),
        name="logits",
    )(*(pltpu.with_memory_space_constraint(a, pltpu.HBM) for a in (x, w, invt, tgt)))
    blocks = [res[c * n_dev:(c + 1) * n_dev] for c in range(len(LATE) + 2)]
    return blocks[0], blocks[1:-1], blocks[-1]


def _merge_kernel(n_dev, *refs):
    stats, (params_ref, at_ref) = refs[:n_dev], refs[n_dev:]
    me = lax.axis_index("vp")
    batch = stats[0].shape[1]
    rows = batch // n_dev
    ms = [s[0:1, :] for s in stats]
    top = functools.reduce(jnp.maximum, ms)
    keep = [jnp.exp(m - top) for m in ms]
    mass = [s[1:2, :] * k for s, k in zip(stats, keep)]
    upto = sum(s[2:3, :] * k for s, k in zip(stats, keep))
    total = sum(mass)
    at_ref[...] = upto / total
    values = [top, 1.0 / total]
    for p in range(n_dev):
        start = jnp.zeros_like(total)
        for q in range(n_dev):
            start += jnp.where((me ^ q) < (me ^ p), mass[q], 0.0)
        values.append(start)
    which = lax.broadcasted_iota(jnp.int32, (LANES, batch), 0)
    table = jnp.zeros((LANES, batch), jnp.float32)
    for i, v in enumerate(values):
        table = jnp.where(which == i, v, table)
    per_row = jnp.transpose(table)
    out = jnp.zeros((rows, LANES), jnp.float32)
    for d in range(n_dev):
        out = jnp.where(me == d, per_row[d * rows:(d + 1) * rows, :], out)
    params_ref[...] = out


def _merge(stats):
    n_dev = len(stats)
    batch = stats[0].shape[1]
    vmem = pl.BlockSpec(memory_space=pltpu.VMEM)
    return pl.pallas_call(
        functools.partial(_merge_kernel, n_dev),
        in_specs=[vmem] * n_dev,
        out_specs=[vmem] * 2,
        out_shape=[
            jax.ShapeDtypeStruct((batch // n_dev, LANES), jnp.float32),
            jax.ShapeDtypeStruct((1, batch), jnp.float32),
        ],
        cost_estimate=pl.CostEstimate(flops=100_000, bytes_accessed=100_000, transcendentals=1000),
        name="merge",
    )(*stats)


def _cdf_kernel(cfg, *refs):
    peers, shard, base, width, first, last = cfg
    n = len(peers)
    params_ref = refs[n]
    if last:
        out_ref, y_ref, sems = refs[n + 2:]
    else:
        out_ref, params_out, y_ref, sems = refs[n + (1 if first else 2):]
    me = lax.axis_index("vp")
    rows = params_ref.shape[0]
    params = params_ref[...]
    top = jnp.broadcast_to(params[:, 0:1], (rows, LANES))
    inv = jnp.broadcast_to(params[:, 1:2], (rows, LANES))
    k_id = lax.broadcasted_iota(jnp.int32, (3 * LANES, 2 * LANES), 0) % LANES
    n_id = lax.broadcasted_iota(jnp.int32, (3 * LANES, 2 * LANES), 1)
    tri = jnp.where(k_id <= n_id, 1.0, 0.0).astype(jnp.bfloat16)
    lane = lax.broadcasted_iota(jnp.int32, (rows, LANES), 1)

    def unit(col, wide, carries):
        ends = []
        for j in range(n):
            cols = [pl.ds(col + t, LANES) for t in range(0, wide, LANES)]
            e = jnp.concatenate([jnp.exp(refs[j][:, c] - top) for c in cols], axis=0)
            hi = e.astype(jnp.bfloat16)
            r1 = e - hi.astype(jnp.float32)
            mid = r1.astype(jnp.bfloat16)
            lo = (r1 - mid.astype(jnp.float32)).astype(jnp.bfloat16)
            sums = jnp.dot(jnp.concatenate([hi, mid, lo], axis=1), tri, preferred_element_type=jnp.float32)
            carry = carries[j]
            for t, c in enumerate(cols):
                block = slice(t * rows, (t + 1) * rows)
                y_ref[j, :, c] = (sums[block, :LANES] + carry) * inv
                carry = carry + sums[block, LANES:]
            ends.append(carry)
        return tuple(ends)

    carries = tuple(jnp.broadcast_to(params[:, 2 + p:3 + p], (rows, LANES)) for p in peers)
    n_full = width // UNIT
    if n_full:
        carries = lax.fori_loop(
            0, n_full, lambda u, c: unit(pl.multiple_of(u * UNIT, UNIT), UNIT, c), carries
        )
    if width % UNIT:
        carries = unit(n_full * UNIT, width % UNIT, carries)
    copies = []
    updated = params
    for j, p in enumerate(peers):
        where = pl.multiple_of((me ^ p) * shard + base, LANES)
        copy = pltpu.make_async_copy(y_ref.at[j], out_ref.at[:, pl.ds(where, width)], sems.at[j])
        copy.start()
        copies.append(copy)
        updated = jnp.where(lane == 2 + p, carries[j], updated)
    if not last:
        params_out[...] = updated
    for copy in copies:
        copy.wait()


def _cdf(blocks, peers, params, out, n_dev, shard, base, last=False):
    rows, width = blocks[0].shape
    n = len(peers)
    first = out is None
    vmem = pl.BlockSpec(memory_space=pltpu.VMEM)
    hbm = pl.BlockSpec(memory_space=pl.ANY)
    return pl.pallas_call(
        functools.partial(_cdf_kernel, (peers, shard, base, width, first, last)),
        in_specs=[vmem] * (n + 1) + ([] if first else [hbm]),
        out_specs=[hbm] + ([] if last else [vmem]),
        out_shape=[jax.ShapeDtypeStruct((rows, n_dev * shard), jnp.float32)]
        + ([] if last else [jax.ShapeDtypeStruct(params.shape, jnp.float32)]),
        scratch_shapes=[
            pltpu.VMEM((n, rows, width), jnp.float32),
            pltpu.SemaphoreType.DMA((n,)),
        ],
        input_output_aliases={} if first else {n + 1: 0},
        compiler_params=pltpu.CompilerParams(vmem_limit_bytes=24 * 2**20),
        cost_estimate=pl.CostEstimate(
            flops=n * 2 * rows * width * 384,
            bytes_accessed=n * rows * width * 8,
            transcendentals=n * rows * width,
        ),
        name="cdf",
    )(*blocks, params, *(() if first else (out,)))


def solution(mesh):
    n_dev = mesh.shape["vp"]
    assert n_dev == 4

    def swap(a, p):
        return lax.ppermute(a, "vp", [(i, i ^ p) for i in range(n_dev)])

    def local_step(hidden, w_local, inv_temp, target_ids):
        shard = w_local.shape[1]
        early, late, packs = _logits(
            hidden, w_local, inv_temp.reshape(1, -1), target_ids.reshape(1, -1), n_dev
        )
        chunks = [(0, early)]
        begin = early[0].shape[1]
        for made in late:
            got = [made[0]]
            for p in range(1, n_dev):
                got.append(swap(made[p], p))
            chunks.append((begin, got))
            begin += made[0].shape[1]
        params, at_target = _merge(packs)
        out = None
        final = len(chunks) - 1
        plan = [(k, peers) for peers in ((0, 1), (2, 3)) for k in range(final + 1)]
        for i, (k, peers) in enumerate(plan):
            begin, got = chunks[k]
            blocks = [got[p] for p in peers]
            if k < final or peers[0] == 0:
                blocks = [pltpu.with_memory_space_constraint(a, pltpu.HBM) for a in blocks]
            res = _cdf(blocks, peers, params, out, n_dev, shard, begin, i == len(plan) - 1)
            out = res[0]
            params = res[1] if len(res) > 1 else None
        return out, at_target.reshape(-1)

    return jax.shard_map(
        local_step,
        mesh=mesh,
        in_specs=(P("dp", None), P(None, "vp"), P("dp"), P("dp")),
        out_specs=(P(("dp", "vp"), None), P("dp")),
        check_vma=False,
    )
```

```python
import functools

import jax
import jax.numpy as jnp
from jax import lax
from jax.experimental import pallas as pl
from jax.experimental.pallas import tpu as pltpu
from jax.sharding import PartitionSpec as P


LANES = 128
UNIT = 512
HALF = 256
DEPTH = 512
SLOTS = 9
FIRST = 256
EARLY = ((256, 1), (512, 1), (1024, 1), (2048, 3))
LATE = (4096, 2048, 1280, 384)
LATE_UNITS = ((2048, 2), (2048, 1), (1280, 1), (384, 1))
STATS = 4


def _to_rows(vec_1xn):
    n = vec_1xn.shape[1]
    return jnp.transpose(jnp.broadcast_to(vec_1xn, (LANES, n)))


def _peer(me, p):
    return [me, me + 1 - 2 * lax.rem(me, 2), lax.rem(me + 2, 4), 3 - me][p]


def _logits_kernel(cfg, x_ref, w_ref, invt_ref, tgt_ref, *refs):
    n_dev, shard, segments, n_late = cfg
    refs = list(refs)

    def take(n):
        out = refs[:n]
        del refs[:n]
        return out

    early = take(n_dev)
    late = [take(n_dev) for _ in range(n_late)]
    packs = take(n_dev)
    xs, wfirst, wbuf, acc, zsend, zbuf, invt_v, tgt_v, pack_v = take(9)
    scale_rows, left_rows, tmp, m_ref, s_ref, t_ref = take(6)
    first_sem, w_sem, z_sem, x_sem, v_sem, own_sem, send_sem, recv_sem, pack_send, pack_recv = take(10)
    me = lax.axis_index("vp")
    batch, depth = xs.shape
    rows = batch // n_dev
    k_steps = depth // DEPTH
    assert SLOTS == k_steps + 1

    def rows_of(p):
        return pl.ds(pl.multiple_of(_peer(me, p) * rows, rows), rows)

    def fetch_w(seg, step):
        width, col0, g0 = segments[seg][0], segments[seg][3], segments[seg][4]
        slot = lax.rem(g0 + step, SLOTS)
        col = col0 + lax.div(step, k_steps) * width
        row = pl.multiple_of(lax.rem(step, k_steps) * DEPTH, DEPTH)
        return pltpu.make_async_copy(
            w_ref.at[pl.ds(row, DEPTH), pl.ds(pl.multiple_of(col, LANES), width)],
            wbuf.at[slot, :, pl.ds(0, width)],
            w_sem.at[slot],
        )

    def fetch_first(k):
        row = pl.ds(pl.multiple_of(k * DEPTH, DEPTH), DEPTH)
        return pltpu.make_async_copy(w_ref.at[row, pl.ds(0, FIRST)], wfirst.at[row, :], first_sem.at[k])

    def put_late(slot, c, off, width):
        return [
            pltpu.make_async_copy(
                zbuf.at[slot, pl.ds(p * rows, rows), pl.ds(0, width)],
                late[c][p].at[:, pl.ds(off, width)],
                z_sem.at[slot, p],
            )
            for p in range(n_dev)
        ]

    def put_own(u, off, width):
        return pltpu.make_async_copy(
            zsend.at[pl.ds(0, rows), pl.ds(off, width)], early[0].at[:, pl.ds(off, width)], own_sem.at[u]
        )

    def send(u, p, off, width):
        return pltpu.make_async_remote_copy(
            src_ref=zsend.at[pl.ds(p * rows, rows), pl.ds(off, width)],
            dst_ref=early[p].at[:, pl.ds(off, width)],
            send_sem=send_sem.at[u, p],
            recv_sem=recv_sem.at[u, p],
            device_id={"vp": _peer(me, p)},
            device_id_type=pl.DeviceIdType.MESH,
        )

    x_copies = [
        pltpu.make_async_copy(x_ref.at[rows_of(p), :], xs.at[pl.ds(p * rows, rows), :], x_sem.at[p])
        for p in range(n_dev)
    ]
    small = [
        pltpu.make_async_copy(invt_ref, invt_v, v_sem.at[0]),
        pltpu.make_async_copy(tgt_ref, tgt_v, v_sem.at[1]),
    ]
    for copy in small + x_copies[2:]:
        copy.start()
    for k in range(k_steps):
        fetch_first(k).start()
    for copy in x_copies[:2]:
        copy.start()
    for i in range(SLOTS - 1):
        fetch_w(0, jnp.int32(i)).start()
    barrier = pltpu.get_barrier_semaphore()
    for p in range(1, n_dev):
        pl.semaphore_signal(
            barrier, inc=1, device_id={"vp": _peer(me, p)}, device_id_type=pl.DeviceIdType.MESH
        )
    m_ref[...] = jnp.full(m_ref.shape, -jnp.inf, jnp.float32)
    s_ref[...] = jnp.zeros_like(s_ref)
    t_ref[...] = jnp.zeros_like(t_ref)
    for copy in small:
        copy.wait()
    tmp[...] = _to_rows(invt_v[...])
    for p in range(n_dev):
        scale_rows[pl.ds(p * rows, rows), :] = tmp[rows_of(p), :]
    tmp[...] = _to_rows(tgt_v[...].astype(jnp.float32))
    lane = lax.broadcasted_iota(jnp.int32, (rows, LANES), 1)
    for p in range(n_dev):
        left_rows[pl.ds(p * rows, rows), :] = tmp[rows_of(p), :].astype(jnp.int32) - me * shard - lane
    for copy in x_copies[2:]:
        copy.wait()

    def multiply(seg, step):
        width = segments[seg][0]
        slot, k = lax.rem(segments[seg][4] + step, SLOTS), lax.rem(step, k_steps)
        x = xs[:, pl.ds(pl.multiple_of(k * DEPTH, DEPTH), DEPTH)]
        for off in range(0, width, HALF):
            wide = min(HALF, width - off)
            part = jnp.dot(x, wbuf[slot, :, off:off + wide], preferred_element_type=jnp.float32)
            acc[:, off:off + wide] = part + jnp.where(k == 0, 0.0, acc[:, off:off + wide])

    def finish(col, width, out_ref, out_off, lo=0, hi=batch):
        group = 32
        span = next(n for n in (UNIT, HALF, LANES) if width % n == 0)

        def some(j, _):
            at = pl.multiple_of(j * span, span)
            for r in range(lo, hi, group):
                block = slice(r, r + group)
                scale = scale_rows[block, :]
                tiles = []
                for t in range(0, span, LANES):
                    tile = acc[block, pl.ds(at + t, LANES)] * scale
                    out_ref[block, pl.ds(pl.multiple_of(out_off + at + t, LANES), LANES)] = tile
                    tiles.append(tile)
                m_old = m_ref[block, :]
                m_new = functools.reduce(jnp.maximum, tiles, m_old)
                keep = jnp.exp(m_old - m_new)
                total = s_ref[block, :] * keep
                upto = t_ref[block, :] * keep
                left = left_rows[block, :]
                for t, tile in enumerate(tiles):
                    e = jnp.exp(tile - m_new)
                    total += e
                    upto += jnp.where(left >= col + at + t * LANES, e, 0.0)
                m_ref[block, :] = m_new
                s_ref[block, :] = total
                t_ref[block, :] = upto
            return 0

        lax.fori_loop(0, width // span, some, 0)

    sent, own, stored = [], [], []

    def send_early(u, peers, col, width):
        for p in peers:
            copy = send(u, p, col, width)
            copy.start()
            sent.append(copy)

    far = 2 * rows

    def multiply_first(k, lo, hi):
        at = pl.ds(pl.multiple_of(k * DEPTH, DEPTH), DEPTH)
        part = jnp.dot(xs[lo:hi, at], wfirst[at, :], preferred_element_type=jnp.float32)
        acc[lo:hi, :FIRST] = part + jnp.where(k == 0, 0.0, acc[lo:hi, :FIRST])

    def far_step(k, _):
        fetch_first(k).wait()
        multiply_first(k, far, batch)
        return 0

    def near_step(k, _):
        multiply_first(k, 0, far)
        return 0

    lax.fori_loop(0, k_steps, far_step, 0)
    finish(0, FIRST, zsend, 0, far, batch)
    pl.semaphore_wait(barrier, n_dev - 1)
    send_early(0, (2, 3), 0, FIRST)
    for copy in x_copies[:2]:
        copy.wait()
    lax.fori_loop(0, k_steps, near_step, 0)
    finish(0, FIRST, zsend, 0, 0, far)
    send_early(0, (1,), 0, FIRST)
    own.append(put_own(0, 0, FIRST))
    own[0].start()

    for seg, (width, n, chunk, col0, g0) in enumerate(segments):
        for i in range(n):

            def body(k, _, seg=seg, i=i, n=n):
                step = i * k_steps + k
                ahead = step + SLOTS - 1

                @pl.when(ahead < n * k_steps)
                def _():
                    fetch_w(seg, ahead).start()

                if seg + 1 < len(segments):
                    @pl.when(ahead >= n * k_steps)
                    def _():
                        fetch_w(seg + 1, ahead - n * k_steps).start()

                fetch_w(seg, step).wait()
                multiply(seg, step)
                return 0

            lax.fori_loop(0, k_steps, body, 0)
            col = col0 + i * width
            if chunk is None:
                finish(col, width, zsend, col)
                u = len(own)
                send_early(u, (2, 3, 1), col, width)
                copy = put_own(u, col, width)
                copy.start()
                own.append(copy)
            else:
                slot = len(stored) % 2
                if len(stored) >= 2:
                    for copy in stored[-2]:
                        copy.wait()
                finish(col, width, zbuf.at[slot], 0)
                c, off = chunk
                copies = put_late(slot, c, off + i * width, width)
                for copy in copies:
                    copy.start()
                stored.append(copies)
    m = m_ref[...]
    m_row = jnp.max(m, axis=1, keepdims=True)
    keep = jnp.exp(m - m_row)
    s_row = jnp.sum(s_ref[...] * keep, axis=1, keepdims=True)
    t_row = jnp.sum(t_ref[...] * keep, axis=1, keepdims=True)
    which = lax.broadcasted_iota(jnp.int32, m.shape, 1)
    packed = jnp.where(which == 0, m_row, jnp.where(which == 1, s_row, t_row))
    for p in range(n_dev):
        tmp[rows_of(p), :] = packed[p * rows:(p + 1) * rows, :]
    pack_v[...] = jnp.transpose(tmp[...])[:STATS, :]
    for p in (2, 3, 1):
        copy = pltpu.make_async_remote_copy(
            src_ref=pack_v,
            dst_ref=packs[p],
            send_sem=pack_send.at[p],
            recv_sem=pack_recv.at[p],
            device_id={"vp": _peer(me, p)},
            device_id_type=pl.DeviceIdType.MESH,
        )
        copy.start()
        sent.append(copy)
    copy = pltpu.make_async_copy(pack_v, packs[0], pack_send.at[0])
    copy.start()
    own.append(copy)
    for copies in stored[-2:]:
        for copy in copies:
            copy.wait()
    for copy in own + sent:
        copy.wait()


def _logits(x, w, invt, tgt, n_dev):
    batch, depth = x.shape
    shard = w.shape[1]
    rows = batch // n_dev
    segments, col, g0 = [], FIRST, 0
    chunk_of = {}
    sent = begin = FIRST + sum(width * n for width, n in EARLY)
    for c, width in enumerate(LATE):
        chunk_of.update({begin + i: (c, i) for i in range(0, width, LANES)})
        begin += width
    for i, (width, n) in enumerate(EARLY + LATE_UNITS):
        segments.append((width, n, None if i < len(EARLY) else chunk_of[col], col, g0))
        col += width * n
        g0 += n * (depth // DEPTH)
    assert col == shard == begin
    n_early = 1 + sum(n for _, n in EARLY)
    hbm = pl.BlockSpec(memory_space=pltpu.HBM)
    out_shape = [pltpu.HBM((rows, sent), jnp.float32)] * n_dev
    out_shape += [pltpu.HBM((rows, width), jnp.float32) for width in LATE for _ in range(n_dev)]
    out_shape += [pltpu.HBM((STATS, batch), jnp.float32)] * n_dev
    table = pltpu.VMEM((batch, LANES), jnp.float32)
    widest = max(width for width, _ in EARLY + LATE_UNITS)
    dma = pltpu.SemaphoreType.DMA
    res = pl.pallas_call(
        functools.partial(_logits_kernel, (n_dev, shard, segments, len(LATE))),
        in_specs=[hbm] * 4,
        out_specs=[hbm] * len(out_shape),
        out_shape=out_shape,
        scratch_shapes=[
            pltpu.VMEM((batch, depth), jnp.bfloat16),
            pltpu.VMEM((depth, FIRST), jnp.bfloat16),
            pltpu.VMEM((SLOTS, DEPTH, widest), jnp.bfloat16),
            pltpu.VMEM((batch, widest), jnp.float32),
            pltpu.VMEM((batch, sent), jnp.float32),
            pltpu.VMEM((2, batch, widest), jnp.float32),
            pltpu.VMEM((1, batch), jnp.float32),
            pltpu.VMEM((1, batch), jnp.int32),
            pltpu.VMEM((STATS, batch), jnp.float32),
            table,
            pltpu.VMEM((batch, LANES), jnp.int32),
            table,
            table,
            table,
            table,
            dma((depth // DEPTH,)),
            dma((SLOTS,)),
            dma((2, n_dev)),
            dma((n_dev,)),
            dma((2,)),
            dma((n_early,)),
            dma((n_early, n_dev)),
            dma((n_early, n_dev)),
            dma((n_dev,)),
            dma((n_dev,)),
        ],
        compiler_params=pltpu.CompilerParams(
            collective_id=0, has_side_effects=True, vmem_limit_bytes=52 * 2**20
        ),
        cost_estimate=pl.CostEstimate(
            flops=2 * batch * depth * shard,
            bytes_accessed=2 * depth * shard,
            transcendentals=batch * shard,
        ),
        name="logits",
    )(*(pltpu.with_memory_space_constraint(a, pltpu.HBM) for a in (x, w, invt, tgt)))
    blocks = [res[c * n_dev:(c + 1) * n_dev] for c in range(len(LATE) + 2)]
    return blocks[0], blocks[1:-1], blocks[-1]


def _merge_kernel(n_dev, *refs):
    stats, (params_ref, at_ref) = refs[:n_dev], refs[n_dev:]
    me = lax.axis_index("vp")
    batch = stats[0].shape[1]
    rows = batch // n_dev
    ms = [s[0:1, :] for s in stats]
    top = functools.reduce(jnp.maximum, ms)
    keep = [jnp.exp(m - top) for m in ms]
    mass = [s[1:2, :] * k for s, k in zip(stats, keep)]
    upto = sum(s[2:3, :] * k for s, k in zip(stats, keep))
    total = sum(mass)
    at_ref[...] = upto / total
    values = [top, 1.0 / total]
    for p in range(n_dev):
        start = jnp.zeros_like(total)
        for q in range(n_dev):
            start += jnp.where((me ^ q) < (me ^ p), mass[q], 0.0)
        values.append(start)
    which = lax.broadcasted_iota(jnp.int32, (LANES, batch), 0)
    table = jnp.zeros((LANES, batch), jnp.float32)
    for i, v in enumerate(values):
        table = jnp.where(which == i, v, table)
    per_row = jnp.transpose(table)
    out = jnp.zeros((rows, LANES), jnp.float32)
    for d in range(n_dev):
        out = jnp.where(me == d, per_row[d * rows:(d + 1) * rows, :], out)
    params_ref[...] = out


def _merge(stats):
    n_dev = len(stats)
    batch = stats[0].shape[1]
    vmem = pl.BlockSpec(memory_space=pltpu.VMEM)
    return pl.pallas_call(
        functools.partial(_merge_kernel, n_dev),
        in_specs=[vmem] * n_dev,
        out_specs=[vmem] * 2,
        out_shape=[
            jax.ShapeDtypeStruct((batch // n_dev, LANES), jnp.float32),
            jax.ShapeDtypeStruct((1, batch), jnp.float32),
        ],
        cost_estimate=pl.CostEstimate(flops=100_000, bytes_accessed=100_000, transcendentals=1000),
        name="merge",
    )(*stats)


def _cdf_kernel(cfg, *refs):
    peers, shard, base, width, first, last = cfg
    n = len(peers)
    params_ref = refs[n]
    if last:
        out_ref, y_ref, sems = refs[n + 2:]
    else:
        out_ref, params_out, y_ref, sems = refs[n + (1 if first else 2):]
    me = lax.axis_index("vp")
    rows = params_ref.shape[0]
    params = params_ref[...]
    top = jnp.broadcast_to(params[:, 0:1], (rows, LANES))
    inv = jnp.broadcast_to(params[:, 1:2], (rows, LANES))
    k_id = lax.broadcasted_iota(jnp.int32, (3 * LANES, 2 * LANES), 0) % LANES
    n_id = lax.broadcasted_iota(jnp.int32, (3 * LANES, 2 * LANES), 1)
    tri = jnp.where(k_id <= n_id, 1.0, 0.0).astype(jnp.bfloat16)
    lane = lax.broadcasted_iota(jnp.int32, (rows, LANES), 1)

    def unit(col, wide, carries):
        ends = []
        for j in range(n):
            cols = [pl.ds(col + t, LANES) for t in range(0, wide, LANES)]
            e = jnp.concatenate([jnp.exp(refs[j][:, c] - top) for c in cols], axis=0)
            hi = e.astype(jnp.bfloat16)
            r1 = e - hi.astype(jnp.float32)
            mid = r1.astype(jnp.bfloat16)
            lo = (r1 - mid.astype(jnp.float32)).astype(jnp.bfloat16)
            sums = jnp.dot(jnp.concatenate([hi, mid, lo], axis=1), tri, preferred_element_type=jnp.float32)
            carry = carries[j]
            for t, c in enumerate(cols):
                block = slice(t * rows, (t + 1) * rows)
                y_ref[j, :, c] = (sums[block, :LANES] + carry) * inv
                carry = carry + sums[block, LANES:]
            ends.append(carry)
        return tuple(ends)

    carries = tuple(jnp.broadcast_to(params[:, 2 + p:3 + p], (rows, LANES)) for p in peers)
    n_full = width // UNIT
    if n_full:
        carries = lax.fori_loop(
            0, n_full, lambda u, c: unit(pl.multiple_of(u * UNIT, UNIT), UNIT, c), carries
        )
    if width % UNIT:
        carries = unit(n_full * UNIT, width % UNIT, carries)
    copies = []
    updated = params
    for j, p in enumerate(peers):
        where = pl.multiple_of((me ^ p) * shard + base, LANES)
        copy = pltpu.make_async_copy(y_ref.at[j], out_ref.at[:, pl.ds(where, width)], sems.at[j])
        copy.start()
        copies.append(copy)
        updated = jnp.where(lane == 2 + p, carries[j], updated)
    if not last:
        params_out[...] = updated
    for copy in copies:
        copy.wait()


def _cdf(blocks, peers, params, out, n_dev, shard, base, last=False):
    rows, width = blocks[0].shape
    n = len(peers)
    first = out is None
    vmem = pl.BlockSpec(memory_space=pltpu.VMEM)
    hbm = pl.BlockSpec(memory_space=pl.ANY)
    return pl.pallas_call(
        functools.partial(_cdf_kernel, (peers, shard, base, width, first, last)),
        in_specs=[vmem] * (n + 1) + ([] if first else [hbm]),
        out_specs=[hbm] + ([] if last else [vmem]),
        out_shape=[jax.ShapeDtypeStruct((rows, n_dev * shard), jnp.float32)]
        + ([] if last else [jax.ShapeDtypeStruct(params.shape, jnp.float32)]),
        scratch_shapes=[
            pltpu.VMEM((n, rows, width), jnp.float32),
            pltpu.SemaphoreType.DMA((n,)),
        ],
        input_output_aliases={} if first else {n + 1: 0},
        compiler_params=pltpu.CompilerParams(vmem_limit_bytes=24 * 2**20),
        cost_estimate=pl.CostEstimate(
            flops=n * 2 * rows * width * 384,
            bytes_accessed=n * rows * width * 8,
            transcendentals=n * rows * width,
        ),
        name="cdf",
    )(*blocks, params, *(() if first else (out,)))


def solution(mesh):
    n_dev = mesh.shape["vp"]
    assert n_dev == 4

    def swap(a, p):
        return lax.ppermute(a, "vp", [(i, i ^ p) for i in range(n_dev)])

    def local_step(hidden, w_local, inv_temp, target_ids):
        shard = w_local.shape[1]
        early, late, packs = _logits(
            hidden, w_local, inv_temp.reshape(1, -1), target_ids.reshape(1, -1), n_dev
        )
        chunks = [(0, early)]
        begin = early[0].shape[1]
        for made in late:
            got = [made[0]]
            for p in range(1, n_dev):
                got.append(swap(made[p], p))
            chunks.append((begin, got))
            begin += made[0].shape[1]
        params, at_target = _merge(packs)
        out = None
        final = len(chunks) - 1
        plan = [(k, peers) for peers in ((0, 1), (2, 3)) for k in range(final + 1)]
        for i, (k, peers) in enumerate(plan):
            begin, got = chunks[k]
            blocks = [got[p] for p in peers]
            if k < final or peers[0] == 0:
                blocks = [pltpu.with_memory_space_constraint(a, pltpu.HBM) for a in blocks]
            res = _cdf(blocks, peers, params, out, n_dev, shard, begin, i == len(plan) - 1)
            out = res[0]
            params = res[1] if len(res) > 1 else None
        return out, at_target.reshape(-1)

    return jax.shard_map(
        local_step,
        mesh=mesh,
        in_specs=(P("dp", None), P(None, "vp"), P("dp"), P("dp")),
        out_specs=(P(("dp", "vp"), None), P("dp")),
        check_vma=False,
    )
```

```python
import functools

import jax
import jax.numpy as jnp
from jax import lax
from jax.experimental import pallas as pl
from jax.experimental.pallas import tpu as pltpu
from jax.sharding import PartitionSpec as P


LANES = 128
UNIT = 512
HALF = 256
DEPTH = 512
SLOTS = 9
FIRST = 256
EARLY = ((256, 1), (512, 1), (1024, 1), (2048, 3))
LATE = (4096, 2048, 1280, 384)
LATE_UNITS = ((2048, 2), (2048, 1), (1280, 1), (384, 1))
STATS = 4


def _to_rows(vec_1xn):
    n = vec_1xn.shape[1]
    return jnp.transpose(jnp.broadcast_to(vec_1xn, (LANES, n)))


def _peer(me, p):
    return [me, me + 1 - 2 * lax.rem(me, 2), lax.rem(me + 2, 4), 3 - me][p]


def _logits_kernel(cfg, x_ref, w_ref, invt_ref, tgt_ref, *refs):
    n_dev, shard, segments, n_late = cfg
    refs = list(refs)

    def take(n):
        out = refs[:n]
        del refs[:n]
        return out

    early = take(n_dev)
    late = [take(n_dev) for _ in range(n_late)]
    packs = take(n_dev)
    xs, wfirst, wbuf, acc, zsend, zbuf, invt_v, tgt_v, pack_v = take(9)
    scale_rows, left_rows, tmp, m_ref, s_ref, t_ref = take(6)
    first_sem, w_sem, z_sem, x_sem, v_sem, own_sem, send_sem, recv_sem, pack_send, pack_recv = take(10)
    me = lax.axis_index("vp")
    batch, depth = xs.shape
    rows = batch // n_dev
    k_steps = depth // DEPTH
    assert SLOTS == k_steps + 1

    def rows_of(p):
        return pl.ds(pl.multiple_of(_peer(me, p) * rows, rows), rows)

    def fetch_w(seg, step):
        width, col0, g0 = segments[seg][0], segments[seg][3], segments[seg][4]
        slot = lax.rem(g0 + step, SLOTS)
        col = col0 + lax.div(step, k_steps) * width
        row = pl.multiple_of(lax.rem(step, k_steps) * DEPTH, DEPTH)
        return pltpu.make_async_copy(
            w_ref.at[pl.ds(row, DEPTH), pl.ds(pl.multiple_of(col, LANES), width)],
            wbuf.at[slot, :, pl.ds(0, width)],
            w_sem.at[slot],
        )

    def fetch_first(k):
        row = pl.ds(pl.multiple_of(k * DEPTH, DEPTH), DEPTH)
        return pltpu.make_async_copy(w_ref.at[row, pl.ds(0, FIRST)], wfirst.at[row, :], first_sem.at[k])

    def put_late(slot, c, off, width):
        return [
            pltpu.make_async_copy(
                zbuf.at[slot, pl.ds(p * rows, rows), pl.ds(0, width)],
                late[c][p].at[:, pl.ds(off, width)],
                z_sem.at[slot, p],
            )
            for p in range(n_dev)
        ]

    def put_own(u, off, width):
        return pltpu.make_async_copy(
            zsend.at[pl.ds(0, rows), pl.ds(off, width)], early[0].at[:, pl.ds(off, width)], own_sem.at[u]
        )

    def send(u, p, off, width):
        return pltpu.make_async_remote_copy(
            src_ref=zsend.at[pl.ds(p * rows, rows), pl.ds(off, width)],
            dst_ref=early[p].at[:, pl.ds(off, width)],
            send_sem=send_sem.at[u, p],
            recv_sem=recv_sem.at[u, p],
            device_id={"vp": _peer(me, p)},
            device_id_type=pl.DeviceIdType.MESH,
        )

    x_copies = [
        pltpu.make_async_copy(x_ref.at[rows_of(p), :], xs.at[pl.ds(p * rows, rows), :], x_sem.at[p])
        for p in range(n_dev)
    ]
    small = [
        pltpu.make_async_copy(invt_ref, invt_v, v_sem.at[0]),
        pltpu.make_async_copy(tgt_ref, tgt_v, v_sem.at[1]),
    ]
    for copy in small + x_copies[2:]:
        copy.start()
    for k in range(k_steps):
        fetch_first(k).start()
    barrier = pltpu.get_barrier_semaphore()
    for p in range(1, n_dev):
        pl.semaphore_signal(
            barrier, inc=1, device_id={"vp": _peer(me, p)}, device_id_type=pl.DeviceIdType.MESH
        )
    m_ref[...] = jnp.full(m_ref.shape, -jnp.inf, jnp.float32)
    s_ref[...] = jnp.zeros_like(s_ref)
    t_ref[...] = jnp.zeros_like(t_ref)
    for copy in small:
        copy.wait()
    tmp[...] = _to_rows(invt_v[...])
    for p in range(n_dev):
        scale_rows[pl.ds(p * rows, rows), :] = tmp[rows_of(p), :]
    tmp[...] = _to_rows(tgt_v[...].astype(jnp.float32))
    lane = lax.broadcasted_iota(jnp.int32, (rows, LANES), 1)
    for p in range(n_dev):
        left_rows[pl.ds(p * rows, rows), :] = tmp[rows_of(p), :].astype(jnp.int32) - me * shard - lane
    for copy in x_copies[2:]:
        copy.wait()

    def multiply(seg, step):
        width = segments[seg][0]
        slot, k = lax.rem(segments[seg][4] + step, SLOTS), lax.rem(step, k_steps)
        x = xs[:, pl.ds(pl.multiple_of(k * DEPTH, DEPTH), DEPTH)]
        for off in range(0, width, HALF):
            wide = min(HALF, width - off)
            part = jnp.dot(x, wbuf[slot, :, off:off + wide], preferred_element_type=jnp.float32)
            acc[:, off:off + wide] = part + jnp.where(k == 0, 0.0, acc[:, off:off + wide])

    def finish(col, width, out_ref, out_off, lo=0, hi=batch):
        group = 32
        span = next(n for n in (UNIT, HALF, LANES) if width % n == 0)

        def some(j, _):
            at = pl.multiple_of(j * span, span)
            for r in range(lo, hi, group):
                block = slice(r, r + group)
                scale = scale_rows[block, :]
                tiles = []
                for t in range(0, span, LANES):
                    tile = acc[block, pl.ds(at + t, LANES)] * scale
                    out_ref[block, pl.ds(pl.multiple_of(out_off + at + t, LANES), LANES)] = tile
                    tiles.append(tile)
                m_old = m_ref[block, :]
                m_new = functools.reduce(jnp.maximum, tiles, m_old)
                keep = jnp.exp(m_old - m_new)
                total = s_ref[block, :] * keep
                upto = t_ref[block, :] * keep
                left = left_rows[block, :]
                for t, tile in enumerate(tiles):
                    e = jnp.exp(tile - m_new)
                    total += e
                    upto += jnp.where(left >= col + at + t * LANES, e, 0.0)
                m_ref[block, :] = m_new
                s_ref[block, :] = total
                t_ref[block, :] = upto
            return 0

        lax.fori_loop(0, width // span, some, 0)

    sent, own, stored = [], [], []

    def send_early(u, peers, col, width):
        for p in peers:
            copy = send(u, p, col, width)
            copy.start()
            sent.append(copy)

    far = 2 * rows

    def multiply_first(k, lo, hi):
        at = pl.ds(pl.multiple_of(k * DEPTH, DEPTH), DEPTH)
        part = jnp.dot(xs[lo:hi, at], wfirst[at, :], preferred_element_type=jnp.float32)
        acc[lo:hi, :FIRST] = part + jnp.where(k == 0, 0.0, acc[lo:hi, :FIRST])

    def far_step(k, _):
        fetch_first(k).wait()

        @pl.when(k == 0)
        def _():
            for copy in x_copies[:2]:
                copy.start()

        fetch_w(0, k).start()
        multiply_first(k, far, batch)
        return 0

    def near_step(k, _):
        multiply_first(k, 0, far)
        return 0

    lax.fori_loop(0, k_steps, far_step, 0)
    finish(0, FIRST, zsend, 0, far, batch)
    pl.semaphore_wait(barrier, n_dev - 1)
    send_early(0, (2, 3), 0, FIRST)
    for copy in x_copies[:2]:
        copy.wait()
    lax.fori_loop(0, k_steps, near_step, 0)
    finish(0, FIRST, zsend, 0, 0, far)
    send_early(0, (1,), 0, FIRST)
    own.append(put_own(0, 0, FIRST))
    own[0].start()

    for seg, (width, n, chunk, col0, g0) in enumerate(segments):
        for i in range(n):

            def body(k, _, seg=seg, i=i, n=n):
                step = i * k_steps + k
                ahead = step + SLOTS - 1

                @pl.when(ahead < n * k_steps)
                def _():
                    fetch_w(seg, ahead).start()

                if seg + 1 < len(segments):
                    @pl.when(ahead >= n * k_steps)
                    def _():
                        fetch_w(seg + 1, ahead - n * k_steps).start()

                fetch_w(seg, step).wait()
                multiply(seg, step)
                return 0

            lax.fori_loop(0, k_steps, body, 0)
            col = col0 + i * width
            if chunk is None:
                finish(col, width, zsend, col)
                u = len(own)
                send_early(u, (2, 3, 1), col, width)
                copy = put_own(u, col, width)
                copy.start()
                own.append(copy)
            else:
                slot = len(stored) % 2
                if len(stored) >= 2:
                    for copy in stored[-2]:
                        copy.wait()
                finish(col, width, zbuf.at[slot], 0)
                c, off = chunk
                copies = put_late(slot, c, off + i * width, width)
                for copy in copies:
                    copy.start()
                stored.append(copies)
    m = m_ref[...]
    m_row = jnp.max(m, axis=1, keepdims=True)
    keep = jnp.exp(m - m_row)
    s_row = jnp.sum(s_ref[...] * keep, axis=1, keepdims=True)
    t_row = jnp.sum(t_ref[...] * keep, axis=1, keepdims=True)
    which = lax.broadcasted_iota(jnp.int32, m.shape, 1)
    packed = jnp.where(which == 0, m_row, jnp.where(which == 1, s_row, t_row))
    for p in range(n_dev):
        tmp[rows_of(p), :] = packed[p * rows:(p + 1) * rows, :]
    pack_v[...] = jnp.transpose(tmp[...])[:STATS, :]
    for p in (2, 3, 1):
        copy = pltpu.make_async_remote_copy(
            src_ref=pack_v,
            dst_ref=packs[p],
            send_sem=pack_send.at[p],
            recv_sem=pack_recv.at[p],
            device_id={"vp": _peer(me, p)},
            device_id_type=pl.DeviceIdType.MESH,
        )
        copy.start()
        sent.append(copy)
    copy = pltpu.make_async_copy(pack_v, packs[0], pack_send.at[0])
    copy.start()
    own.append(copy)
    for copies in stored[-2:]:
        for copy in copies:
            copy.wait()
    for copy in own + sent:
        copy.wait()


def _logits(x, w, invt, tgt, n_dev):
    batch, depth = x.shape
    shard = w.shape[1]
    rows = batch // n_dev
    segments, col, g0 = [], FIRST, 0
    chunk_of = {}
    sent = begin = FIRST + sum(width * n for width, n in EARLY)
    for c, width in enumerate(LATE):
        chunk_of.update({begin + i: (c, i) for i in range(0, width, LANES)})
        begin += width
    for i, (width, n) in enumerate(EARLY + LATE_UNITS):
        segments.append((width, n, None if i < len(EARLY) else chunk_of[col], col, g0))
        col += width * n
        g0 += n * (depth // DEPTH)
    assert col == shard == begin
    n_early = 1 + sum(n for _, n in EARLY)
    hbm = pl.BlockSpec(memory_space=pltpu.HBM)
    out_shape = [pltpu.HBM((rows, sent), jnp.float32)] * n_dev
    out_shape += [pltpu.HBM((rows, width), jnp.float32) for width in LATE for _ in range(n_dev)]
    out_shape += [pltpu.HBM((STATS, batch), jnp.float32)] * n_dev
    table = pltpu.VMEM((batch, LANES), jnp.float32)
    widest = max(width for width, _ in EARLY + LATE_UNITS)
    dma = pltpu.SemaphoreType.DMA
    res = pl.pallas_call(
        functools.partial(_logits_kernel, (n_dev, shard, segments, len(LATE))),
        in_specs=[hbm] * 4,
        out_specs=[hbm] * len(out_shape),
        out_shape=out_shape,
        scratch_shapes=[
            pltpu.VMEM((batch, depth), jnp.bfloat16),
            pltpu.VMEM((depth, FIRST), jnp.bfloat16),
            pltpu.VMEM((SLOTS, DEPTH, widest), jnp.bfloat16),
            pltpu.VMEM((batch, widest), jnp.float32),
            pltpu.VMEM((batch, sent), jnp.float32),
            pltpu.VMEM((2, batch, widest), jnp.float32),
            pltpu.VMEM((1, batch), jnp.float32),
            pltpu.VMEM((1, batch), jnp.int32),
            pltpu.VMEM((STATS, batch), jnp.float32),
            table,
            pltpu.VMEM((batch, LANES), jnp.int32),
            table,
            table,
            table,
            table,
            dma((depth // DEPTH,)),
            dma((SLOTS,)),
            dma((2, n_dev)),
            dma((n_dev,)),
            dma((2,)),
            dma((n_early,)),
            dma((n_early, n_dev)),
            dma((n_early, n_dev)),
            dma((n_dev,)),
            dma((n_dev,)),
        ],
        compiler_params=pltpu.CompilerParams(
            collective_id=0, has_side_effects=True, vmem_limit_bytes=52 * 2**20
        ),
        cost_estimate=pl.CostEstimate(
            flops=2 * batch * depth * shard,
            bytes_accessed=2 * depth * shard,
            transcendentals=batch * shard,
        ),
        name="logits",
    )(*(pltpu.with_memory_space_constraint(a, pltpu.HBM) for a in (x, w, invt, tgt)))
    blocks = [res[c * n_dev:(c + 1) * n_dev] for c in range(len(LATE) + 2)]
    return blocks[0], blocks[1:-1], blocks[-1]


def _merge_kernel(n_dev, *refs):
    stats, (params_ref, at_ref) = refs[:n_dev], refs[n_dev:]
    me = lax.axis_index("vp")
    batch = stats[0].shape[1]
    rows = batch // n_dev
    ms = [s[0:1, :] for s in stats]
    top = functools.reduce(jnp.maximum, ms)
    keep = [jnp.exp(m - top) for m in ms]
    mass = [s[1:2, :] * k for s, k in zip(stats, keep)]
    upto = sum(s[2:3, :] * k for s, k in zip(stats, keep))
    total = sum(mass)
    at_ref[...] = upto / total
    values = [top, 1.0 / total]
    for p in range(n_dev):
        start = jnp.zeros_like(total)
        for q in range(n_dev):
            start += jnp.where((me ^ q) < (me ^ p), mass[q], 0.0)
        values.append(start)
    which = lax.broadcasted_iota(jnp.int32, (LANES, batch), 0)
    table = jnp.zeros((LANES, batch), jnp.float32)
    for i, v in enumerate(values):
        table = jnp.where(which == i, v, table)
    per_row = jnp.transpose(table)
    out = jnp.zeros((rows, LANES), jnp.float32)
    for d in range(n_dev):
        out = jnp.where(me == d, per_row[d * rows:(d + 1) * rows, :], out)
    params_ref[...] = out


def _merge(stats):
    n_dev = len(stats)
    batch = stats[0].shape[1]
    vmem = pl.BlockSpec(memory_space=pltpu.VMEM)
    return pl.pallas_call(
        functools.partial(_merge_kernel, n_dev),
        in_specs=[vmem] * n_dev,
        out_specs=[vmem] * 2,
        out_shape=[
            jax.ShapeDtypeStruct((batch // n_dev, LANES), jnp.float32),
            jax.ShapeDtypeStruct((1, batch), jnp.float32),
        ],
        cost_estimate=pl.CostEstimate(flops=100_000, bytes_accessed=100_000, transcendentals=1000),
        name="merge",
    )(*stats)


def _cdf_kernel(cfg, *refs):
    peers, shard, base, width, first, last = cfg
    n = len(peers)
    params_ref = refs[n]
    if last:
        out_ref, y_ref, sems = refs[n + 2:]
    else:
        out_ref, params_out, y_ref, sems = refs[n + (1 if first else 2):]
    me = lax.axis_index("vp")
    rows = params_ref.shape[0]
    params = params_ref[...]
    top = jnp.broadcast_to(params[:, 0:1], (rows, LANES))
    inv = jnp.broadcast_to(params[:, 1:2], (rows, LANES))
    k_id = lax.broadcasted_iota(jnp.int32, (3 * LANES, 2 * LANES), 0) % LANES
    n_id = lax.broadcasted_iota(jnp.int32, (3 * LANES, 2 * LANES), 1)
    tri = jnp.where(k_id <= n_id, 1.0, 0.0).astype(jnp.bfloat16)
    lane = lax.broadcasted_iota(jnp.int32, (rows, LANES), 1)

    def unit(col, wide, carries):
        ends = []
        for j in range(n):
            cols = [pl.ds(col + t, LANES) for t in range(0, wide, LANES)]
            e = jnp.concatenate([jnp.exp(refs[j][:, c] - top) for c in cols], axis=0)
            hi = e.astype(jnp.bfloat16)
            r1 = e - hi.astype(jnp.float32)
            mid = r1.astype(jnp.bfloat16)
            lo = (r1 - mid.astype(jnp.float32)).astype(jnp.bfloat16)
            sums = jnp.dot(jnp.concatenate([hi, mid, lo], axis=1), tri, preferred_element_type=jnp.float32)
            carry = carries[j]
            for t, c in enumerate(cols):
                block = slice(t * rows, (t + 1) * rows)
                y_ref[j, :, c] = (sums[block, :LANES] + carry) * inv
                carry = carry + sums[block, LANES:]
            ends.append(carry)
        return tuple(ends)

    carries = tuple(jnp.broadcast_to(params[:, 2 + p:3 + p], (rows, LANES)) for p in peers)
    n_full = width // UNIT
    if n_full:
        carries = lax.fori_loop(
            0, n_full, lambda u, c: unit(pl.multiple_of(u * UNIT, UNIT), UNIT, c), carries
        )
    if width % UNIT:
        carries = unit(n_full * UNIT, width % UNIT, carries)
    copies = []
    updated = params
    for j, p in enumerate(peers):
        where = pl.multiple_of((me ^ p) * shard + base, LANES)
        copy = pltpu.make_async_copy(y_ref.at[j], out_ref.at[:, pl.ds(where, width)], sems.at[j])
        copy.start()
        copies.append(copy)
        updated = jnp.where(lane == 2 + p, carries[j], updated)
    if not last:
        params_out[...] = updated
    for copy in copies:
        copy.wait()


def _cdf(blocks, peers, params, out, n_dev, shard, base, last=False):
    rows, width = blocks[0].shape
    n = len(peers)
    first = out is None
    vmem = pl.BlockSpec(memory_space=pltpu.VMEM)
    hbm = pl.BlockSpec(memory_space=pl.ANY)
    return pl.pallas_call(
        functools.partial(_cdf_kernel, (peers, shard, base, width, first, last)),
        in_specs=[vmem] * (n + 1) + ([] if first else [hbm]),
        out_specs=[hbm] + ([] if last else [vmem]),
        out_shape=[jax.ShapeDtypeStruct((rows, n_dev * shard), jnp.float32)]
        + ([] if last else [jax.ShapeDtypeStruct(params.shape, jnp.float32)]),
        scratch_shapes=[
            pltpu.VMEM((n, rows, width), jnp.float32),
            pltpu.SemaphoreType.DMA((n,)),
        ],
        input_output_aliases={} if first else {n + 1: 0},
        compiler_params=pltpu.CompilerParams(vmem_limit_bytes=24 * 2**20),
        cost_estimate=pl.CostEstimate(
            flops=n * 2 * rows * width * 384,
            bytes_accessed=n * rows * width * 8,
            transcendentals=n * rows * width,
        ),
        name="cdf",
    )(*blocks, params, *(() if first else (out,)))


def solution(mesh):
    n_dev = mesh.shape["vp"]
    assert n_dev == 4

    def swap(a, p):
        return lax.ppermute(a, "vp", [(i, i ^ p) for i in range(n_dev)])

    def local_step(hidden, w_local, inv_temp, target_ids):
        shard = w_local.shape[1]
        early, late, packs = _logits(
            hidden, w_local, inv_temp.reshape(1, -1), target_ids.reshape(1, -1), n_dev
        )
        chunks = [(0, early)]
        begin = early[0].shape[1]
        for made in late:
            got = [made[0]]
            for p in range(1, n_dev):
                got.append(swap(made[p], p))
            chunks.append((begin, got))
            begin += made[0].shape[1]
        params, at_target = _merge(packs)
        out = None
        final = len(chunks) - 1
        plan = [(k, peers) for peers in ((0, 1), (2, 3)) for k in range(final + 1)]
        for i, (k, peers) in enumerate(plan):
            begin, got = chunks[k]
            blocks = [got[p] for p in peers]
            if k < final or peers[0] == 0:
                blocks = [pltpu.with_memory_space_constraint(a, pltpu.HBM) for a in blocks]
            res = _cdf(blocks, peers, params, out, n_dev, shard, begin, i == len(plan) - 1)
            out = res[0]
            params = res[1] if len(res) > 1 else None
        return out, at_target.reshape(-1)

    return jax.shard_map(
        local_step,
        mesh=mesh,
        in_specs=(P("dp", None), P(None, "vp"), P("dp"), P("dp")),
        out_specs=(P(("dp", "vp"), None), P("dp")),
        check_vma=False,
    )
```

```python
import functools

import jax
import jax.numpy as jnp
from jax import lax
from jax.experimental import pallas as pl
from jax.experimental.pallas import tpu as pltpu
from jax.sharding import PartitionSpec as P


LANES = 128
UNIT = 512
HALF = 256
DEPTH = 512
SLOTS = 9
FIRST = 256
EARLY = ((256, 1), (512, 1), (1024, 1), (2048, 3))
URGENT = 2
LATE = (4096, 2048, 1280, 384)
LATE_UNITS = ((2048, 2), (2048, 1), (1280, 1), (384, 1))
STATS = 4


def _to_rows(vec_1xn):
    n = vec_1xn.shape[1]
    return jnp.transpose(jnp.broadcast_to(vec_1xn, (LANES, n)))


def _peer(me, p):
    return [me, me + 1 - 2 * lax.rem(me, 2), lax.rem(me + 2, 4), 3 - me][p]


def _logits_kernel(cfg, x_ref, w_ref, invt_ref, tgt_ref, *refs):
    n_dev, shard, segments, n_late = cfg
    refs = list(refs)

    def take(n):
        out = refs[:n]
        del refs[:n]
        return out

    early = take(n_dev)
    late = [take(n_dev) for _ in range(n_late)]
    packs = take(n_dev)
    xs, wfirst, wbuf, acc, zsend, zbuf, invt_v, tgt_v, pack_v = take(9)
    scale_rows, left_rows, tmp, m_ref, s_ref, t_ref = take(6)
    first_sem, w_sem, z_sem, x_sem, v_sem, own_sem, send_sem, recv_sem, pack_send, pack_recv = take(10)
    me = lax.axis_index("vp")
    batch, depth = xs.shape
    rows = batch // n_dev
    k_steps = depth // DEPTH
    assert SLOTS == k_steps + 1 and all(n == 1 for _, n in EARLY[:URGENT])

    def rows_of(p):
        return pl.ds(pl.multiple_of(_peer(me, p) * rows, rows), rows)

    def fetch_w(seg, step):
        width, col0, g0 = segments[seg][0], segments[seg][3], segments[seg][4]
        slot = lax.rem(g0 + step, SLOTS)
        col = col0 + lax.div(step, k_steps) * width
        row = pl.multiple_of(lax.rem(step, k_steps) * DEPTH, DEPTH)
        return pltpu.make_async_copy(
            w_ref.at[pl.ds(row, DEPTH), pl.ds(pl.multiple_of(col, LANES), width)],
            wbuf.at[slot, :, pl.ds(0, width)],
            w_sem.at[slot],
        )

    def fetch_first(k):
        row = pl.ds(pl.multiple_of(k * DEPTH, DEPTH), DEPTH)
        return pltpu.make_async_copy(w_ref.at[row, pl.ds(0, FIRST)], wfirst.at[row, :], first_sem.at[k])

    def put_late(slot, c, off, width):
        return [
            pltpu.make_async_copy(
                zbuf.at[slot, pl.ds(p * rows, rows), pl.ds(0, width)],
                late[c][p].at[:, pl.ds(off, width)],
                z_sem.at[slot, p],
            )
            for p in range(n_dev)
        ]

    def put_own(u, off, width):
        return pltpu.make_async_copy(
            zsend.at[pl.ds(0, rows), pl.ds(off, width)], early[0].at[:, pl.ds(off, width)], own_sem.at[u]
        )

    def send(u, p, off, width):
        return pltpu.make_async_remote_copy(
            src_ref=zsend.at[pl.ds(p * rows, rows), pl.ds(off, width)],
            dst_ref=early[p].at[:, pl.ds(off, width)],
            send_sem=send_sem.at[u, p],
            recv_sem=recv_sem.at[u, p],
            device_id={"vp": _peer(me, p)},
            device_id_type=pl.DeviceIdType.MESH,
        )

    x_copies = [
        pltpu.make_async_copy(x_ref.at[rows_of(p), :], xs.at[pl.ds(p * rows, rows), :], x_sem.at[p])
        for p in range(n_dev)
    ]
    small = [
        pltpu.make_async_copy(invt_ref, invt_v, v_sem.at[0]),
        pltpu.make_async_copy(tgt_ref, tgt_v, v_sem.at[1]),
    ]
    for copy in small + x_copies[2:]:
        copy.start()
    for k in range(k_steps):
        fetch_first(k).start()
    barrier = pltpu.get_barrier_semaphore()
    for p in range(1, n_dev):
        pl.semaphore_signal(
            barrier, inc=1, device_id={"vp": _peer(me, p)}, device_id_type=pl.DeviceIdType.MESH
        )
    m_ref[...] = jnp.full(m_ref.shape, -jnp.inf, jnp.float32)
    s_ref[...] = jnp.zeros_like(s_ref)
    t_ref[...] = jnp.zeros_like(t_ref)
    for copy in small:
        copy.wait()
    tmp[...] = _to_rows(invt_v[...])
    for p in range(n_dev):
        scale_rows[pl.ds(p * rows, rows), :] = tmp[rows_of(p), :]
    tmp[...] = _to_rows(tgt_v[...].astype(jnp.float32))
    lane = lax.broadcasted_iota(jnp.int32, (rows, LANES), 1)
    for p in range(n_dev):
        left_rows[pl.ds(p * rows, rows), :] = tmp[rows_of(p), :].astype(jnp.int32) - me * shard - lane
    for copy in x_copies[2:]:
        copy.wait()

    def multiply(seg, step):
        width = segments[seg][0]
        slot, k = lax.rem(segments[seg][4] + step, SLOTS), lax.rem(step, k_steps)
        x = xs[:, pl.ds(pl.multiple_of(k * DEPTH, DEPTH), DEPTH)]
        for off in range(0, width, HALF):
            wide = min(HALF, width - off)
            part = jnp.dot(x, wbuf[slot, :, off:off + wide], preferred_element_type=jnp.float32)
            acc[:, off:off + wide] = part + jnp.where(k == 0, 0.0, acc[:, off:off + wide])

    def finish(col, width, out_ref, out_off, lo=0, hi=batch):
        group = 32
        span = next(n for n in (UNIT, HALF, LANES) if width % n == 0)

        def some(j, _):
            at = pl.multiple_of(j * span, span)
            for r in range(lo, hi, group):
                block = slice(r, r + group)
                scale = scale_rows[block, :]
                tiles = []
                for t in range(0, span, LANES):
                    tile = acc[block, pl.ds(at + t, LANES)] * scale
                    out_ref[block, pl.ds(pl.multiple_of(out_off + at + t, LANES), LANES)] = tile
                    tiles.append(tile)
                m_old = m_ref[block, :]
                m_new = functools.reduce(jnp.maximum, tiles, m_old)
                keep = jnp.exp(m_old - m_new)
                total = s_ref[block, :] * keep
                upto = t_ref[block, :] * keep
                left = left_rows[block, :]
                for t, tile in enumerate(tiles):
                    e = jnp.exp(tile - m_new)
                    total += e
                    upto += jnp.where(left >= col + at + t * LANES, e, 0.0)
                m_ref[block, :] = m_new
                s_ref[block, :] = total
                t_ref[block, :] = upto
            return 0

        lax.fori_loop(0, width // span, some, 0)

    sent, own, stored = [], [], []

    def send_early(u, peers, col, width):
        for p in peers:
            copy = send(u, p, col, width)
            copy.start()
            sent.append(copy)

    far = 2 * rows

    def multiply_first(k, lo, hi):
        at = pl.ds(pl.multiple_of(k * DEPTH, DEPTH), DEPTH)
        part = jnp.dot(xs[lo:hi, at], wfirst[at, :], preferred_element_type=jnp.float32)
        acc[lo:hi, :FIRST] = part + jnp.where(k == 0, 0.0, acc[lo:hi, :FIRST])

    def far_step(k, _):
        fetch_first(k).wait()

        @pl.when(k == 0)
        def _():
            for copy in x_copies[:2]:
                copy.start()

        fetch_w(0, k).start()
        multiply_first(k, far, batch)
        return 0

    def near_step(k, _):
        multiply_first(k, 0, far)
        return 0

    lax.fori_loop(0, k_steps, far_step, 0)
    finish(0, FIRST, zsend, 0, far, batch)
    pl.semaphore_wait(barrier, n_dev - 1)
    send_early(0, (2, 3), 0, FIRST)
    for copy in x_copies[:2]:
        copy.wait()
    lax.fori_loop(0, k_steps, near_step, 0)
    finish(0, FIRST, zsend, 0, 0, far)
    send_early(0, (1,), 0, FIRST)
    own.append(put_own(0, 0, FIRST))
    own[0].start()

    for seg, (width, n, chunk, col0, g0) in enumerate(segments):
        for i in range(n):

            def body(k, _, seg=seg, i=i, n=n):
                step = i * k_steps + k
                ahead = step + SLOTS - 1
                if seg < URGENT:
                    fetch_w(seg, step).wait()

                    @pl.when(k == k_steps - 1)
                    def _():
                        for later in range(k_steps):
                            fetch_w(seg + 1, jnp.int32(later)).start()

                    multiply(seg, step)
                    return 0

                @pl.when(ahead < n * k_steps)
                def _():
                    fetch_w(seg, ahead).start()

                if seg + 1 < len(segments):
                    @pl.when(ahead >= n * k_steps)
                    def _():
                        fetch_w(seg + 1, ahead - n * k_steps).start()

                fetch_w(seg, step).wait()
                multiply(seg, step)
                return 0

            lax.fori_loop(0, k_steps, body, 0)
            col = col0 + i * width
            if chunk is None:
                finish(col, width, zsend, col)
                u = len(own)
                send_early(u, (2, 3, 1), col, width)
                copy = put_own(u, col, width)
                copy.start()
                own.append(copy)
            else:
                slot = len(stored) % 2
                if len(stored) >= 2:
                    for copy in stored[-2]:
                        copy.wait()
                finish(col, width, zbuf.at[slot], 0)
                c, off = chunk
                copies = put_late(slot, c, off + i * width, width)
                for copy in copies:
                    copy.start()
                stored.append(copies)
    m = m_ref[...]
    m_row = jnp.max(m, axis=1, keepdims=True)
    keep = jnp.exp(m - m_row)
    s_row = jnp.sum(s_ref[...] * keep, axis=1, keepdims=True)
    t_row = jnp.sum(t_ref[...] * keep, axis=1, keepdims=True)
    which = lax.broadcasted_iota(jnp.int32, m.shape, 1)
    packed = jnp.where(which == 0, m_row, jnp.where(which == 1, s_row, t_row))
    for p in range(n_dev):
        tmp[rows_of(p), :] = packed[p * rows:(p + 1) * rows, :]
    pack_v[...] = jnp.transpose(tmp[...])[:STATS, :]
    for p in (2, 3, 1):
        copy = pltpu.make_async_remote_copy(
            src_ref=pack_v,
            dst_ref=packs[p],
            send_sem=pack_send.at[p],
            recv_sem=pack_recv.at[p],
            device_id={"vp": _peer(me, p)},
            device_id_type=pl.DeviceIdType.MESH,
        )
        copy.start()
        sent.append(copy)
    copy = pltpu.make_async_copy(pack_v, packs[0], pack_send.at[0])
    copy.start()
    own.append(copy)
    for copies in stored[-2:]:
        for copy in copies:
            copy.wait()
    for copy in own + sent:
        copy.wait()


def _logits(x, w, invt, tgt, n_dev):
    batch, depth = x.shape
    shard = w.shape[1]
    rows = batch // n_dev
    segments, col, g0 = [], FIRST, 0
    chunk_of = {}
    sent = begin = FIRST + sum(width * n for width, n in EARLY)
    for c, width in enumerate(LATE):
        chunk_of.update({begin + i: (c, i) for i in range(0, width, LANES)})
        begin += width
    for i, (width, n) in enumerate(EARLY + LATE_UNITS):
        segments.append((width, n, None if i < len(EARLY) else chunk_of[col], col, g0))
        col += width * n
        g0 += n * (depth // DEPTH)
    assert col == shard == begin
    n_early = 1 + sum(n for _, n in EARLY)
    hbm = pl.BlockSpec(memory_space=pltpu.HBM)
    out_shape = [pltpu.HBM((rows, sent), jnp.float32)] * n_dev
    out_shape += [pltpu.HBM((rows, width), jnp.float32) for width in LATE for _ in range(n_dev)]
    out_shape += [pltpu.HBM((STATS, batch), jnp.float32)] * n_dev
    table = pltpu.VMEM((batch, LANES), jnp.float32)
    widest = max(width for width, _ in EARLY + LATE_UNITS)
    dma = pltpu.SemaphoreType.DMA
    res = pl.pallas_call(
        functools.partial(_logits_kernel, (n_dev, shard, segments, len(LATE))),
        in_specs=[hbm] * 4,
        out_specs=[hbm] * len(out_shape),
        out_shape=out_shape,
        scratch_shapes=[
            pltpu.VMEM((batch, depth), jnp.bfloat16),
            pltpu.VMEM((depth, FIRST), jnp.bfloat16),
            pltpu.VMEM((SLOTS, DEPTH, widest), jnp.bfloat16),
            pltpu.VMEM((batch, widest), jnp.float32),
            pltpu.VMEM((batch, sent), jnp.float32),
            pltpu.VMEM((2, batch, widest), jnp.float32),
            pltpu.VMEM((1, batch), jnp.float32),
            pltpu.VMEM((1, batch), jnp.int32),
            pltpu.VMEM((STATS, batch), jnp.float32),
            table,
            pltpu.VMEM((batch, LANES), jnp.int32),
            table,
            table,
            table,
            table,
            dma((depth // DEPTH,)),
            dma((SLOTS,)),
            dma((2, n_dev)),
            dma((n_dev,)),
            dma((2,)),
            dma((n_early,)),
            dma((n_early, n_dev)),
            dma((n_early, n_dev)),
            dma((n_dev,)),
            dma((n_dev,)),
        ],
        compiler_params=pltpu.CompilerParams(
            collective_id=0, has_side_effects=True, vmem_limit_bytes=52 * 2**20
        ),
        cost_estimate=pl.CostEstimate(
            flops=2 * batch * depth * shard,
            bytes_accessed=2 * depth * shard,
            transcendentals=batch * shard,
        ),
        name="logits",
    )(*(pltpu.with_memory_space_constraint(a, pltpu.HBM) for a in (x, w, invt, tgt)))
    blocks = [res[c * n_dev:(c + 1) * n_dev] for c in range(len(LATE) + 2)]
    return blocks[0], blocks[1:-1], blocks[-1]


def _merge_kernel(n_dev, *refs):
    stats, (params_ref, at_ref) = refs[:n_dev], refs[n_dev:]
    me = lax.axis_index("vp")
    batch = stats[0].shape[1]
    rows = batch // n_dev
    ms = [s[0:1, :] for s in stats]
    top = functools.reduce(jnp.maximum, ms)
    keep = [jnp.exp(m - top) for m in ms]
    mass = [s[1:2, :] * k for s, k in zip(stats, keep)]
    upto = sum(s[2:3, :] * k for s, k in zip(stats, keep))
    total = sum(mass)
    at_ref[...] = upto / total
    values = [top, 1.0 / total]
    for p in range(n_dev):
        start = jnp.zeros_like(total)
        for q in range(n_dev):
            start += jnp.where((me ^ q) < (me ^ p), mass[q], 0.0)
        values.append(start)
    which = lax.broadcasted_iota(jnp.int32, (LANES, batch), 0)
    table = jnp.zeros((LANES, batch), jnp.float32)
    for i, v in enumerate(values):
        table = jnp.where(which == i, v, table)
    per_row = jnp.transpose(table)
    out = jnp.zeros((rows, LANES), jnp.float32)
    for d in range(n_dev):
        out = jnp.where(me == d, per_row[d * rows:(d + 1) * rows, :], out)
    params_ref[...] = out


def _merge(stats):
    n_dev = len(stats)
    batch = stats[0].shape[1]
    vmem = pl.BlockSpec(memory_space=pltpu.VMEM)
    return pl.pallas_call(
        functools.partial(_merge_kernel, n_dev),
        in_specs=[vmem] * n_dev,
        out_specs=[vmem] * 2,
        out_shape=[
            jax.ShapeDtypeStruct((batch // n_dev, LANES), jnp.float32),
            jax.ShapeDtypeStruct((1, batch), jnp.float32),
        ],
        cost_estimate=pl.CostEstimate(flops=100_000, bytes_accessed=100_000, transcendentals=1000),
        name="merge",
    )(*stats)


def _cdf_kernel(cfg, *refs):
    peers, shard, base, width, first, last = cfg
    n = len(peers)
    params_ref = refs[n]
    if last:
        out_ref, y_ref, sems = refs[n + 2:]
    else:
        out_ref, params_out, y_ref, sems = refs[n + (1 if first else 2):]
    me = lax.axis_index("vp")
    rows = params_ref.shape[0]
    params = params_ref[...]
    top = jnp.broadcast_to(params[:, 0:1], (rows, LANES))
    inv = jnp.broadcast_to(params[:, 1:2], (rows, LANES))
    k_id = lax.broadcasted_iota(jnp.int32, (3 * LANES, 2 * LANES), 0) % LANES
    n_id = lax.broadcasted_iota(jnp.int32, (3 * LANES, 2 * LANES), 1)
    tri = jnp.where(k_id <= n_id, 1.0, 0.0).astype(jnp.bfloat16)
    lane = lax.broadcasted_iota(jnp.int32, (rows, LANES), 1)

    def unit(col, wide, carries):
        ends = []
        for j in range(n):
            cols = [pl.ds(col + t, LANES) for t in range(0, wide, LANES)]
            e = jnp.concatenate([jnp.exp(refs[j][:, c] - top) for c in cols], axis=0)
            hi = e.astype(jnp.bfloat16)
            r1 = e - hi.astype(jnp.float32)
            mid = r1.astype(jnp.bfloat16)
            lo = (r1 - mid.astype(jnp.float32)).astype(jnp.bfloat16)
            sums = jnp.dot(jnp.concatenate([hi, mid, lo], axis=1), tri, preferred_element_type=jnp.float32)
            carry = carries[j]
            for t, c in enumerate(cols):
                block = slice(t * rows, (t + 1) * rows)
                y_ref[j, :, c] = (sums[block, :LANES] + carry) * inv
                carry = carry + sums[block, LANES:]
            ends.append(carry)
        return tuple(ends)

    carries = tuple(jnp.broadcast_to(params[:, 2 + p:3 + p], (rows, LANES)) for p in peers)
    n_full = width // UNIT
    if n_full:
        carries = lax.fori_loop(
            0, n_full, lambda u, c: unit(pl.multiple_of(u * UNIT, UNIT), UNIT, c), carries
        )
    if width % UNIT:
        carries = unit(n_full * UNIT, width % UNIT, carries)
    copies = []
    updated = params
    for j, p in enumerate(peers):
        where = pl.multiple_of((me ^ p) * shard + base, LANES)
        copy = pltpu.make_async_copy(y_ref.at[j], out_ref.at[:, pl.ds(where, width)], sems.at[j])
        copy.start()
        copies.append(copy)
        updated = jnp.where(lane == 2 + p, carries[j], updated)
    if not last:
        params_out[...] = updated
    for copy in copies:
        copy.wait()


def _cdf(blocks, peers, params, out, n_dev, shard, base, last=False):
    rows, width = blocks[0].shape
    n = len(peers)
    first = out is None
    vmem = pl.BlockSpec(memory_space=pltpu.VMEM)
    hbm = pl.BlockSpec(memory_space=pl.ANY)
    return pl.pallas_call(
        functools.partial(_cdf_kernel, (peers, shard, base, width, first, last)),
        in_specs=[vmem] * (n + 1) + ([] if first else [hbm]),
        out_specs=[hbm] + ([] if last else [vmem]),
        out_shape=[jax.ShapeDtypeStruct((rows, n_dev * shard), jnp.float32)]
        + ([] if last else [jax.ShapeDtypeStruct(params.shape, jnp.float32)]),
        scratch_shapes=[
            pltpu.VMEM((n, rows, width), jnp.float32),
            pltpu.SemaphoreType.DMA((n,)),
        ],
        input_output_aliases={} if first else {n + 1: 0},
        compiler_params=pltpu.CompilerParams(vmem_limit_bytes=24 * 2**20),
        cost_estimate=pl.CostEstimate(
            flops=n * 2 * rows * width * 384,
            bytes_accessed=n * rows * width * 8,
            transcendentals=n * rows * width,
        ),
        name="cdf",
    )(*blocks, params, *(() if first else (out,)))


def solution(mesh):
    n_dev = mesh.shape["vp"]
    assert n_dev == 4

    def swap(a, p):
        return lax.ppermute(a, "vp", [(i, i ^ p) for i in range(n_dev)])

    def local_step(hidden, w_local, inv_temp, target_ids):
        shard = w_local.shape[1]
        early, late, packs = _logits(
            hidden, w_local, inv_temp.reshape(1, -1), target_ids.reshape(1, -1), n_dev
        )
        chunks = [(0, early)]
        begin = early[0].shape[1]
        for made in late:
            got = [made[0]]
            for p in range(1, n_dev):
                got.append(swap(made[p], p))
            chunks.append((begin, got))
            begin += made[0].shape[1]
        params, at_target = _merge(packs)
        out = None
        final = len(chunks) - 1
        plan = [(k, peers) for peers in ((0, 1), (2, 3)) for k in range(final + 1)]
        for i, (k, peers) in enumerate(plan):
            begin, got = chunks[k]
            blocks = [got[p] for p in peers]
            if k < final or peers[0] == 0:
                blocks = [pltpu.with_memory_space_constraint(a, pltpu.HBM) for a in blocks]
            res = _cdf(blocks, peers, params, out, n_dev, shard, begin, i == len(plan) - 1)
            out = res[0]
            params = res[1] if len(res) > 1 else None
        return out, at_target.reshape(-1)

    return jax.shard_map(
        local_step,
        mesh=mesh,
        in_specs=(P("dp", None), P(None, "vp"), P("dp"), P("dp")),
        out_specs=(P(("dp", "vp"), None), P("dp")),
        check_vma=False,
    )
```

```python
import functools

import jax
import jax.numpy as jnp
from jax import lax
from jax.experimental import pallas as pl
from jax.experimental.pallas import tpu as pltpu
from jax.sharding import PartitionSpec as P


LANES = 128
UNIT = 512
HALF = 256
DEPTH = 512
SLOTS = 9
FIRST = 256
EARLY = ((512, 15),)
LATE = (4096, 2048, 1536, 384)
LATE_UNITS = ((2048, 2), (2048, 1), (1536, 1), (384, 1))
STATS = 4


def _to_rows(vec_1xn):
    n = vec_1xn.shape[1]
    return jnp.transpose(jnp.broadcast_to(vec_1xn, (LANES, n)))


def _peer(me, p):
    return [me, me + 1 - 2 * lax.rem(me, 2), lax.rem(me + 2, 4), 3 - me][p]


def _logits_kernel(cfg, x_ref, w_ref, invt_ref, tgt_ref, *refs):
    n_dev, shard, segments, n_late = cfg
    refs = list(refs)

    def take(n):
        out = refs[:n]
        del refs[:n]
        return out

    early = take(n_dev)
    late = [take(n_dev) for _ in range(n_late)]
    packs = take(n_dev)
    xs, wfirst, wbuf, acc, zsend, zbuf, invt_v, tgt_v, pack_v = take(9)
    scale_rows, left_rows, tmp, m_ref, s_ref, t_ref = take(6)
    first_sem, w_sem, z_sem, x_sem, v_sem, own_sem, send_sem, recv_sem, pack_send, pack_recv = take(10)
    me = lax.axis_index("vp")
    batch, depth = xs.shape
    rows = batch // n_dev
    k_steps = depth // DEPTH
    assert SLOTS == k_steps + 1

    def rows_of(p):
        return pl.ds(pl.multiple_of(_peer(me, p) * rows, rows), rows)

    def fetch_w(seg, step):
        width, col0, g0 = segments[seg][0], segments[seg][3], segments[seg][4]
        slot = lax.rem(g0 + step, SLOTS)
        col = col0 + lax.div(step, k_steps) * width
        row = pl.multiple_of(lax.rem(step, k_steps) * DEPTH, DEPTH)
        return pltpu.make_async_copy(
            w_ref.at[pl.ds(row, DEPTH), pl.ds(pl.multiple_of(col, LANES), width)],
            wbuf.at[slot, :, pl.ds(0, width)],
            w_sem.at[slot],
        )

    def fetch_first(k):
        row = pl.ds(pl.multiple_of(k * DEPTH, DEPTH), DEPTH)
        return pltpu.make_async_copy(w_ref.at[row, pl.ds(0, FIRST)], wfirst.at[row, :], first_sem.at[k])

    def put_late(slot, c, off, width):
        return [
            pltpu.make_async_copy(
                zbuf.at[slot, pl.ds(p * rows, rows), pl.ds(0, width)],
                late[c][p].at[:, pl.ds(off, width)],
                z_sem.at[slot, p],
            )
            for p in range(n_dev)
        ]

    def put_own(u, off, width):
        return pltpu.make_async_copy(
            zsend.at[pl.ds(0, rows), pl.ds(off, width)], early[0].at[:, pl.ds(off, width)], own_sem.at[u]
        )

    def send(u, p, off, width):
        return pltpu.make_async_remote_copy(
            src_ref=zsend.at[pl.ds(p * rows, rows), pl.ds(off, width)],
            dst_ref=early[p].at[:, pl.ds(off, width)],
            send_sem=send_sem.at[u, p],
            recv_sem=recv_sem.at[u, p],
            device_id={"vp": _peer(me, p)},
            device_id_type=pl.DeviceIdType.MESH,
        )

    x_copies = [
        pltpu.make_async_copy(x_ref.at[rows_of(p), :], xs.at[pl.ds(p * rows, rows), :], x_sem.at[p])
        for p in range(n_dev)
    ]
    small = [
        pltpu.make_async_copy(invt_ref, invt_v, v_sem.at[0]),
        pltpu.make_async_copy(tgt_ref, tgt_v, v_sem.at[1]),
    ]
    for copy in small + x_copies[2:]:
        copy.start()
    for k in range(k_steps):
        fetch_first(k).start()
    barrier = pltpu.get_barrier_semaphore()
    for p in range(1, n_dev):
        pl.semaphore_signal(
            barrier, inc=1, device_id={"vp": _peer(me, p)}, device_id_type=pl.DeviceIdType.MESH
        )
    m_ref[...] = jnp.full(m_ref.shape, -jnp.inf, jnp.float32)
    s_ref[...] = jnp.zeros_like(s_ref)
    t_ref[...] = jnp.zeros_like(t_ref)
    for copy in small:
        copy.wait()
    tmp[...] = _to_rows(invt_v[...])
    for p in range(n_dev):
        scale_rows[pl.ds(p * rows, rows), :] = tmp[rows_of(p), :]
    tmp[...] = _to_rows(tgt_v[...].astype(jnp.float32))
    lane = lax.broadcasted_iota(jnp.int32, (rows, LANES), 1)
    for p in range(n_dev):
        left_rows[pl.ds(p * rows, rows), :] = tmp[rows_of(p), :].astype(jnp.int32) - me * shard - lane
    for copy in x_copies[2:]:
        copy.wait()

    def multiply(seg, step):
        width = segments[seg][0]
        slot, k = lax.rem(segments[seg][4] + step, SLOTS), lax.rem(step, k_steps)
        x = xs[:, pl.ds(pl.multiple_of(k * DEPTH, DEPTH), DEPTH)]
        for off in range(0, width, HALF):
            wide = min(HALF, width - off)
            part = jnp.dot(x, wbuf[slot, :, off:off + wide], preferred_element_type=jnp.float32)
            acc[:, off:off + wide] = part + jnp.where(k == 0, 0.0, acc[:, off:off + wide])

    def finish(col, width, out_ref, out_off, lo=0, hi=batch):
        group = 32
        span = next(n for n in (UNIT, HALF, LANES) if width % n == 0)

        def some(j, _):
            at = pl.multiple_of(j * span, span)
            for r in range(lo, hi, group):
                block = slice(r, r + group)
                scale = scale_rows[block, :]
                tiles = []
                for t in range(0, span, LANES):
                    tile = acc[block, pl.ds(at + t, LANES)] * scale
                    out_ref[block, pl.ds(pl.multiple_of(out_off + at + t, LANES), LANES)] = tile
                    tiles.append(tile)
                m_old = m_ref[block, :]
                m_new = functools.reduce(jnp.maximum, tiles, m_old)
                keep = jnp.exp(m_old - m_new)
                total = s_ref[block, :] * keep
                upto = t_ref[block, :] * keep
                left = left_rows[block, :]
                for t, tile in enumerate(tiles):
                    e = jnp.exp(tile - m_new)
                    total += e
                    upto += jnp.where(left >= col + at + t * LANES, e, 0.0)
                m_ref[block, :] = m_new
                s_ref[block, :] = total
                t_ref[block, :] = upto
            return 0

        lax.fori_loop(0, width // span, some, 0)

    sent, own, stored = [], [], []

    def send_early(u, peers, col, width):
        for p in peers:
            copy = send(u, p, col, width)
            copy.start()
            sent.append(copy)

    far = 2 * rows

    def multiply_first(k, lo, hi):
        at = pl.ds(pl.multiple_of(k * DEPTH, DEPTH), DEPTH)
        part = jnp.dot(xs[lo:hi, at], wfirst[at, :], preferred_element_type=jnp.float32)
        acc[lo:hi, :FIRST] = part + jnp.where(k == 0, 0.0, acc[lo:hi, :FIRST])

    def far_step(k, _):
        fetch_first(k).wait()

        @pl.when(k == 0)
        def _():
            for copy in x_copies[:2]:
                copy.start()

        fetch_w(0, k).start()
        multiply_first(k, far, batch)
        return 0

    def near_step(k, _):
        multiply_first(k, 0, far)
        return 0

    lax.fori_loop(0, k_steps, far_step, 0)
    finish(0, FIRST, zsend, 0, far, batch)
    pl.semaphore_wait(barrier, n_dev - 1)
    send_early(0, (2, 3), 0, FIRST)
    for copy in x_copies[:2]:
        copy.wait()
    lax.fori_loop(0, k_steps, near_step, 0)
    finish(0, FIRST, zsend, 0, 0, far)
    send_early(0, (1,), 0, FIRST)
    own.append(put_own(0, 0, FIRST))
    own[0].start()

    def run_unit(seg, i):
        n = segments[seg][1]

        def body(k, _):
            step = i * k_steps + k
            ahead = step + SLOTS - 1

            @pl.when(ahead < n * k_steps)
            def _():
                fetch_w(seg, ahead).start()

            if seg + 1 < len(segments):
                @pl.when(ahead >= n * k_steps)
                def _():
                    fetch_w(seg + 1, ahead - n * k_steps).start()

            fetch_w(seg, step).wait()
            multiply(seg, step)
            return 0

        lax.fori_loop(0, k_steps, body, 0)

    for seg, (width, n, chunk, col0, g0) in enumerate(segments):
        if chunk is None:
            u0 = len(own)

            def early_unit(i, _, seg=seg, width=width, col0=col0, u0=u0):
                run_unit(seg, i)
                col = pl.multiple_of(col0 + i * width, LANES)
                finish(col, width, zsend, col)
                for p in (2, 3, 1):
                    send(u0 + i, p, col, width).start()
                put_own(u0 + i, col, width).start()
                return 0

            lax.fori_loop(0, n, early_unit, 0)
            for i in range(n):
                sent += [send(u0 + i, p, col0 + i * width, width) for p in (2, 3, 1)]
                own.append(put_own(u0 + i, col0 + i * width, width))
            continue
        for i in range(n):
            run_unit(seg, i)
            slot = len(stored) % 2
            if len(stored) >= 2:
                for copy in stored[-2]:
                    copy.wait()
            finish(col0 + i * width, width, zbuf.at[slot], 0)
            c, off = chunk
            copies = put_late(slot, c, off + i * width, width)
            for copy in copies:
                copy.start()
            stored.append(copies)
    m = m_ref[...]
    m_row = jnp.max(m, axis=1, keepdims=True)
    keep = jnp.exp(m - m_row)
    s_row = jnp.sum(s_ref[...] * keep, axis=1, keepdims=True)
    t_row = jnp.sum(t_ref[...] * keep, axis=1, keepdims=True)
    which = lax.broadcasted_iota(jnp.int32, m.shape, 1)
    packed = jnp.where(which == 0, m_row, jnp.where(which == 1, s_row, t_row))
    for p in range(n_dev):
        tmp[rows_of(p), :] = packed[p * rows:(p + 1) * rows, :]
    pack_v[...] = jnp.transpose(tmp[...])[:STATS, :]
    for p in (2, 3, 1):
        copy = pltpu.make_async_remote_copy(
            src_ref=pack_v,
            dst_ref=packs[p],
            send_sem=pack_send.at[p],
            recv_sem=pack_recv.at[p],
            device_id={"vp": _peer(me, p)},
            device_id_type=pl.DeviceIdType.MESH,
        )
        copy.start()
        sent.append(copy)
    copy = pltpu.make_async_copy(pack_v, packs[0], pack_send.at[0])
    copy.start()
    own.append(copy)
    for copies in stored[-2:]:
        for copy in copies:
            copy.wait()
    for copy in own + sent:
        copy.wait()


def _logits(x, w, invt, tgt, n_dev):
    batch, depth = x.shape
    shard = w.shape[1]
    rows = batch // n_dev
    segments, col, g0 = [], FIRST, 0
    chunk_of = {}
    sent = begin = FIRST + sum(width * n for width, n in EARLY)
    for c, width in enumerate(LATE):
        chunk_of.update({begin + i: (c, i) for i in range(0, width, LANES)})
        begin += width
    for i, (width, n) in enumerate(EARLY + LATE_UNITS):
        segments.append((width, n, None if i < len(EARLY) else chunk_of[col], col, g0))
        col += width * n
        g0 += n * (depth // DEPTH)
    assert col == shard == begin
    n_early = 1 + sum(n for _, n in EARLY)
    hbm = pl.BlockSpec(memory_space=pltpu.HBM)
    out_shape = [pltpu.HBM((rows, sent), jnp.float32)] * n_dev
    out_shape += [pltpu.HBM((rows, width), jnp.float32) for width in LATE for _ in range(n_dev)]
    out_shape += [pltpu.HBM((STATS, batch), jnp.float32)] * n_dev
    table = pltpu.VMEM((batch, LANES), jnp.float32)
    widest = max(width for width, _ in EARLY + LATE_UNITS)
    dma = pltpu.SemaphoreType.DMA
    res = pl.pallas_call(
        functools.partial(_logits_kernel, (n_dev, shard, segments, len(LATE))),
        in_specs=[hbm] * 4,
        out_specs=[hbm] * len(out_shape),
        out_shape=out_shape,
        scratch_shapes=[
            pltpu.VMEM((batch, depth), jnp.bfloat16),
            pltpu.VMEM((depth, FIRST), jnp.bfloat16),
            pltpu.VMEM((SLOTS, DEPTH, widest), jnp.bfloat16),
            pltpu.VMEM((batch, widest), jnp.float32),
            pltpu.VMEM((batch, sent), jnp.float32),
            pltpu.VMEM((2, batch, widest), jnp.float32),
            pltpu.VMEM((1, batch), jnp.float32),
            pltpu.VMEM((1, batch), jnp.int32),
            pltpu.VMEM((STATS, batch), jnp.float32),
            table,
            pltpu.VMEM((batch, LANES), jnp.int32),
            table,
            table,
            table,
            table,
            dma((depth // DEPTH,)),
            dma((SLOTS,)),
            dma((2, n_dev)),
            dma((n_dev,)),
            dma((2,)),
            dma((n_early,)),
            dma((n_early, n_dev)),
            dma((n_early, n_dev)),
            dma((n_dev,)),
            dma((n_dev,)),
        ],
        compiler_params=pltpu.CompilerParams(
            collective_id=0, has_side_effects=True, vmem_limit_bytes=52 * 2**20
        ),
        cost_estimate=pl.CostEstimate(
            flops=2 * batch * depth * shard,
            bytes_accessed=2 * depth * shard,
            transcendentals=batch * shard,
        ),
        name="logits",
    )(*(pltpu.with_memory_space_constraint(a, pltpu.HBM) for a in (x, w, invt, tgt)))
    blocks = [res[c * n_dev:(c + 1) * n_dev] for c in range(len(LATE) + 2)]
    return blocks[0], blocks[1:-1], blocks[-1]


def _merge_kernel(n_dev, *refs):
    stats, (params_ref, at_ref) = refs[:n_dev], refs[n_dev:]
    me = lax.axis_index("vp")
    batch = stats[0].shape[1]
    rows = batch // n_dev
    ms = [s[0:1, :] for s in stats]
    top = functools.reduce(jnp.maximum, ms)
    keep = [jnp.exp(m - top) for m in ms]
    mass = [s[1:2, :] * k for s, k in zip(stats, keep)]
    upto = sum(s[2:3, :] * k for s, k in zip(stats, keep))
    total = sum(mass)
    at_ref[...] = upto / total
    values = [top, 1.0 / total]
    for p in range(n_dev):
        start = jnp.zeros_like(total)
        for q in range(n_dev):
            start += jnp.where((me ^ q) < (me ^ p), mass[q], 0.0)
        values.append(start)
    which = lax.broadcasted_iota(jnp.int32, (LANES, batch), 0)
    table = jnp.zeros((LANES, batch), jnp.float32)
    for i, v in enumerate(values):
        table = jnp.where(which == i, v, table)
    per_row = jnp.transpose(table)
    out = jnp.zeros((rows, LANES), jnp.float32)
    for d in range(n_dev):
        out = jnp.where(me == d, per_row[d * rows:(d + 1) * rows, :], out)
    params_ref[...] = out


def _merge(stats):
    n_dev = len(stats)
    batch = stats[0].shape[1]
    vmem = pl.BlockSpec(memory_space=pltpu.VMEM)
    return pl.pallas_call(
        functools.partial(_merge_kernel, n_dev),
        in_specs=[vmem] * n_dev,
        out_specs=[vmem] * 2,
        out_shape=[
            jax.ShapeDtypeStruct((batch // n_dev, LANES), jnp.float32),
            jax.ShapeDtypeStruct((1, batch), jnp.float32),
        ],
        cost_estimate=pl.CostEstimate(flops=100_000, bytes_accessed=100_000, transcendentals=1000),
        name="merge",
    )(*stats)


def _cdf_kernel(cfg, *refs):
    peers, shard, base, width, first, last = cfg
    n = len(peers)
    params_ref = refs[n]
    if last:
        out_ref, y_ref, sems = refs[n + 2:]
    else:
        out_ref, params_out, y_ref, sems = refs[n + (1 if first else 2):]
    me = lax.axis_index("vp")
    rows = params_ref.shape[0]
    params = params_ref[...]
    top = jnp.broadcast_to(params[:, 0:1], (rows, LANES))
    inv = jnp.broadcast_to(params[:, 1:2], (rows, LANES))
    k_id = lax.broadcasted_iota(jnp.int32, (3 * LANES, 2 * LANES), 0) % LANES
    n_id = lax.broadcasted_iota(jnp.int32, (3 * LANES, 2 * LANES), 1)
    tri = jnp.where(k_id <= n_id, 1.0, 0.0).astype(jnp.bfloat16)
    lane = lax.broadcasted_iota(jnp.int32, (rows, LANES), 1)

    def unit(col, wide, carries):
        ends = []
        for j in range(n):
            cols = [pl.ds(col + t, LANES) for t in range(0, wide, LANES)]
            e = jnp.concatenate([jnp.exp(refs[j][:, c] - top) for c in cols], axis=0)
            hi = e.astype(jnp.bfloat16)
            r1 = e - hi.astype(jnp.float32)
            mid = r1.astype(jnp.bfloat16)
            lo = (r1 - mid.astype(jnp.float32)).astype(jnp.bfloat16)
            sums = jnp.dot(jnp.concatenate([hi, mid, lo], axis=1), tri, preferred_element_type=jnp.float32)
            carry = carries[j]
            for t, c in enumerate(cols):
                block = slice(t * rows, (t + 1) * rows)
                y_ref[j, :, c] = (sums[block, :LANES] + carry) * inv
                carry = carry + sums[block, LANES:]
            ends.append(carry)
        return tuple(ends)

    carries = tuple(jnp.broadcast_to(params[:, 2 + p:3 + p], (rows, LANES)) for p in peers)
    n_full = width // UNIT
    if n_full:
        carries = lax.fori_loop(
            0, n_full, lambda u, c: unit(pl.multiple_of(u * UNIT, UNIT), UNIT, c), carries
        )
    if width % UNIT:
        carries = unit(n_full * UNIT, width % UNIT, carries)
    copies = []
    updated = params
    for j, p in enumerate(peers):
        where = pl.multiple_of((me ^ p) * shard + base, LANES)
        copy = pltpu.make_async_copy(y_ref.at[j], out_ref.at[:, pl.ds(where, width)], sems.at[j])
        copy.start()
        copies.append(copy)
        updated = jnp.where(lane == 2 + p, carries[j], updated)
    if not last:
        params_out[...] = updated
    for copy in copies:
        copy.wait()


def _cdf(blocks, peers, params, out, n_dev, shard, base, last=False):
    rows, width = blocks[0].shape
    n = len(peers)
    first = out is None
    vmem = pl.BlockSpec(memory_space=pltpu.VMEM)
    hbm = pl.BlockSpec(memory_space=pl.ANY)
    return pl.pallas_call(
        functools.partial(_cdf_kernel, (peers, shard, base, width, first, last)),
        in_specs=[vmem] * (n + 1) + ([] if first else [hbm]),
        out_specs=[hbm] + ([] if last else [vmem]),
        out_shape=[jax.ShapeDtypeStruct((rows, n_dev * shard), jnp.float32)]
        + ([] if last else [jax.ShapeDtypeStruct(params.shape, jnp.float32)]),
        scratch_shapes=[
            pltpu.VMEM((n, rows, width), jnp.float32),
            pltpu.SemaphoreType.DMA((n,)),
        ],
        input_output_aliases={} if first else {n + 1: 0},
        compiler_params=pltpu.CompilerParams(vmem_limit_bytes=24 * 2**20),
        cost_estimate=pl.CostEstimate(
            flops=n * 2 * rows * width * 384,
            bytes_accessed=n * rows * width * 8,
            transcendentals=n * rows * width,
        ),
        name="cdf",
    )(*blocks, params, *(() if first else (out,)))


def solution(mesh):
    n_dev = mesh.shape["vp"]
    assert n_dev == 4

    def swap(a, p):
        return lax.ppermute(a, "vp", [(i, i ^ p) for i in range(n_dev)])

    def local_step(hidden, w_local, inv_temp, target_ids):
        shard = w_local.shape[1]
        early, late, packs = _logits(
            hidden, w_local, inv_temp.reshape(1, -1), target_ids.reshape(1, -1), n_dev
        )
        chunks = [(0, early)]
        begin = early[0].shape[1]
        for made in late:
            got = [made[0]]
            for p in range(1, n_dev):
                got.append(swap(made[p], p))
            chunks.append((begin, got))
            begin += made[0].shape[1]
        params, at_target = _merge(packs)
        out = None
        final = len(chunks) - 1
        plan = [(k, peers) for peers in ((0, 1), (2, 3)) for k in range(final + 1)]
        for i, (k, peers) in enumerate(plan):
            begin, got = chunks[k]
            blocks = [got[p] for p in peers]
            if k < final or peers[0] == 0:
                blocks = [pltpu.with_memory_space_constraint(a, pltpu.HBM) for a in blocks]
            res = _cdf(blocks, peers, params, out, n_dev, shard, begin, i == len(plan) - 1)
            out = res[0]
            params = res[1] if len(res) > 1 else None
        return out, at_target.reshape(-1)

    return jax.shard_map(
        local_step,
        mesh=mesh,
        in_specs=(P("dp", None), P(None, "vp"), P("dp"), P("dp")),
        out_specs=(P(("dp", "vp"), None), P("dp")),
        check_vma=False,
    )
```

```python
import functools

import jax
import jax.numpy as jnp
from jax import lax
from jax.experimental import pallas as pl
from jax.experimental.pallas import tpu as pltpu
from jax.sharding import PartitionSpec as P


LANES = 128
UNIT = 512
HALF = 256
DEPTH = 512
SLOTS = 9
FIRST = 256
EARLY = ((256, 1), (512, 1), (1024, 1), (2048, 2))
LATE = (4096, 2048, 2048, 1280, 384)
LATE_UNITS = ((2048, 2), (2048, 1), (2048, 1), (1280, 1), (384, 1))
STATS = 4


def _to_rows(vec_1xn):
    n = vec_1xn.shape[1]
    return jnp.transpose(jnp.broadcast_to(vec_1xn, (LANES, n)))


def _peer(me, p):
    return [me, me + 1 - 2 * lax.rem(me, 2), lax.rem(me + 2, 4), 3 - me][p]


def _logits_kernel(cfg, x_ref, w_ref, invt_ref, tgt_ref, *refs):
    n_dev, shard, segments, n_early, n_late = cfg
    refs = list(refs)

    def take(n):
        out = refs[:n]
        del refs[:n]
        return out

    early = [take(n_dev) for _ in range(n_early)]
    late = [take(n_dev) for _ in range(n_late)]
    packs = take(n_dev)
    zsend = take(n_early)
    xs, wfirst, wbuf, acc, zbuf, invt_v, tgt_v, pack_v = take(8)
    scale_rows, left_rows, tmp, m_ref, s_ref, t_ref = take(6)
    first_sem, w_sem, z_sem, x_sem, v_sem, own_sem, send_sem, recv_sem, pack_send, pack_recv = take(10)
    me = lax.axis_index("vp")
    batch, depth = xs.shape
    rows = batch // n_dev
    k_steps = depth // DEPTH
    assert SLOTS == k_steps + 1

    def rows_of(p):
        return pl.ds(pl.multiple_of(_peer(me, p) * rows, rows), rows)

    def fetch_w(seg, step):
        width, col0, g0 = segments[seg][0], segments[seg][3], segments[seg][4]
        slot = lax.rem(g0 + step, SLOTS)
        col = col0 + lax.div(step, k_steps) * width
        row = pl.multiple_of(lax.rem(step, k_steps) * DEPTH, DEPTH)
        return pltpu.make_async_copy(
            w_ref.at[pl.ds(row, DEPTH), pl.ds(pl.multiple_of(col, LANES), width)],
            wbuf.at[slot, :, pl.ds(0, width)],
            w_sem.at[slot],
        )

    def fetch_first(k):
        row = pl.ds(pl.multiple_of(k * DEPTH, DEPTH), DEPTH)
        return pltpu.make_async_copy(w_ref.at[row, pl.ds(0, FIRST)], wfirst.at[row, :], first_sem.at[k])

    def put_late(slot, c, off, width):
        return [
            pltpu.make_async_copy(
                zbuf.at[slot, pl.ds(p * rows, rows), pl.ds(0, width)],
                late[c][p].at[:, pl.ds(off, width)],
                z_sem.at[slot, p],
            )
            for p in range(n_dev)
        ]

    def put_own(u):
        return pltpu.make_async_copy(zsend[u].at[pl.ds(0, rows), :], early[u][0], own_sem.at[u])

    def send(u, p):
        return pltpu.make_async_remote_copy(
            src_ref=zsend[u].at[pl.ds(p * rows, rows), :],
            dst_ref=early[u][p],
            send_sem=send_sem.at[u, p],
            recv_sem=recv_sem.at[u, p],
            device_id={"vp": _peer(me, p)},
            device_id_type=pl.DeviceIdType.MESH,
        )

    x_copies = [
        pltpu.make_async_copy(x_ref.at[rows_of(p), :], xs.at[pl.ds(p * rows, rows), :], x_sem.at[p])
        for p in range(n_dev)
    ]
    small = [
        pltpu.make_async_copy(invt_ref, invt_v, v_sem.at[0]),
        pltpu.make_async_copy(tgt_ref, tgt_v, v_sem.at[1]),
    ]
    for copy in small + x_copies[2:]:
        copy.start()
    for k in range(k_steps):
        fetch_first(k).start()
    barrier = pltpu.get_barrier_semaphore()
    for p in range(1, n_dev):
        pl.semaphore_signal(
            barrier, inc=1, device_id={"vp": _peer(me, p)}, device_id_type=pl.DeviceIdType.MESH
        )
    m_ref[...] = jnp.full(m_ref.shape, -jnp.inf, jnp.float32)
    s_ref[...] = jnp.zeros_like(s_ref)
    t_ref[...] = jnp.zeros_like(t_ref)
    for copy in small:
        copy.wait()
    tmp[...] = _to_rows(invt_v[...])
    for p in range(n_dev):
        scale_rows[pl.ds(p * rows, rows), :] = tmp[rows_of(p), :]
    tmp[...] = _to_rows(tgt_v[...].astype(jnp.float32))
    lane = lax.broadcasted_iota(jnp.int32, (rows, LANES), 1)
    for p in range(n_dev):
        left_rows[pl.ds(p * rows, rows), :] = tmp[rows_of(p), :].astype(jnp.int32) - me * shard - lane
    for copy in x_copies[2:]:
        copy.wait()

    def multiply(seg, step):
        width = segments[seg][0]
        slot, k = lax.rem(segments[seg][4] + step, SLOTS), lax.rem(step, k_steps)
        x = xs[:, pl.ds(pl.multiple_of(k * DEPTH, DEPTH), DEPTH)]
        for off in range(0, width, HALF):
            wide = min(HALF, width - off)
            part = jnp.dot(x, wbuf[slot, :, off:off + wide], preferred_element_type=jnp.float32)
            acc[:, off:off + wide] = part + jnp.where(k == 0, 0.0, acc[:, off:off + wide])

    def finish(col, width, out_ref, out_off, lo=0, hi=batch):
        group = 32
        span = next(n for n in (UNIT, HALF, LANES) if width % n == 0)

        def some(j, _):
            at = pl.multiple_of(j * span, span)
            for r in range(lo, hi, group):
                block = slice(r, r + group)
                scale = scale_rows[block, :]
                tiles = []
                for t in range(0, span, LANES):
                    tile = acc[block, pl.ds(at + t, LANES)] * scale
                    out_ref[block, pl.ds(pl.multiple_of(out_off + at + t, LANES), LANES)] = tile
                    tiles.append(tile)
                m_old = m_ref[block, :]
                m_new = functools.reduce(jnp.maximum, tiles, m_old)
                keep = jnp.exp(m_old - m_new)
                total = s_ref[block, :] * keep
                upto = t_ref[block, :] * keep
                left = left_rows[block, :]
                for t, tile in enumerate(tiles):
                    e = jnp.exp(tile - m_new)
                    total += e
                    upto += jnp.where(left >= col + at + t * LANES, e, 0.0)
                m_ref[block, :] = m_new
                s_ref[block, :] = total
                t_ref[block, :] = upto
            return 0

        lax.fori_loop(0, width // span, some, 0)

    sent, own, stored = [], [], []

    def send_early(u, peers):
        for p in peers:
            copy = send(u, p)
            copy.start()
            sent.append(copy)

    far = 2 * rows

    def multiply_first(k, lo, hi):
        at = pl.ds(pl.multiple_of(k * DEPTH, DEPTH), DEPTH)
        part = jnp.dot(xs[lo:hi, at], wfirst[at, :], preferred_element_type=jnp.float32)
        acc[lo:hi, :FIRST] = part + jnp.where(k == 0, 0.0, acc[lo:hi, :FIRST])

    def far_step(k, _):
        fetch_first(k).wait()

        @pl.when(k == 0)
        def _():
            for copy in x_copies[:2]:
                copy.start()

        fetch_w(0, k).start()
        multiply_first(k, far, batch)
        return 0

    def near_step(k, _):
        multiply_first(k, 0, far)
        return 0

    lax.fori_loop(0, k_steps, far_step, 0)
    finish(0, FIRST, zsend[0], 0, far, batch)
    pl.semaphore_wait(barrier, n_dev - 1)
    send_early(0, (2, 3))
    for copy in x_copies[:2]:
        copy.wait()
    lax.fori_loop(0, k_steps, near_step, 0)
    finish(0, FIRST, zsend[0], 0, 0, far)
    send_early(0, (1,))
    own.append(put_own(0))
    own[0].start()

    for seg, (width, n, chunk, col0, g0) in enumerate(segments):
        for i in range(n):

            def body(k, _, seg=seg, i=i, n=n):
                step = i * k_steps + k
                ahead = step + SLOTS - 1

                @pl.when(ahead < n * k_steps)
                def _():
                    fetch_w(seg, ahead).start()

                if seg + 1 < len(segments):
                    @pl.when(ahead >= n * k_steps)
                    def _():
                        fetch_w(seg + 1, ahead - n * k_steps).start()

                fetch_w(seg, step).wait()
                multiply(seg, step)
                return 0

            lax.fori_loop(0, k_steps, body, 0)
            col = col0 + i * width
            if chunk is None:
                u = len(own)
                finish(col, width, zsend[u], 0)
                send_early(u, (2, 3, 1))
                copy = put_own(u)
                copy.start()
                own.append(copy)
            else:
                slot = len(stored) % 2
                if len(stored) >= 2:
                    for copy in stored[-2]:
                        copy.wait()
                finish(col, width, zbuf.at[slot], 0)
                c, off = chunk
                copies = put_late(slot, c, off + i * width, width)
                for copy in copies:
                    copy.start()
                stored.append(copies)
    m = m_ref[...]
    m_row = jnp.max(m, axis=1, keepdims=True)
    keep = jnp.exp(m - m_row)
    s_row = jnp.sum(s_ref[...] * keep, axis=1, keepdims=True)
    t_row = jnp.sum(t_ref[...] * keep, axis=1, keepdims=True)
    which = lax.broadcasted_iota(jnp.int32, m.shape, 1)
    packed = jnp.where(which == 0, m_row, jnp.where(which == 1, s_row, t_row))
    for p in range(n_dev):
        tmp[rows_of(p), :] = packed[p * rows:(p + 1) * rows, :]
    pack_v[...] = jnp.transpose(tmp[...])[:STATS, :]
    for p in (2, 3, 1):
        copy = pltpu.make_async_remote_copy(
            src_ref=pack_v,
            dst_ref=packs[p],
            send_sem=pack_send.at[p],
            recv_sem=pack_recv.at[p],
            device_id={"vp": _peer(me, p)},
            device_id_type=pl.DeviceIdType.MESH,
        )
        copy.start()
        sent.append(copy)
    copy = pltpu.make_async_copy(pack_v, packs[0], pack_send.at[0])
    copy.start()
    own.append(copy)
    for copies in stored[-2:]:
        for copy in copies:
            copy.wait()
    for copy in own + sent:
        copy.wait()


def _logits(x, w, invt, tgt, n_dev):
    batch, depth = x.shape
    shard = w.shape[1]
    rows = batch // n_dev
    segments, col, g0 = [], FIRST, 0
    chunk_of = {}
    units = [FIRST] + [width for width, n in EARLY for _ in range(n)]
    n_early, begin = len(units), sum(units)
    for c, width in enumerate(LATE):
        chunk_of.update({begin + i: (c, i) for i in range(0, width, LANES)})
        begin += width
    for i, (width, n) in enumerate(EARLY + LATE_UNITS):
        segments.append((width, n, None if i < len(EARLY) else chunk_of[col], col, g0))
        col += width * n
        g0 += n * (depth // DEPTH)
    assert col == shard == begin
    hbm = pl.BlockSpec(memory_space=pltpu.HBM)
    out_shape = [pltpu.HBM((rows, width), jnp.float32) for width in [*units, *LATE] for _ in range(n_dev)]
    out_shape += [pltpu.HBM((STATS, batch), jnp.float32)] * n_dev
    table = pltpu.VMEM((batch, LANES), jnp.float32)
    widest = max(width for width, _ in EARLY + LATE_UNITS)
    dma = pltpu.SemaphoreType.DMA
    res = pl.pallas_call(
        functools.partial(_logits_kernel, (n_dev, shard, segments, n_early, len(LATE))),
        in_specs=[hbm] * 4,
        out_specs=[hbm] * len(out_shape),
        out_shape=out_shape,
        scratch_shapes=[pltpu.VMEM((batch, width), jnp.float32) for width in units] + [
            pltpu.VMEM((batch, depth), jnp.bfloat16),
            pltpu.VMEM((depth, FIRST), jnp.bfloat16),
            pltpu.VMEM((SLOTS, DEPTH, widest), jnp.bfloat16),
            pltpu.VMEM((batch, widest), jnp.float32),
            pltpu.VMEM((2, batch, widest), jnp.float32),
            pltpu.VMEM((1, batch), jnp.float32),
            pltpu.VMEM((1, batch), jnp.int32),
            pltpu.VMEM((STATS, batch), jnp.float32),
            table,
            pltpu.VMEM((batch, LANES), jnp.int32),
            table,
            table,
            table,
            table,
            dma((depth // DEPTH,)),
            dma((SLOTS,)),
            dma((2, n_dev)),
            dma((n_dev,)),
            dma((2,)),
            dma((n_early,)),
            dma((n_early, n_dev)),
            dma((n_early, n_dev)),
            dma((n_dev,)),
            dma((n_dev,)),
        ],
        compiler_params=pltpu.CompilerParams(
            collective_id=0, has_side_effects=True, vmem_limit_bytes=52 * 2**20
        ),
        cost_estimate=pl.CostEstimate(
            flops=2 * batch * depth * shard,
            bytes_accessed=2 * depth * shard,
            transcendentals=batch * shard,
        ),
        name="logits",
    )(*(pltpu.with_memory_space_constraint(a, pltpu.HBM) for a in (x, w, invt, tgt)))
    blocks = [res[c * n_dev:(c + 1) * n_dev] for c in range(n_early + len(LATE) + 1)]
    return blocks[:n_early], blocks[n_early:-1], blocks[-1]


def _merge_kernel(n_dev, *refs):
    stats, (params_ref, at_ref) = refs[:n_dev], refs[n_dev:]
    me = lax.axis_index("vp")
    batch = stats[0].shape[1]
    rows = batch // n_dev
    ms = [s[0:1, :] for s in stats]
    top = functools.reduce(jnp.maximum, ms)
    keep = [jnp.exp(m - top) for m in ms]
    mass = [s[1:2, :] * k for s, k in zip(stats, keep)]
    upto = sum(s[2:3, :] * k for s, k in zip(stats, keep))
    total = sum(mass)
    at_ref[...] = upto / total
    values = [top, 1.0 / total]
    for p in range(n_dev):
        start = jnp.zeros_like(total)
        for q in range(n_dev):
            start += jnp.where((me ^ q) < (me ^ p), mass[q], 0.0)
        values.append(start)
    which = lax.broadcasted_iota(jnp.int32, (LANES, batch), 0)
    table = jnp.zeros((LANES, batch), jnp.float32)
    for i, v in enumerate(values):
        table = jnp.where(which == i, v, table)
    per_row = jnp.transpose(table)
    out = jnp.zeros((rows, LANES), jnp.float32)
    for d in range(n_dev):
        out = jnp.where(me == d, per_row[d * rows:(d + 1) * rows, :], out)
    params_ref[...] = out


def _merge(stats):
    n_dev = len(stats)
    batch = stats[0].shape[1]
    vmem = pl.BlockSpec(memory_space=pltpu.VMEM)
    return pl.pallas_call(
        functools.partial(_merge_kernel, n_dev),
        in_specs=[vmem] * n_dev,
        out_specs=[vmem] * 2,
        out_shape=[
            jax.ShapeDtypeStruct((batch // n_dev, LANES), jnp.float32),
            jax.ShapeDtypeStruct((1, batch), jnp.float32),
        ],
        cost_estimate=pl.CostEstimate(flops=100_000, bytes_accessed=100_000, transcendentals=1000),
        name="merge",
    )(*stats)


def _cdf_kernel(cfg, *refs):
    peers, shard, base, widths, first, last = cfg
    n = len(peers)
    width = sum(widths)
    parts, refs = [refs[a * n:(a + 1) * n] for a in range(len(widths))], refs[len(widths) * n:]
    params_ref = refs[0]
    if last:
        out_ref, y_ref, sems = refs[2:]
    else:
        out_ref, params_out, y_ref, sems = refs[1 if first else 2:]
    me = lax.axis_index("vp")
    rows = params_ref.shape[0]
    params = params_ref[...]
    top = jnp.broadcast_to(params[:, 0:1], (rows, LANES))
    inv = jnp.broadcast_to(params[:, 1:2], (rows, LANES))
    k_id = lax.broadcasted_iota(jnp.int32, (3 * LANES, 2 * LANES), 0) % LANES
    n_id = lax.broadcasted_iota(jnp.int32, (3 * LANES, 2 * LANES), 1)
    tri = jnp.where(k_id <= n_id, 1.0, 0.0).astype(jnp.bfloat16)
    lane = lax.broadcasted_iota(jnp.int32, (rows, LANES), 1)

    def unit(part, at, col, wide, carries):
        ends = []
        for j in range(n):
            cols = [pl.ds(col + t, LANES) for t in range(0, wide, LANES)]
            e = jnp.concatenate([jnp.exp(part[j][:, c] - top) for c in cols], axis=0)
            hi = e.astype(jnp.bfloat16)
            r1 = e - hi.astype(jnp.float32)
            mid = r1.astype(jnp.bfloat16)
            lo = (r1 - mid.astype(jnp.float32)).astype(jnp.bfloat16)
            sums = jnp.dot(jnp.concatenate([hi, mid, lo], axis=1), tri, preferred_element_type=jnp.float32)
            carry = carries[j]
            for t in range(len(cols)):
                block = slice(t * rows, (t + 1) * rows)
                y_ref[j, :, pl.ds(at + col + t * LANES, LANES)] = (sums[block, :LANES] + carry) * inv
                carry = carry + sums[block, LANES:]
            ends.append(carry)
        return tuple(ends)

    carries = tuple(jnp.broadcast_to(params[:, 2 + p:3 + p], (rows, LANES)) for p in peers)
    at = 0
    for part, wide in zip(parts, widths):
        n_full = wide // UNIT
        if n_full:
            carries = lax.fori_loop(
                0, n_full, lambda u, c, part=part, at=at: unit(part, at, pl.multiple_of(u * UNIT, UNIT), UNIT, c), carries
            )
        if wide % UNIT:
            carries = unit(part, at, n_full * UNIT, wide % UNIT, carries)
        at += wide
    copies = []
    updated = params
    for j, p in enumerate(peers):
        where = pl.multiple_of((me ^ p) * shard + base, LANES)
        copy = pltpu.make_async_copy(y_ref.at[j], out_ref.at[:, pl.ds(where, width)], sems.at[j])
        copy.start()
        copies.append(copy)
        updated = jnp.where(lane == 2 + p, carries[j], updated)
    if not last:
        params_out[...] = updated
    for copy in copies:
        copy.wait()


def _cdf(blocks, peers, params, out, n_dev, shard, base, last=False):
    n = len(peers)
    rows = blocks[0].shape[0]
    widths = tuple(b.shape[1] for b in blocks[::n])
    width = sum(widths)
    first = out is None
    vmem = pl.BlockSpec(memory_space=pltpu.VMEM)
    hbm = pl.BlockSpec(memory_space=pl.ANY)
    return pl.pallas_call(
        functools.partial(_cdf_kernel, (peers, shard, base, widths, first, last)),
        in_specs=[vmem] * (len(blocks) + 1) + ([] if first else [hbm]),
        out_specs=[hbm] + ([] if last else [vmem]),
        out_shape=[jax.ShapeDtypeStruct((rows, n_dev * shard), jnp.float32)]
        + ([] if last else [jax.ShapeDtypeStruct(params.shape, jnp.float32)]),
        scratch_shapes=[
            pltpu.VMEM((n, rows, width), jnp.float32),
            pltpu.SemaphoreType.DMA((n,)),
        ],
        input_output_aliases={} if first else {len(blocks) + 1: 0},
        compiler_params=pltpu.CompilerParams(vmem_limit_bytes=24 * 2**20),
        cost_estimate=pl.CostEstimate(
            flops=n * 2 * rows * width * 384,
            bytes_accessed=n * rows * width * 8,
            transcendentals=n * rows * width,
        ),
        name="cdf",
    )(*blocks, params, *(() if first else (out,)))


def solution(mesh):
    n_dev = mesh.shape["vp"]
    assert n_dev == 4

    def swap(a, p):
        return lax.ppermute(a, "vp", [(i, i ^ p) for i in range(n_dev)])

    def local_step(hidden, w_local, inv_temp, target_ids):
        shard = w_local.shape[1]
        early, late, packs = _logits(
            hidden, w_local, inv_temp.reshape(1, -1), target_ids.reshape(1, -1), n_dev
        )
        chunks = [(0, early)]
        begin = sum(made[0].shape[1] for made in early)
        for made in late:
            got = [made[0]]
            for p in range(1, n_dev):
                got.append(swap(made[p], p))
            chunks.append((begin, [got]))
            begin += made[0].shape[1]
        params, at_target = _merge(packs)
        out = None
        final = len(chunks) - 1
        plan = [(k, peers) for peers in ((0, 1), (2, 3)) for k in range(final + 1)]
        for i, (k, peers) in enumerate(plan):
            begin, got = chunks[k]
            blocks = [made[p] for made in got for p in peers]
            if k < final or peers[0] == 0:
                blocks = [pltpu.with_memory_space_constraint(a, pltpu.HBM) for a in blocks]
            res = _cdf(blocks, peers, params, out, n_dev, shard, begin, i == len(plan) - 1)
            out = res[0]
            params = res[1] if len(res) > 1 else None
        return out, at_target.reshape(-1)

    return jax.shard_map(
        local_step,
        mesh=mesh,
        in_specs=(P("dp", None), P(None, "vp"), P("dp"), P("dp")),
        out_specs=(P(("dp", "vp"), None), P("dp")),
        check_vma=False,
    )
```

```python
import functools

import jax
import jax.numpy as jnp
from jax import lax
from jax.experimental import pallas as pl
from jax.experimental.pallas import tpu as pltpu
from jax.sharding import PartitionSpec as P


LANES = 128
UNIT = 512
HALF = 256
DEPTH = 512
SLOTS = 9
FIRST, FIRSTS = 128, 4
EARLY = ((512, 1), (1024, 1), (2048, 2))
LATE = (4096, 2048, 2048, 1280, 384)
LATE_UNITS = ((2048, 2), (2048, 1), (2048, 1), (1280, 1), (384, 1))
STATS = 4


def _to_rows(vec_1xn):
    n = vec_1xn.shape[1]
    return jnp.transpose(jnp.broadcast_to(vec_1xn, (LANES, n)))


def _peer(me, p):
    return [me, me + 1 - 2 * lax.rem(me, 2), lax.rem(me + 2, 4), 3 - me][p]


def _logits_kernel(cfg, x_ref, w_ref, invt_ref, tgt_ref, *refs):
    n_dev, shard, segments, n_early, n_late = cfg
    refs = list(refs)

    def take(n):
        out = refs[:n]
        del refs[:n]
        return out

    early = [take(n_dev) for _ in range(n_early)]
    late = [take(n_dev) for _ in range(n_late)]
    packs = take(n_dev)
    zsend = take(n_early)
    xs, wfirst, wbuf, acc, zbuf, invt_v, tgt_v, pack_v = take(8)
    scale_rows, left_rows, tmp, m_ref, s_ref, t_ref = take(6)
    first_sem, w_sem, z_sem, x_sem, v_sem, own_sem, send_sem, recv_sem, pack_send, pack_recv = take(10)
    me = lax.axis_index("vp")
    batch, depth = xs.shape
    rows = batch // n_dev
    k_steps = depth // DEPTH
    assert SLOTS == k_steps + 1

    def rows_of(p):
        return pl.ds(pl.multiple_of(_peer(me, p) * rows, rows), rows)

    def fetch_w(seg, step):
        width, col0, g0 = segments[seg][0], segments[seg][3], segments[seg][4]
        slot = lax.rem(g0 + step, SLOTS)
        col = col0 + lax.div(step, k_steps) * width
        row = pl.multiple_of(lax.rem(step, k_steps) * DEPTH, DEPTH)
        return pltpu.make_async_copy(
            w_ref.at[pl.ds(row, DEPTH), pl.ds(pl.multiple_of(col, LANES), width)],
            wbuf.at[slot, :, pl.ds(0, width)],
            w_sem.at[slot],
        )

    def fetch_first(f, k):
        row = pl.ds(pl.multiple_of(k * DEPTH, DEPTH), DEPTH)
        return pltpu.make_async_copy(
            w_ref.at[row, pl.ds(f * FIRST, FIRST)], wfirst.at[f, row, :], first_sem.at[f, k]
        )

    def put_late(slot, c, off, width):
        return [
            pltpu.make_async_copy(
                zbuf.at[slot, pl.ds(p * rows, rows), pl.ds(0, width)],
                late[c][p].at[:, pl.ds(off, width)],
                z_sem.at[slot, p],
            )
            for p in range(n_dev)
        ]

    def put_own(u):
        return pltpu.make_async_copy(zsend[u].at[pl.ds(0, rows), :], early[u][0], own_sem.at[u])

    def send(u, p):
        return pltpu.make_async_remote_copy(
            src_ref=zsend[u].at[pl.ds(p * rows, rows), :],
            dst_ref=early[u][p],
            send_sem=send_sem.at[u, p],
            recv_sem=recv_sem.at[u, p],
            device_id={"vp": _peer(me, p)},
            device_id_type=pl.DeviceIdType.MESH,
        )

    x_copies = [
        pltpu.make_async_copy(x_ref.at[rows_of(p), :], xs.at[pl.ds(p * rows, rows), :], x_sem.at[p])
        for p in range(n_dev)
    ]
    small = [
        pltpu.make_async_copy(invt_ref, invt_v, v_sem.at[0]),
        pltpu.make_async_copy(tgt_ref, tgt_v, v_sem.at[1]),
    ]
    for copy in small + x_copies[2:]:
        copy.start()
    for k in range(k_steps):
        fetch_first(0, k).start()
    barrier = pltpu.get_barrier_semaphore()
    for p in range(1, n_dev):
        pl.semaphore_signal(
            barrier, inc=1, device_id={"vp": _peer(me, p)}, device_id_type=pl.DeviceIdType.MESH
        )
    m_ref[...] = jnp.full(m_ref.shape, -jnp.inf, jnp.float32)
    s_ref[...] = jnp.zeros_like(s_ref)
    t_ref[...] = jnp.zeros_like(t_ref)
    for copy in small:
        copy.wait()
    tmp[...] = _to_rows(invt_v[...])
    for p in range(n_dev):
        scale_rows[pl.ds(p * rows, rows), :] = tmp[rows_of(p), :]
    tmp[...] = _to_rows(tgt_v[...].astype(jnp.float32))
    lane = lax.broadcasted_iota(jnp.int32, (rows, LANES), 1)
    for p in range(n_dev):
        left_rows[pl.ds(p * rows, rows), :] = tmp[rows_of(p), :].astype(jnp.int32) - me * shard - lane
    for copy in x_copies[2:]:
        copy.wait()

    def multiply(seg, step):
        width = segments[seg][0]
        slot, k = lax.rem(segments[seg][4] + step, SLOTS), lax.rem(step, k_steps)
        x = xs[:, pl.ds(pl.multiple_of(k * DEPTH, DEPTH), DEPTH)]
        for off in range(0, width, HALF):
            wide = min(HALF, width - off)
            part = jnp.dot(x, wbuf[slot, :, off:off + wide], preferred_element_type=jnp.float32)
            acc[:, off:off + wide] = part + jnp.where(k == 0, 0.0, acc[:, off:off + wide])

    def finish(col, width, out_ref, out_off, lo=0, hi=batch):
        group = 32
        span = next(n for n in (UNIT, HALF, LANES) if width % n == 0)

        def some(j, _):
            at = pl.multiple_of(j * span, span)
            for r in range(lo, hi, group):
                block = slice(r, r + group)
                scale = scale_rows[block, :]
                tiles = []
                for t in range(0, span, LANES):
                    tile = acc[block, pl.ds(at + t, LANES)] * scale
                    out_ref[block, pl.ds(pl.multiple_of(out_off + at + t, LANES), LANES)] = tile
                    tiles.append(tile)
                m_old = m_ref[block, :]
                m_new = functools.reduce(jnp.maximum, tiles, m_old)
                keep = jnp.exp(m_old - m_new)
                total = s_ref[block, :] * keep
                upto = t_ref[block, :] * keep
                left = left_rows[block, :]
                for t, tile in enumerate(tiles):
                    e = jnp.exp(tile - m_new)
                    total += e
                    upto += jnp.where(left >= col + at + t * LANES, e, 0.0)
                m_ref[block, :] = m_new
                s_ref[block, :] = total
                t_ref[block, :] = upto
            return 0

        lax.fori_loop(0, width // span, some, 0)

    sent, own, stored = [], [], []

    def send_early(u, peers):
        for p in peers:
            copy = send(u, p)
            copy.start()
            sent.append(copy)

    far = 2 * rows

    def multiply_first(f, k, lo, hi):
        at = pl.ds(pl.multiple_of(k * DEPTH, DEPTH), DEPTH)
        part = jnp.dot(xs[lo:hi, at], wfirst[f, at, :], preferred_element_type=jnp.float32)
        acc[lo:hi, :FIRST] = part + jnp.where(k == 0, 0.0, acc[lo:hi, :FIRST])

    def first_far(f):
        def far_step(k, _):
            fetch_first(f, k).wait()

            if f + 1 < FIRSTS:
                fetch_first(f + 1, k).start()
            else:
                @pl.when(k == 0)
                def _():
                    for copy in x_copies[:2]:
                        copy.start()

                fetch_w(0, k).start()
            multiply_first(f, k, far, batch)
            return 0

        lax.fori_loop(0, k_steps, far_step, 0)
        finish(f * FIRST, FIRST, zsend[f], 0, far, batch)
        if f == 0:
            pl.semaphore_wait(barrier, n_dev - 1)
        send_early(f, (2, 3))

    def first_near(f):
        def near_step(k, _):
            multiply_first(f, k, 0, far)
            return 0

        lax.fori_loop(0, k_steps, near_step, 0)
        finish(f * FIRST, FIRST, zsend[f], 0, 0, far)
        send_early(f, (1,))
        copy = put_own(f)
        copy.start()
        own.append(copy)

    for f in range(FIRSTS):
        first_far(f)
    for copy in x_copies[:2]:
        copy.wait()
    early_units = FIRSTS

    for seg, (width, n, chunk, col0, g0) in enumerate(segments):
        for i in range(n):

            def body(k, _, seg=seg, i=i, n=n):
                step = i * k_steps + k
                ahead = step + SLOTS - 1

                @pl.when(ahead < n * k_steps)
                def _():
                    fetch_w(seg, ahead).start()

                if seg + 1 < len(segments):
                    @pl.when(ahead >= n * k_steps)
                    def _():
                        fetch_w(seg + 1, ahead - n * k_steps).start()

                fetch_w(seg, step).wait()
                multiply(seg, step)
                return 0

            lax.fori_loop(0, k_steps, body, 0)
            col = col0 + i * width
            if chunk is None:
                u = early_units
                early_units += 1
                finish(col, width, zsend[u], 0)
                send_early(u, (2, 3, 1))
                copy = put_own(u)
                copy.start()
                own.append(copy)
                if u == FIRSTS + 1:
                    for f in range(FIRSTS):
                        first_near(f)
            else:
                slot = len(stored) % 2
                if len(stored) >= 2:
                    for copy in stored[-2]:
                        copy.wait()
                finish(col, width, zbuf.at[slot], 0)
                c, off = chunk
                copies = put_late(slot, c, off + i * width, width)
                for copy in copies:
                    copy.start()
                stored.append(copies)
    m = m_ref[...]
    m_row = jnp.max(m, axis=1, keepdims=True)
    keep = jnp.exp(m - m_row)
    s_row = jnp.sum(s_ref[...] * keep, axis=1, keepdims=True)
    t_row = jnp.sum(t_ref[...] * keep, axis=1, keepdims=True)
    which = lax.broadcasted_iota(jnp.int32, m.shape, 1)
    packed = jnp.where(which == 0, m_row, jnp.where(which == 1, s_row, t_row))
    for p in range(n_dev):
        tmp[rows_of(p), :] = packed[p * rows:(p + 1) * rows, :]
    pack_v[...] = jnp.transpose(tmp[...])[:STATS, :]
    for p in (2, 3, 1):
        copy = pltpu.make_async_remote_copy(
            src_ref=pack_v,
            dst_ref=packs[p],
            send_sem=pack_send.at[p],
            recv_sem=pack_recv.at[p],
            device_id={"vp": _peer(me, p)},
            device_id_type=pl.DeviceIdType.MESH,
        )
        copy.start()
        sent.append(copy)
    copy = pltpu.make_async_copy(pack_v, packs[0], pack_send.at[0])
    copy.start()
    own.append(copy)
    for copies in stored[-2:]:
        for copy in copies:
            copy.wait()
    for copy in own + sent:
        copy.wait()


def _logits(x, w, invt, tgt, n_dev):
    batch, depth = x.shape
    shard = w.shape[1]
    rows = batch // n_dev
    segments, col, g0 = [], FIRST * FIRSTS, 0
    chunk_of = {}
    units = [FIRST] * FIRSTS + [width for width, n in EARLY for _ in range(n)]
    n_early, begin = len(units), sum(units)
    for c, width in enumerate(LATE):
        chunk_of.update({begin + i: (c, i) for i in range(0, width, LANES)})
        begin += width
    for i, (width, n) in enumerate(EARLY + LATE_UNITS):
        segments.append((width, n, None if i < len(EARLY) else chunk_of[col], col, g0))
        col += width * n
        g0 += n * (depth // DEPTH)
    assert col == shard == begin
    hbm = pl.BlockSpec(memory_space=pltpu.HBM)
    out_shape = [pltpu.HBM((rows, width), jnp.float32) for width in [*units, *LATE] for _ in range(n_dev)]
    out_shape += [pltpu.HBM((STATS, batch), jnp.float32)] * n_dev
    table = pltpu.VMEM((batch, LANES), jnp.float32)
    widest = max(width for width, _ in EARLY + LATE_UNITS)
    dma = pltpu.SemaphoreType.DMA
    res = pl.pallas_call(
        functools.partial(_logits_kernel, (n_dev, shard, segments, n_early, len(LATE))),
        in_specs=[hbm] * 4,
        out_specs=[hbm] * len(out_shape),
        out_shape=out_shape,
        scratch_shapes=[pltpu.VMEM((batch, width), jnp.float32) for width in units] + [
            pltpu.VMEM((batch, depth), jnp.bfloat16),
            pltpu.VMEM((FIRSTS, depth, FIRST), jnp.bfloat16),
            pltpu.VMEM((SLOTS, DEPTH, widest), jnp.bfloat16),
            pltpu.VMEM((batch, widest), jnp.float32),
            pltpu.VMEM((2, batch, widest), jnp.float32),
            pltpu.VMEM((1, batch), jnp.float32),
            pltpu.VMEM((1, batch), jnp.int32),
            pltpu.VMEM((STATS, batch), jnp.float32),
            table,
            pltpu.VMEM((batch, LANES), jnp.int32),
            table,
            table,
            table,
            table,
            dma((FIRSTS, depth // DEPTH)),
            dma((SLOTS,)),
            dma((2, n_dev)),
            dma((n_dev,)),
            dma((2,)),
            dma((n_early,)),
            dma((n_early, n_dev)),
            dma((n_early, n_dev)),
            dma((n_dev,)),
            dma((n_dev,)),
        ],
        compiler_params=pltpu.CompilerParams(
            collective_id=0, has_side_effects=True, vmem_limit_bytes=52 * 2**20
        ),
        cost_estimate=pl.CostEstimate(
            flops=2 * batch * depth * shard,
            bytes_accessed=2 * depth * shard,
            transcendentals=batch * shard,
        ),
        name="logits",
    )(*(pltpu.with_memory_space_constraint(a, pltpu.HBM) for a in (x, w, invt, tgt)))
    blocks = [res[c * n_dev:(c + 1) * n_dev] for c in range(n_early + len(LATE) + 1)]
    return blocks[:n_early], blocks[n_early:-1], blocks[-1]


def _merge_kernel(n_dev, *refs):
    stats, (params_ref, at_ref) = refs[:n_dev], refs[n_dev:]
    me = lax.axis_index("vp")
    batch = stats[0].shape[1]
    rows = batch // n_dev
    ms = [s[0:1, :] for s in stats]
    top = functools.reduce(jnp.maximum, ms)
    keep = [jnp.exp(m - top) for m in ms]
    mass = [s[1:2, :] * k for s, k in zip(stats, keep)]
    upto = sum(s[2:3, :] * k for s, k in zip(stats, keep))
    total = sum(mass)
    at_ref[...] = upto / total
    values = [top, 1.0 / total]
    for p in range(n_dev):
        start = jnp.zeros_like(total)
        for q in range(n_dev):
            start += jnp.where((me ^ q) < (me ^ p), mass[q], 0.0)
        values.append(start)
    which = lax.broadcasted_iota(jnp.int32, (LANES, batch), 0)
    table = jnp.zeros((LANES, batch), jnp.float32)
    for i, v in enumerate(values):
        table = jnp.where(which == i, v, table)
    per_row = jnp.transpose(table)
    out = jnp.zeros((rows, LANES), jnp.float32)
    for d in range(n_dev):
        out = jnp.where(me == d, per_row[d * rows:(d + 1) * rows, :], out)
    params_ref[...] = out


def _merge(stats):
    n_dev = len(stats)
    batch = stats[0].shape[1]
    vmem = pl.BlockSpec(memory_space=pltpu.VMEM)
    return pl.pallas_call(
        functools.partial(_merge_kernel, n_dev),
        in_specs=[vmem] * n_dev,
        out_specs=[vmem] * 2,
        out_shape=[
            jax.ShapeDtypeStruct((batch // n_dev, LANES), jnp.float32),
            jax.ShapeDtypeStruct((1, batch), jnp.float32),
        ],
        cost_estimate=pl.CostEstimate(flops=100_000, bytes_accessed=100_000, transcendentals=1000),
        name="merge",
    )(*stats)


def _cdf_kernel(cfg, *refs):
    peers, shard, base, widths, first, last = cfg
    n = len(peers)
    width = sum(widths)
    parts, refs = [refs[a * n:(a + 1) * n] for a in range(len(widths))], refs[len(widths) * n:]
    params_ref = refs[0]
    if last:
        out_ref, y_ref, sems = refs[2:]
    else:
        out_ref, params_out, y_ref, sems = refs[1 if first else 2:]
    me = lax.axis_index("vp")
    rows = params_ref.shape[0]
    params = params_ref[...]
    top = jnp.broadcast_to(params[:, 0:1], (rows, LANES))
    inv = jnp.broadcast_to(params[:, 1:2], (rows, LANES))
    k_id = lax.broadcasted_iota(jnp.int32, (3 * LANES, 2 * LANES), 0) % LANES
    n_id = lax.broadcasted_iota(jnp.int32, (3 * LANES, 2 * LANES), 1)
    tri = jnp.where(k_id <= n_id, 1.0, 0.0).astype(jnp.bfloat16)
    lane = lax.broadcasted_iota(jnp.int32, (rows, LANES), 1)

    def unit(part, at, col, wide, carries):
        ends = []
        for j in range(n):
            cols = [pl.ds(col + t, LANES) for t in range(0, wide, LANES)]
            e = jnp.concatenate([jnp.exp(part[j][:, c] - top) for c in cols], axis=0)
            hi = e.astype(jnp.bfloat16)
            r1 = e - hi.astype(jnp.float32)
            mid = r1.astype(jnp.bfloat16)
            lo = (r1 - mid.astype(jnp.float32)).astype(jnp.bfloat16)
            sums = jnp.dot(jnp.concatenate([hi, mid, lo], axis=1), tri, preferred_element_type=jnp.float32)
            carry = carries[j]
            for t in range(len(cols)):
                block = slice(t * rows, (t + 1) * rows)
                y_ref[j, :, pl.ds(at + col + t * LANES, LANES)] = (sums[block, :LANES] + carry) * inv
                carry = carry + sums[block, LANES:]
            ends.append(carry)
        return tuple(ends)

    carries = tuple(jnp.broadcast_to(params[:, 2 + p:3 + p], (rows, LANES)) for p in peers)
    at = 0
    for part, wide in zip(parts, widths):
        n_full = wide // UNIT
        if n_full:
            carries = lax.fori_loop(
                0, n_full, lambda u, c, part=part, at=at: unit(part, at, pl.multiple_of(u * UNIT, UNIT), UNIT, c), carries
            )
        if wide % UNIT:
            carries = unit(part, at, n_full * UNIT, wide % UNIT, carries)
        at += wide
    copies = []
    updated = params
    for j, p in enumerate(peers):
        where = pl.multiple_of((me ^ p) * shard + base, LANES)
        copy = pltpu.make_async_copy(y_ref.at[j], out_ref.at[:, pl.ds(where, width)], sems.at[j])
        copy.start()
        copies.append(copy)
        updated = jnp.where(lane == 2 + p, carries[j], updated)
    if not last:
        params_out[...] = updated
    for copy in copies:
        copy.wait()


def _cdf(blocks, peers, params, out, n_dev, shard, base, last=False):
    n = len(peers)
    rows = blocks[0].shape[0]
    widths = tuple(b.shape[1] for b in blocks[::n])
    width = sum(widths)
    first = out is None
    vmem = pl.BlockSpec(memory_space=pltpu.VMEM)
    hbm = pl.BlockSpec(memory_space=pl.ANY)
    return pl.pallas_call(
        functools.partial(_cdf_kernel, (peers, shard, base, widths, first, last)),
        in_specs=[vmem] * (len(blocks) + 1) + ([] if first else [hbm]),
        out_specs=[hbm] + ([] if last else [vmem]),
        out_shape=[jax.ShapeDtypeStruct((rows, n_dev * shard), jnp.float32)]
        + ([] if last else [jax.ShapeDtypeStruct(params.shape, jnp.float32)]),
        scratch_shapes=[
            pltpu.VMEM((n, rows, width), jnp.float32),
            pltpu.SemaphoreType.DMA((n,)),
        ],
        input_output_aliases={} if first else {len(blocks) + 1: 0},
        compiler_params=pltpu.CompilerParams(vmem_limit_bytes=24 * 2**20),
        cost_estimate=pl.CostEstimate(
            flops=n * 2 * rows * width * 384,
            bytes_accessed=n * rows * width * 8,
            transcendentals=n * rows * width,
        ),
        name="cdf",
    )(*blocks, params, *(() if first else (out,)))


def solution(mesh):
    n_dev = mesh.shape["vp"]
    assert n_dev == 4

    def swap(a, p):
        return lax.ppermute(a, "vp", [(i, i ^ p) for i in range(n_dev)])

    def local_step(hidden, w_local, inv_temp, target_ids):
        shard = w_local.shape[1]
        early, late, packs = _logits(
            hidden, w_local, inv_temp.reshape(1, -1), target_ids.reshape(1, -1), n_dev
        )
        chunks = [(0, early)]
        begin = sum(made[0].shape[1] for made in early)
        for made in late:
            got = [made[0]]
            for p in range(1, n_dev):
                got.append(swap(made[p], p))
            chunks.append((begin, [got]))
            begin += made[0].shape[1]
        params, at_target = _merge(packs)
        out = None
        final = len(chunks) - 1
        plan = [(k, peers) for peers in ((0, 1), (2, 3)) for k in range(final + 1)]
        for i, (k, peers) in enumerate(plan):
            begin, got = chunks[k]
            blocks = [made[p] for made in got for p in peers]
            if k < final or peers[0] == 0:
                blocks = [pltpu.with_memory_space_constraint(a, pltpu.HBM) for a in blocks]
            res = _cdf(blocks, peers, params, out, n_dev, shard, begin, i == len(plan) - 1)
            out = res[0]
            params = res[1] if len(res) > 1 else None
        return out, at_target.reshape(-1)

    return jax.shard_map(
        local_step,
        mesh=mesh,
        in_specs=(P("dp", None), P(None, "vp"), P("dp"), P("dp")),
        out_specs=(P(("dp", "vp"), None), P("dp")),
        check_vma=False,
    )
```

```python
import functools

import jax
import jax.numpy as jnp
from jax import lax
from jax.experimental import pallas as pl
from jax.experimental.pallas import tpu as pltpu
from jax.sharding import PartitionSpec as P


LANES = 128
UNIT = 512
HALF = 256
DEPTH = 512
SLOTS = 9
FIRST = 256
EARLY = ((256, 1), (512, 1), (1024, 1), (2048, 2))
LATE = (4096, 2048, 2048, 1280, 384)
LATE_UNITS = ((2048, 2), (2048, 1), (2048, 1), (1280, 1), (384, 1))
STATS = 4


def _to_rows(vec_1xn):
    n = vec_1xn.shape[1]
    return jnp.transpose(jnp.broadcast_to(vec_1xn, (LANES, n)))


def _peer(me, p):
    return [me, me + 1 - 2 * lax.rem(me, 2), lax.rem(me + 2, 4), 3 - me][p]


def _logits_kernel(cfg, x_ref, w_ref, invt_ref, tgt_ref, *refs):
    n_dev, shard, segments, n_early, n_late = cfg
    refs = list(refs)

    def take(n):
        out = refs[:n]
        del refs[:n]
        return out

    early = [take(n_dev) for _ in range(n_early)]
    late = [take(n_dev) for _ in range(n_late)]
    packs = take(n_dev)
    zsend = take(n_early)
    xs, wfirst, wbuf, acc, zbuf, invt_v, tgt_v, pack_v = take(8)
    scale_rows, left_rows, tmp, m_ref, s_ref, t_ref = take(6)
    first_sem, w_sem, z_sem, x_sem, v_sem, own_sem, send_sem, recv_sem, pack_send, pack_recv = take(10)
    me = lax.axis_index("vp")
    batch, depth = xs.shape
    rows = batch // n_dev
    k_steps = depth // DEPTH
    assert SLOTS == k_steps + 1

    def rows_of(p):
        return pl.ds(pl.multiple_of(_peer(me, p) * rows, rows), rows)

    def fetch_w(seg, step):
        width, col0, g0 = segments[seg][0], segments[seg][3], segments[seg][4]
        slot = lax.rem(g0 + step, SLOTS)
        col = col0 + lax.div(step, k_steps) * width
        row = pl.multiple_of(lax.rem(step, k_steps) * DEPTH, DEPTH)
        return pltpu.make_async_copy(
            w_ref.at[pl.ds(row, DEPTH), pl.ds(pl.multiple_of(col, LANES), width)],
            wbuf.at[slot, :, pl.ds(0, width)],
            w_sem.at[slot],
        )

    def fetch_first(k):
        row = pl.ds(pl.multiple_of(k * DEPTH, DEPTH), DEPTH)
        return pltpu.make_async_copy(w_ref.at[row, pl.ds(0, FIRST)], wfirst.at[row, :], first_sem.at[k])

    def put_late(slot, c, off, width):
        return [
            pltpu.make_async_copy(
                zbuf.at[slot, pl.ds(p * rows, rows), pl.ds(0, width)],
                late[c][p].at[:, pl.ds(off, width)],
                z_sem.at[slot, p],
            )
            for p in range(n_dev)
        ]

    def put_own(u):
        return pltpu.make_async_copy(zsend[u].at[pl.ds(0, rows), :], early[u][0], own_sem.at[u])

    def send(u, p):
        return pltpu.make_async_remote_copy(
            src_ref=zsend[u].at[pl.ds(p * rows, rows), :],
            dst_ref=early[u][p],
            send_sem=send_sem.at[u, p],
            recv_sem=recv_sem.at[u, p],
            device_id={"vp": _peer(me, p)},
            device_id_type=pl.DeviceIdType.MESH,
        )

    x_copies = [
        pltpu.make_async_copy(x_ref.at[rows_of(p), :], xs.at[pl.ds(p * rows, rows), :], x_sem.at[p])
        for p in range(n_dev)
    ]
    small = [
        pltpu.make_async_copy(invt_ref, invt_v, v_sem.at[0]),
        pltpu.make_async_copy(tgt_ref, tgt_v, v_sem.at[1]),
    ]
    for copy in small + x_copies[2:]:
        copy.start()
    for k in range(k_steps):
        fetch_first(k).start()
    barrier = pltpu.get_barrier_semaphore()
    for p in range(1, n_dev):
        pl.semaphore_signal(
            barrier, inc=1, device_id={"vp": _peer(me, p)}, device_id_type=pl.DeviceIdType.MESH
        )
    m_ref[...] = jnp.full(m_ref.shape, -jnp.inf, jnp.float32)
    s_ref[...] = jnp.zeros_like(s_ref)
    t_ref[...] = jnp.zeros_like(t_ref)
    for copy in small:
        copy.wait()
    tmp[...] = _to_rows(invt_v[...])
    for p in range(n_dev):
        scale_rows[pl.ds(p * rows, rows), :] = tmp[rows_of(p), :]
    tmp[...] = _to_rows(tgt_v[...].astype(jnp.float32))
    lane = lax.broadcasted_iota(jnp.int32, (rows, LANES), 1)
    for p in range(n_dev):
        left_rows[pl.ds(p * rows, rows), :] = tmp[rows_of(p), :].astype(jnp.int32) - me * shard - lane
    for copy in x_copies[2:]:
        copy.wait()

    def multiply(seg, step):
        width = segments[seg][0]
        slot, k = lax.rem(segments[seg][4] + step, SLOTS), lax.rem(step, k_steps)
        x = xs[:, pl.ds(pl.multiple_of(k * DEPTH, DEPTH), DEPTH)]
        for off in range(0, width, HALF):
            wide = min(HALF, width - off)
            part = jnp.dot(x, wbuf[slot, :, off:off + wide], preferred_element_type=jnp.float32)
            acc[:, off:off + wide] = part + jnp.where(k == 0, 0.0, acc[:, off:off + wide])

    def finish(col, width, out_ref, out_off, lo=0, hi=batch):
        group = 32
        span = next(n for n in (UNIT, HALF, LANES) if width % n == 0)

        def some(j, _):
            at = pl.multiple_of(j * span, span)
            for r in range(lo, hi, group):
                block = slice(r, r + group)
                scale = scale_rows[block, :]
                tiles = []
                for t in range(0, span, LANES):
                    tile = acc[block, pl.ds(at + t, LANES)] * scale
                    out_ref[block, pl.ds(pl.multiple_of(out_off + at + t, LANES), LANES)] = tile
                    tiles.append(tile)
                m_old = m_ref[block, :]
                m_new = functools.reduce(jnp.maximum, tiles, m_old)
                keep = jnp.exp(m_old - m_new)
                total = s_ref[block, :] * keep
                upto = t_ref[block, :] * keep
                left = left_rows[block, :]
                for t, tile in enumerate(tiles):
                    e = jnp.exp(tile - m_new)
                    total += e
                    upto += jnp.where(left >= col + at + t * LANES, e, 0.0)
                m_ref[block, :] = m_new
                s_ref[block, :] = total
                t_ref[block, :] = upto
            return 0

        lax.fori_loop(0, width // span, some, 0)

    sent, own, stored = [], [], []

    def send_early(u, peers):
        for p in peers:
            copy = send(u, p)
            copy.start()
            sent.append(copy)

    far = 2 * rows

    def multiply_first(k, lo, hi):
        at = pl.ds(pl.multiple_of(k * DEPTH, DEPTH), DEPTH)
        part = jnp.dot(xs[lo:hi, at], wfirst[at, :], preferred_element_type=jnp.float32)
        acc[lo:hi, :FIRST] = part + jnp.where(k == 0, 0.0, acc[lo:hi, :FIRST])

    def far_step(k, _):
        fetch_first(k).wait()

        @pl.when(k == 0)
        def _():
            for copy in x_copies[:2]:
                copy.start()

        fetch_w(0, k).start()
        multiply_first(k, far, batch)
        return 0

    def near_step(k, _):
        multiply_first(k, 0, far)
        return 0

    lax.fori_loop(0, k_steps, far_step, 0)
    finish(0, FIRST, zsend[0], 0, far, batch)
    pl.semaphore_wait(barrier, n_dev - 1)
    send_early(0, (2, 3))
    for copy in x_copies[:2]:
        copy.wait()

    def first_near():
        lax.fori_loop(0, k_steps, near_step, 0)
        finish(0, FIRST, zsend[0], 0, 0, far)
        send_early(0, (1,))
        copy = put_own(0)
        copy.start()
        own.append(copy)

    early_units = 1
    for seg, (width, n, chunk, col0, g0) in enumerate(segments):
        for i in range(n):

            def body(k, _, seg=seg, i=i, n=n):
                step = i * k_steps + k
                ahead = step + SLOTS - 1

                @pl.when(ahead < n * k_steps)
                def _():
                    fetch_w(seg, ahead).start()

                if seg + 1 < len(segments):
                    @pl.when(ahead >= n * k_steps)
                    def _():
                        fetch_w(seg + 1, ahead - n * k_steps).start()

                fetch_w(seg, step).wait()
                multiply(seg, step)
                return 0

            lax.fori_loop(0, k_steps, body, 0)
            col = col0 + i * width
            if chunk is None:
                u = early_units
                early_units += 1
                finish(col, width, zsend[u], 0)
                send_early(u, (2, 3, 1))
                copy = put_own(u)
                copy.start()
                own.append(copy)
                if u == 2:
                    first_near()
            else:
                slot = len(stored) % 2
                if len(stored) >= 2:
                    for copy in stored[-2]:
                        copy.wait()
                finish(col, width, zbuf.at[slot], 0)
                c, off = chunk
                copies = put_late(slot, c, off + i * width, width)
                for copy in copies:
                    copy.start()
                stored.append(copies)
    m = m_ref[...]
    m_row = jnp.max(m, axis=1, keepdims=True)
    keep = jnp.exp(m - m_row)
    s_row = jnp.sum(s_ref[...] * keep, axis=1, keepdims=True)
    t_row = jnp.sum(t_ref[...] * keep, axis=1, keepdims=True)
    which = lax.broadcasted_iota(jnp.int32, m.shape, 1)
    packed = jnp.where(which == 0, m_row, jnp.where(which == 1, s_row, t_row))
    for p in range(n_dev):
        tmp[rows_of(p), :] = packed[p * rows:(p + 1) * rows, :]
    pack_v[...] = jnp.transpose(tmp[...])[:STATS, :]
    for p in (2, 3, 1):
        copy = pltpu.make_async_remote_copy(
            src_ref=pack_v,
            dst_ref=packs[p],
            send_sem=pack_send.at[p],
            recv_sem=pack_recv.at[p],
            device_id={"vp": _peer(me, p)},
            device_id_type=pl.DeviceIdType.MESH,
        )
        copy.start()
        sent.append(copy)
    copy = pltpu.make_async_copy(pack_v, packs[0], pack_send.at[0])
    copy.start()
    own.append(copy)
    for copies in stored[-2:]:
        for copy in copies:
            copy.wait()
    for copy in own + sent:
        copy.wait()


def _logits(x, w, invt, tgt, n_dev):
    batch, depth = x.shape
    shard = w.shape[1]
    rows = batch // n_dev
    segments, col, g0 = [], FIRST, 0
    chunk_of = {}
    units = [FIRST] + [width for width, n in EARLY for _ in range(n)]
    n_early, begin = len(units), sum(units)
    for c, width in enumerate(LATE):
        chunk_of.update({begin + i: (c, i) for i in range(0, width, LANES)})
        begin += width
    for i, (width, n) in enumerate(EARLY + LATE_UNITS):
        segments.append((width, n, None if i < len(EARLY) else chunk_of[col], col, g0))
        col += width * n
        g0 += n * (depth // DEPTH)
    assert col == shard == begin
    hbm = pl.BlockSpec(memory_space=pltpu.HBM)
    out_shape = [pltpu.HBM((rows, width), jnp.float32) for width in [*units, *LATE] for _ in range(n_dev)]
    out_shape += [pltpu.HBM((STATS, batch), jnp.float32)] * n_dev
    table = pltpu.VMEM((batch, LANES), jnp.float32)
    widest = max(width for width, _ in EARLY + LATE_UNITS)
    dma = pltpu.SemaphoreType.DMA
    res = pl.pallas_call(
        functools.partial(_logits_kernel, (n_dev, shard, segments, n_early, len(LATE))),
        in_specs=[hbm] * 4,
        out_specs=[hbm] * len(out_shape),
        out_shape=out_shape,
        scratch_shapes=[pltpu.VMEM((batch, width), jnp.float32) for width in units] + [
            pltpu.VMEM((batch, depth), jnp.bfloat16),
            pltpu.VMEM((depth, FIRST), jnp.bfloat16),
            pltpu.VMEM((SLOTS, DEPTH, widest), jnp.bfloat16),
            pltpu.VMEM((batch, widest), jnp.float32),
            pltpu.VMEM((2, batch, widest), jnp.float32),
            pltpu.VMEM((1, batch), jnp.float32),
            pltpu.VMEM((1, batch), jnp.int32),
            pltpu.VMEM((STATS, batch), jnp.float32),
            table,
            pltpu.VMEM((batch, LANES), jnp.int32),
            table,
            table,
            table,
            table,
            dma((depth // DEPTH,)),
            dma((SLOTS,)),
            dma((2, n_dev)),
            dma((n_dev,)),
            dma((2,)),
            dma((n_early,)),
            dma((n_early, n_dev)),
            dma((n_early, n_dev)),
            dma((n_dev,)),
            dma((n_dev,)),
        ],
        compiler_params=pltpu.CompilerParams(
            collective_id=0, has_side_effects=True, vmem_limit_bytes=52 * 2**20
        ),
        cost_estimate=pl.CostEstimate(
            flops=2 * batch * depth * shard,
            bytes_accessed=2 * depth * shard,
            transcendentals=batch * shard,
        ),
        name="logits",
    )(*(pltpu.with_memory_space_constraint(a, pltpu.HBM) for a in (x, w, invt, tgt)))
    blocks = [res[c * n_dev:(c + 1) * n_dev] for c in range(n_early + len(LATE) + 1)]
    return blocks[:n_early], blocks[n_early:-1], blocks[-1]


def _merge_kernel(n_dev, *refs):
    stats, (params_ref, at_ref) = refs[:n_dev], refs[n_dev:]
    me = lax.axis_index("vp")
    batch = stats[0].shape[1]
    rows = batch // n_dev
    ms = [s[0:1, :] for s in stats]
    top = functools.reduce(jnp.maximum, ms)
    keep = [jnp.exp(m - top) for m in ms]
    mass = [s[1:2, :] * k for s, k in zip(stats, keep)]
    upto = sum(s[2:3, :] * k for s, k in zip(stats, keep))
    total = sum(mass)
    at_ref[...] = upto / total
    values = [top, 1.0 / total]
    for p in range(n_dev):
        start = jnp.zeros_like(total)
        for q in range(n_dev):
            start += jnp.where((me ^ q) < (me ^ p), mass[q], 0.0)
        values.append(start)
    which = lax.broadcasted_iota(jnp.int32, (LANES, batch), 0)
    table = jnp.zeros((LANES, batch), jnp.float32)
    for i, v in enumerate(values):
        table = jnp.where(which == i, v, table)
    per_row = jnp.transpose(table)
    out = jnp.zeros((rows, LANES), jnp.float32)
    for d in range(n_dev):
        out = jnp.where(me == d, per_row[d * rows:(d + 1) * rows, :], out)
    params_ref[...] = out


def _merge(stats):
    n_dev = len(stats)
    batch = stats[0].shape[1]
    vmem = pl.BlockSpec(memory_space=pltpu.VMEM)
    return pl.pallas_call(
        functools.partial(_merge_kernel, n_dev),
        in_specs=[vmem] * n_dev,
        out_specs=[vmem] * 2,
        out_shape=[
            jax.ShapeDtypeStruct((batch // n_dev, LANES), jnp.float32),
            jax.ShapeDtypeStruct((1, batch), jnp.float32),
        ],
        cost_estimate=pl.CostEstimate(flops=100_000, bytes_accessed=100_000, transcendentals=1000),
        name="merge",
    )(*stats)


def _cdf_kernel(cfg, *refs):
    peers, shard, base, widths, first, last = cfg
    n = len(peers)
    width = sum(widths)
    parts, refs = [refs[a * n:(a + 1) * n] for a in range(len(widths))], refs[len(widths) * n:]
    params_ref = refs[0]
    if last:
        out_ref, y_ref, sems = refs[2:]
    else:
        out_ref, params_out, y_ref, sems = refs[1 if first else 2:]
    me = lax.axis_index("vp")
    rows = params_ref.shape[0]
    params = params_ref[...]
    top = jnp.broadcast_to(params[:, 0:1], (rows, LANES))
    inv = jnp.broadcast_to(params[:, 1:2], (rows, LANES))
    k_id = lax.broadcasted_iota(jnp.int32, (3 * LANES, 2 * LANES), 0) % LANES
    n_id = lax.broadcasted_iota(jnp.int32, (3 * LANES, 2 * LANES), 1)
    tri = jnp.where(k_id <= n_id, 1.0, 0.0).astype(jnp.bfloat16)
    lane = lax.broadcasted_iota(jnp.int32, (rows, LANES), 1)

    def unit(part, at, col, wide, carries):
        ends = []
        for j in range(n):
            cols = [pl.ds(col + t, LANES) for t in range(0, wide, LANES)]
            e = jnp.concatenate([jnp.exp(part[j][:, c] - top) for c in cols], axis=0)
            hi = e.astype(jnp.bfloat16)
            r1 = e - hi.astype(jnp.float32)
            mid = r1.astype(jnp.bfloat16)
            lo = (r1 - mid.astype(jnp.float32)).astype(jnp.bfloat16)
            sums = jnp.dot(jnp.concatenate([hi, mid, lo], axis=1), tri, preferred_element_type=jnp.float32)
            carry = carries[j]
            for t in range(len(cols)):
                block = slice(t * rows, (t + 1) * rows)
                y_ref[j, :, pl.ds(at + col + t * LANES, LANES)] = (sums[block, :LANES] + carry) * inv
                carry = carry + sums[block, LANES:]
            ends.append(carry)
        return tuple(ends)

    carries = tuple(jnp.broadcast_to(params[:, 2 + p:3 + p], (rows, LANES)) for p in peers)
    at = 0
    for part, wide in zip(parts, widths):
        n_full = wide // UNIT
        if n_full:
            carries = lax.fori_loop(
                0, n_full, lambda u, c, part=part, at=at: unit(part, at, pl.multiple_of(u * UNIT, UNIT), UNIT, c), carries
            )
        if wide % UNIT:
            carries = unit(part, at, n_full * UNIT, wide % UNIT, carries)
        at += wide
    copies = []
    updated = params
    for j, p in enumerate(peers):
        where = pl.multiple_of((me ^ p) * shard + base, LANES)
        copy = pltpu.make_async_copy(y_ref.at[j], out_ref.at[:, pl.ds(where, width)], sems.at[j])
        copy.start()
        copies.append(copy)
        updated = jnp.where(lane == 2 + p, carries[j], updated)
    if not last:
        params_out[...] = updated
    for copy in copies:
        copy.wait()


def _cdf(blocks, peers, params, out, n_dev, shard, base, last=False):
    n = len(peers)
    rows = blocks[0].shape[0]
    widths = tuple(b.shape[1] for b in blocks[::n])
    width = sum(widths)
    first = out is None
    vmem = pl.BlockSpec(memory_space=pltpu.VMEM)
    hbm = pl.BlockSpec(memory_space=pl.ANY)
    return pl.pallas_call(
        functools.partial(_cdf_kernel, (peers, shard, base, widths, first, last)),
        in_specs=[vmem] * (len(blocks) + 1) + ([] if first else [hbm]),
        out_specs=[hbm] + ([] if last else [vmem]),
        out_shape=[jax.ShapeDtypeStruct((rows, n_dev * shard), jnp.float32)]
        + ([] if last else [jax.ShapeDtypeStruct(params.shape, jnp.float32)]),
        scratch_shapes=[
            pltpu.VMEM((n, rows, width), jnp.float32),
            pltpu.SemaphoreType.DMA((n,)),
        ],
        input_output_aliases={} if first else {len(blocks) + 1: 0},
        compiler_params=pltpu.CompilerParams(vmem_limit_bytes=24 * 2**20),
        cost_estimate=pl.CostEstimate(
            flops=n * 2 * rows * width * 384,
            bytes_accessed=n * rows * width * 8,
            transcendentals=n * rows * width,
        ),
        name="cdf",
    )(*blocks, params, *(() if first else (out,)))


def solution(mesh):
    n_dev = mesh.shape["vp"]
    assert n_dev == 4

    def swap(a, p):
        return lax.ppermute(a, "vp", [(i, i ^ p) for i in range(n_dev)])

    def local_step(hidden, w_local, inv_temp, target_ids):
        shard = w_local.shape[1]
        early, late, packs = _logits(
            hidden, w_local, inv_temp.reshape(1, -1), target_ids.reshape(1, -1), n_dev
        )
        chunks = [(0, early)]
        begin = sum(made[0].shape[1] for made in early)
        for made in late:
            got = [made[0]]
            for p in range(1, n_dev):
                got.append(swap(made[p], p))
            chunks.append((begin, [got]))
            begin += made[0].shape[1]
        params, at_target = _merge(packs)
        out = None
        final = len(chunks) - 1
        plan = [(k, (0, 1)) for k in range(final + 1)] + [(k, (2, 3)) for k in range(final - 1)]
        plan += [(k, (p,)) for p in (2, 3) for k in (final - 1, final)]
        for i, (k, peers) in enumerate(plan):
            begin, got = chunks[k]
            blocks = [made[p] for made in got for p in peers]
            if k < final or peers[0] == 0:
                blocks = [pltpu.with_memory_space_constraint(a, pltpu.HBM) for a in blocks]
            res = _cdf(blocks, peers, params, out, n_dev, shard, begin, i == len(plan) - 1)
            out = res[0]
            params = res[1] if len(res) > 1 else None
        return out, at_target.reshape(-1)

    return jax.shard_map(
        local_step,
        mesh=mesh,
        in_specs=(P("dp", None), P(None, "vp"), P("dp"), P("dp")),
        out_specs=(P(("dp", "vp"), None), P("dp")),
        check_vma=False,
    )
```

```python
import functools

import jax
import jax.numpy as jnp
from jax import lax
from jax.experimental import pallas as pl
from jax.experimental.pallas import tpu as pltpu
from jax.sharding import PartitionSpec as P


LANES = 128
UNIT = 512
HALF = 256
DEPTH = 512
SLOTS = 9
FIRST = 256
EARLY = ((256, 1), (512, 1), (1024, 1), (2048, 2))
LATE = (4096, 2048, 2432, 1024, 256)
LATE_UNITS = ((2048, 2), (2048, 1), (2432, 1), (1024, 1), (256, 1))
STATS = 4


def _to_rows(vec_1xn):
    n = vec_1xn.shape[1]
    return jnp.transpose(jnp.broadcast_to(vec_1xn, (LANES, n)))


def _peer(me, p):
    return [me, me + 1 - 2 * lax.rem(me, 2), lax.rem(me + 2, 4), 3 - me][p]


def _logits_kernel(cfg, x_ref, w_ref, invt_ref, tgt_ref, *refs):
    n_dev, shard, segments, n_early, n_late = cfg
    refs = list(refs)

    def take(n):
        out = refs[:n]
        del refs[:n]
        return out

    early = [take(n_dev) for _ in range(n_early)]
    late = [take(n_dev) for _ in range(n_late)]
    packs = take(n_dev)
    zsend = take(n_early)
    xs, wfirst, wbuf, acc, zbuf, invt_v, tgt_v, pack_v = take(8)
    scale_rows, left_rows, tmp, m_ref, s_ref, t_ref = take(6)
    first_sem, w_sem, z_sem, x_sem, v_sem, own_sem, send_sem, recv_sem, pack_send, pack_recv = take(10)
    me = lax.axis_index("vp")
    batch, depth = xs.shape
    rows = batch // n_dev
    k_steps = depth // DEPTH
    assert SLOTS == k_steps + 1

    def rows_of(p):
        return pl.ds(pl.multiple_of(_peer(me, p) * rows, rows), rows)

    def fetch_w(seg, step):
        width, col0, g0 = segments[seg][0], segments[seg][3], segments[seg][4]
        slot = lax.rem(g0 + step, SLOTS)
        col = col0 + lax.div(step, k_steps) * width
        row = pl.multiple_of(lax.rem(step, k_steps) * DEPTH, DEPTH)
        return pltpu.make_async_copy(
            w_ref.at[pl.ds(row, DEPTH), pl.ds(pl.multiple_of(col, LANES), width)],
            wbuf.at[slot, :, pl.ds(0, width)],
            w_sem.at[slot],
        )

    def fetch_first(k):
        row = pl.ds(pl.multiple_of(k * DEPTH, DEPTH), DEPTH)
        return pltpu.make_async_copy(w_ref.at[row, pl.ds(0, FIRST)], wfirst.at[row, :], first_sem.at[k])

    def put_late(slot, c, off, width):
        return [
            pltpu.make_async_copy(
                zbuf.at[slot, pl.ds(p * rows, rows), pl.ds(0, width)],
                late[c][p].at[:, pl.ds(off, width)],
                z_sem.at[slot, p],
            )
            for p in range(n_dev)
        ]

    def put_own(u):
        return pltpu.make_async_copy(zsend[u].at[pl.ds(0, rows), :], early[u][0], own_sem.at[u])

    def send(u, p):
        return pltpu.make_async_remote_copy(
            src_ref=zsend[u].at[pl.ds(p * rows, rows), :],
            dst_ref=early[u][p],
            send_sem=send_sem.at[u, p],
            recv_sem=recv_sem.at[u, p],
            device_id={"vp": _peer(me, p)},
            device_id_type=pl.DeviceIdType.MESH,
        )

    x_copies = [
        pltpu.make_async_copy(x_ref.at[rows_of(p), :], xs.at[pl.ds(p * rows, rows), :], x_sem.at[p])
        for p in range(n_dev)
    ]
    small = [
        pltpu.make_async_copy(invt_ref, invt_v, v_sem.at[0]),
        pltpu.make_async_copy(tgt_ref, tgt_v, v_sem.at[1]),
    ]
    for copy in small + x_copies[2:]:
        copy.start()
    for k in range(k_steps):
        fetch_first(k).start()
    barrier = pltpu.get_barrier_semaphore()
    for p in range(1, n_dev):
        pl.semaphore_signal(
            barrier, inc=1, device_id={"vp": _peer(me, p)}, device_id_type=pl.DeviceIdType.MESH
        )
    m_ref[...] = jnp.full(m_ref.shape, -jnp.inf, jnp.float32)
    s_ref[...] = jnp.zeros_like(s_ref)
    t_ref[...] = jnp.zeros_like(t_ref)
    for copy in small:
        copy.wait()
    tmp[...] = _to_rows(invt_v[...])
    for p in range(n_dev):
        scale_rows[pl.ds(p * rows, rows), :] = tmp[rows_of(p), :]
    tmp[...] = _to_rows(tgt_v[...].astype(jnp.float32))
    lane = lax.broadcasted_iota(jnp.int32, (rows, LANES), 1)
    for p in range(n_dev):
        left_rows[pl.ds(p * rows, rows), :] = tmp[rows_of(p), :].astype(jnp.int32) - me * shard - lane
    for copy in x_copies[2:]:
        copy.wait()

    def multiply(seg, step):
        width = segments[seg][0]
        slot, k = lax.rem(segments[seg][4] + step, SLOTS), lax.rem(step, k_steps)
        x = xs[:, pl.ds(pl.multiple_of(k * DEPTH, DEPTH), DEPTH)]
        for off in range(0, width, HALF):
            wide = min(HALF, width - off)
            part = jnp.dot(x, wbuf[slot, :, off:off + wide], preferred_element_type=jnp.float32)
            acc[:, off:off + wide] = part + jnp.where(k == 0, 0.0, acc[:, off:off + wide])

    def finish(col, width, out_ref, out_off, lo=0, hi=batch):
        group = 32
        span = next(n for n in (UNIT, HALF, LANES) if width % n == 0)

        def some(j, _):
            at = pl.multiple_of(j * span, span)
            for r in range(lo, hi, group):
                block = slice(r, r + group)
                scale = scale_rows[block, :]
                tiles = []
                for t in range(0, span, LANES):
                    tile = acc[block, pl.ds(at + t, LANES)] * scale
                    out_ref[block, pl.ds(pl.multiple_of(out_off + at + t, LANES), LANES)] = tile
                    tiles.append(tile)
                m_old = m_ref[block, :]
                m_new = functools.reduce(jnp.maximum, tiles, m_old)
                keep = jnp.exp(m_old - m_new)
                total = s_ref[block, :] * keep
                upto = t_ref[block, :] * keep
                left = left_rows[block, :]
                for t, tile in enumerate(tiles):
                    e = jnp.exp(tile - m_new)
                    total += e
                    upto += jnp.where(left >= col + at + t * LANES, e, 0.0)
                m_ref[block, :] = m_new
                s_ref[block, :] = total
                t_ref[block, :] = upto
            return 0

        lax.fori_loop(0, width // span, some, 0)

    sent, own, stored = [], [], []

    def send_early(u, peers):
        for p in peers:
            copy = send(u, p)
            copy.start()
            sent.append(copy)

    far = 2 * rows

    def multiply_first(k, lo, hi):
        at = pl.ds(pl.multiple_of(k * DEPTH, DEPTH), DEPTH)
        part = jnp.dot(xs[lo:hi, at], wfirst[at, :], preferred_element_type=jnp.float32)
        acc[lo:hi, :FIRST] = part + jnp.where(k == 0, 0.0, acc[lo:hi, :FIRST])

    def far_step(k, _):
        fetch_first(k).wait()

        @pl.when(k == 0)
        def _():
            for copy in x_copies[:2]:
                copy.start()

        fetch_w(0, k).start()
        multiply_first(k, far, batch)
        return 0

    def near_step(k, _):
        multiply_first(k, 0, far)
        return 0

    lax.fori_loop(0, k_steps, far_step, 0)
    finish(0, FIRST, zsend[0], 0, far, batch)
    pl.semaphore_wait(barrier, n_dev - 1)
    send_early(0, (2, 3))
    for copy in x_copies[:2]:
        copy.wait()

    def first_near():
        lax.fori_loop(0, k_steps, near_step, 0)
        finish(0, FIRST, zsend[0], 0, 0, far)
        send_early(0, (1,))
        copy = put_own(0)
        copy.start()
        own.append(copy)

    early_units = 1
    for seg, (width, n, chunk, col0, g0) in enumerate(segments):
        for i in range(n):

            def body(k, _, seg=seg, i=i, n=n):
                step = i * k_steps + k
                ahead = step + SLOTS - 1

                @pl.when(ahead < n * k_steps)
                def _():
                    fetch_w(seg, ahead).start()

                if seg + 1 < len(segments):
                    @pl.when(ahead >= n * k_steps)
                    def _():
                        fetch_w(seg + 1, ahead - n * k_steps).start()

                fetch_w(seg, step).wait()
                multiply(seg, step)
                return 0

            lax.fori_loop(0, k_steps, body, 0)
            col = col0 + i * width
            if chunk is None:
                u = early_units
                early_units += 1
                finish(col, width, zsend[u], 0)
                send_early(u, (2, 3, 1))
                copy = put_own(u)
                copy.start()
                own.append(copy)
                if u == 2:
                    first_near()
            else:
                slot = len(stored) % 2
                if len(stored) >= 2:
                    for copy in stored[-2]:
                        copy.wait()
                finish(col, width, zbuf.at[slot], 0)
                c, off = chunk
                copies = put_late(slot, c, off + i * width, width)
                for copy in copies:
                    copy.start()
                stored.append(copies)
    m = m_ref[...]
    m_row = jnp.max(m, axis=1, keepdims=True)
    keep = jnp.exp(m - m_row)
    s_row = jnp.sum(s_ref[...] * keep, axis=1, keepdims=True)
    t_row = jnp.sum(t_ref[...] * keep, axis=1, keepdims=True)
    which = lax.broadcasted_iota(jnp.int32, m.shape, 1)
    packed = jnp.where(which == 0, m_row, jnp.where(which == 1, s_row, t_row))
    for p in range(n_dev):
        tmp[rows_of(p), :] = packed[p * rows:(p + 1) * rows, :]
    pack_v[...] = jnp.transpose(tmp[...])[:STATS, :]
    for p in (2, 3, 1):
        copy = pltpu.make_async_remote_copy(
            src_ref=pack_v,
            dst_ref=packs[p],
            send_sem=pack_send.at[p],
            recv_sem=pack_recv.at[p],
            device_id={"vp": _peer(me, p)},
            device_id_type=pl.DeviceIdType.MESH,
        )
        copy.start()
        sent.append(copy)
    copy = pltpu.make_async_copy(pack_v, packs[0], pack_send.at[0])
    copy.start()
    own.append(copy)
    for copies in stored[-2:]:
        for copy in copies:
            copy.wait()
    for copy in own + sent:
        copy.wait()


def _logits(x, w, invt, tgt, n_dev):
    batch, depth = x.shape
    shard = w.shape[1]
    rows = batch // n_dev
    segments, col, g0 = [], FIRST, 0
    chunk_of = {}
    units = [FIRST] + [width for width, n in EARLY for _ in range(n)]
    n_early, begin = len(units), sum(units)
    for c, width in enumerate(LATE):
        chunk_of.update({begin + i: (c, i) for i in range(0, width, LANES)})
        begin += width
    for i, (width, n) in enumerate(EARLY + LATE_UNITS):
        segments.append((width, n, None if i < len(EARLY) else chunk_of[col], col, g0))
        col += width * n
        g0 += n * (depth // DEPTH)
    assert col == shard == begin
    hbm = pl.BlockSpec(memory_space=pltpu.HBM)
    out_shape = [pltpu.HBM((rows, width), jnp.float32) for width in [*units, *LATE] for _ in range(n_dev)]
    out_shape += [pltpu.HBM((STATS, batch), jnp.float32)] * n_dev
    table = pltpu.VMEM((batch, LANES), jnp.float32)
    widest = max(width for width, _ in EARLY + LATE_UNITS)
    dma = pltpu.SemaphoreType.DMA
    res = pl.pallas_call(
        functools.partial(_logits_kernel, (n_dev, shard, segments, n_early, len(LATE))),
        in_specs=[hbm] * 4,
        out_specs=[hbm] * len(out_shape),
        out_shape=out_shape,
        scratch_shapes=[pltpu.VMEM((batch, width), jnp.float32) for width in units] + [
            pltpu.VMEM((batch, depth), jnp.bfloat16),
            pltpu.VMEM((depth, FIRST), jnp.bfloat16),
            pltpu.VMEM((SLOTS, DEPTH, widest), jnp.bfloat16),
            pltpu.VMEM((batch, widest), jnp.float32),
            pltpu.VMEM((2, batch, widest), jnp.float32),
            pltpu.VMEM((1, batch), jnp.float32),
            pltpu.VMEM((1, batch), jnp.int32),
            pltpu.VMEM((STATS, batch), jnp.float32),
            table,
            pltpu.VMEM((batch, LANES), jnp.int32),
            table,
            table,
            table,
            table,
            dma((depth // DEPTH,)),
            dma((SLOTS,)),
            dma((2, n_dev)),
            dma((n_dev,)),
            dma((2,)),
            dma((n_early,)),
            dma((n_early, n_dev)),
            dma((n_early, n_dev)),
            dma((n_dev,)),
            dma((n_dev,)),
        ],
        compiler_params=pltpu.CompilerParams(
            collective_id=0, has_side_effects=True, vmem_limit_bytes=52 * 2**20
        ),
        cost_estimate=pl.CostEstimate(
            flops=2 * batch * depth * shard,
            bytes_accessed=2 * depth * shard,
            transcendentals=batch * shard,
        ),
        name="logits",
    )(*(pltpu.with_memory_space_constraint(a, pltpu.HBM) for a in (x, w, invt, tgt)))
    blocks = [res[c * n_dev:(c + 1) * n_dev] for c in range(n_early + len(LATE) + 1)]
    return blocks[:n_early], blocks[n_early:-1], blocks[-1]


def _merge_kernel(n_dev, *refs):
    stats, (params_ref, at_ref) = refs[:n_dev], refs[n_dev:]
    me = lax.axis_index("vp")
    batch = stats[0].shape[1]
    rows = batch // n_dev
    ms = [s[0:1, :] for s in stats]
    top = functools.reduce(jnp.maximum, ms)
    keep = [jnp.exp(m - top) for m in ms]
    mass = [s[1:2, :] * k for s, k in zip(stats, keep)]
    upto = sum(s[2:3, :] * k for s, k in zip(stats, keep))
    total = sum(mass)
    at_ref[...] = upto / total
    values = [top, 1.0 / total]
    for p in range(n_dev):
        start = jnp.zeros_like(total)
        for q in range(n_dev):
            start += jnp.where((me ^ q) < (me ^ p), mass[q], 0.0)
        values.append(start)
    which = lax.broadcasted_iota(jnp.int32, (LANES, batch), 0)
    table = jnp.zeros((LANES, batch), jnp.float32)
    for i, v in enumerate(values):
        table = jnp.where(which == i, v, table)
    per_row = jnp.transpose(table)
    out = jnp.zeros((rows, LANES), jnp.float32)
    for d in range(n_dev):
        out = jnp.where(me == d, per_row[d * rows:(d + 1) * rows, :], out)
    params_ref[...] = out


def _merge(stats):
    n_dev = len(stats)
    batch = stats[0].shape[1]
    vmem = pl.BlockSpec(memory_space=pltpu.VMEM)
    return pl.pallas_call(
        functools.partial(_merge_kernel, n_dev),
        in_specs=[vmem] * n_dev,
        out_specs=[vmem] * 2,
        out_shape=[
            jax.ShapeDtypeStruct((batch // n_dev, LANES), jnp.float32),
            jax.ShapeDtypeStruct((1, batch), jnp.float32),
        ],
        cost_estimate=pl.CostEstimate(flops=100_000, bytes_accessed=100_000, transcendentals=1000),
        name="merge",
    )(*stats)


def _cdf_kernel(cfg, *refs):
    peers, shard, base, widths, first, last = cfg
    n = len(peers)
    width = sum(widths)
    parts, refs = [refs[a * n:(a + 1) * n] for a in range(len(widths))], refs[len(widths) * n:]
    params_ref = refs[0]
    if last:
        out_ref, y_ref, sems = refs[2:]
    else:
        out_ref, params_out, y_ref, sems = refs[1 if first else 2:]
    me = lax.axis_index("vp")
    rows = params_ref.shape[0]
    params = params_ref[...]
    top = jnp.broadcast_to(params[:, 0:1], (rows, LANES))
    inv = jnp.broadcast_to(params[:, 1:2], (rows, LANES))
    k_id = lax.broadcasted_iota(jnp.int32, (3 * LANES, 2 * LANES), 0) % LANES
    n_id = lax.broadcasted_iota(jnp.int32, (3 * LANES, 2 * LANES), 1)
    tri = jnp.where(k_id <= n_id, 1.0, 0.0).astype(jnp.bfloat16)
    lane = lax.broadcasted_iota(jnp.int32, (rows, LANES), 1)

    def unit(part, at, col, wide, carries):
        ends = []
        for j in range(n):
            cols = [pl.ds(col + t, LANES) for t in range(0, wide, LANES)]
            e = jnp.concatenate([jnp.exp(part[j][:, c] - top) for c in cols], axis=0)
            hi = e.astype(jnp.bfloat16)
            r1 = e - hi.astype(jnp.float32)
            mid = r1.astype(jnp.bfloat16)
            lo = (r1 - mid.astype(jnp.float32)).astype(jnp.bfloat16)
            sums = jnp.dot(jnp.concatenate([hi, mid, lo], axis=1), tri, preferred_element_type=jnp.float32)
            carry = carries[j]
            for t in range(len(cols)):
                block = slice(t * rows, (t + 1) * rows)
                y_ref[j, :, pl.ds(at + col + t * LANES, LANES)] = (sums[block, :LANES] + carry) * inv
                carry = carry + sums[block, LANES:]
            ends.append(carry)
        return tuple(ends)

    carries = tuple(jnp.broadcast_to(params[:, 2 + p:3 + p], (rows, LANES)) for p in peers)
    at = 0
    for part, wide in zip(parts, widths):
        n_full = wide // UNIT
        if n_full:
            carries = lax.fori_loop(
                0, n_full, lambda u, c, part=part, at=at: unit(part, at, pl.multiple_of(u * UNIT, UNIT), UNIT, c), carries
            )
        if wide % UNIT:
            carries = unit(part, at, n_full * UNIT, wide % UNIT, carries)
        at += wide
    copies = []
    updated = params
    for j, p in enumerate(peers):
        where = pl.multiple_of((me ^ p) * shard + base, LANES)
        copy = pltpu.make_async_copy(y_ref.at[j], out_ref.at[:, pl.ds(where, width)], sems.at[j])
        copy.start()
        copies.append(copy)
        updated = jnp.where(lane == 2 + p, carries[j], updated)
    if not last:
        params_out[...] = updated
    for copy in copies:
        copy.wait()


def _cdf(blocks, peers, params, out, n_dev, shard, base, last=False):
    n = len(peers)
    rows = blocks[0].shape[0]
    widths = tuple(b.shape[1] for b in blocks[::n])
    width = sum(widths)
    first = out is None
    vmem = pl.BlockSpec(memory_space=pltpu.VMEM)
    hbm = pl.BlockSpec(memory_space=pl.ANY)
    return pl.pallas_call(
        functools.partial(_cdf_kernel, (peers, shard, base, widths, first, last)),
        in_specs=[vmem] * (len(blocks) + 1) + ([] if first else [hbm]),
        out_specs=[hbm] + ([] if last else [vmem]),
        out_shape=[jax.ShapeDtypeStruct((rows, n_dev * shard), jnp.float32)]
        + ([] if last else [jax.ShapeDtypeStruct(params.shape, jnp.float32)]),
        scratch_shapes=[
            pltpu.VMEM((n, rows, width), jnp.float32),
            pltpu.SemaphoreType.DMA((n,)),
        ],
        input_output_aliases={} if first else {len(blocks) + 1: 0},
        compiler_params=pltpu.CompilerParams(vmem_limit_bytes=24 * 2**20),
        cost_estimate=pl.CostEstimate(
            flops=n * 2 * rows * width * 384,
            bytes_accessed=n * rows * width * 8,
            transcendentals=n * rows * width,
        ),
        name="cdf",
    )(*blocks, params, *(() if first else (out,)))


def solution(mesh):
    n_dev = mesh.shape["vp"]
    assert n_dev == 4

    def swap(a, p):
        return lax.ppermute(a, "vp", [(i, i ^ p) for i in range(n_dev)])

    def local_step(hidden, w_local, inv_temp, target_ids):
        shard = w_local.shape[1]
        early, late, packs = _logits(
            hidden, w_local, inv_temp.reshape(1, -1), target_ids.reshape(1, -1), n_dev
        )
        chunks = [(0, early)]
        begin = sum(made[0].shape[1] for made in early)
        for made in late:
            got = [made[0]]
            for p in range(1, n_dev):
                got.append(swap(made[p], p))
            chunks.append((begin, [got]))
            begin += made[0].shape[1]
        params, at_target = _merge(packs)
        out = None
        final = len(chunks) - 1
        plan = [(k, peers) for peers in ((0, 1), (2, 3)) for k in range(final + 1)]
        for i, (k, peers) in enumerate(plan):
            begin, got = chunks[k]
            blocks = [made[p] for made in got for p in peers]
            if k < final or peers[0] == 0:
                blocks = [pltpu.with_memory_space_constraint(a, pltpu.HBM) for a in blocks]
            res = _cdf(blocks, peers, params, out, n_dev, shard, begin, i == len(plan) - 1)
            out = res[0]
            params = res[1] if len(res) > 1 else None
        return out, at_target.reshape(-1)

    return jax.shard_map(
        local_step,
        mesh=mesh,
        in_specs=(P("dp", None), P(None, "vp"), P("dp"), P("dp")),
        out_specs=(P(("dp", "vp"), None), P("dp")),
        check_vma=False,
    )
```
